8 devices in a mesh: dp: 1 (over z), ep: 8 (over y, x, core).
Axes of the slice: x: 2, y: 2, z: 1, core: 2. Of those that a mesh axis runs over, the one named last changes fastest.
Arguments:
- hidden: bfloat16 [2048, 1536], P(('dp', 'ep'))
- router_w: float32 [1536, 32], replicated
- expert_ids: int32 [2048, 2], P(('dp', 'ep'))
- w_gate: bfloat16 [32, 1536, 2304], P('ep')
- w_up: bfloat16 [32, 1536, 2304], P('ep')
- w_down: bfloat16 [32, 2304, 1536], P('ep')
- post_scale: float32 [2], replicated
Outputs:
- output: bfloat16 [2048, 1536], P(('dp', 'ep'))
All inputs are finite; a program needn't handle non-finite values.
Results may differ from the reference program's by a relative error of at most 0.001.
Values are sent between devices in bfloat16 or wider.
A program may use at most 1 GiB of HBM per device.

```python
import jax
import jax.numpy as jnp
from jax import lax

GROUP_SIZE = 8
TOKENS_DEV = 256
EXPERTS = 32
HIDDEN = 1536
FFN_DIM = 2304
TOP_K = 2
BATCH_ROWS = GROUP_SIZE * TOKENS_DEV
HOT_COUNT = max(1, EXPERTS // 8)
CAPACITY = TOKENS_DEV // HOT_COUNT
MAX_ROWS = GROUP_SIZE * CAPACITY


def draw_routing(ids_key, part):
    order_key, shard_key = jax.random.split(ids_key)
    expert_order = jax.random.permutation(order_key, EXPERTS)
    hot_ids = expert_order[:HOT_COUNT]
    cold_ids = expert_order[HOT_COUNT:]
    shard_keys = jax.random.split(jax.random.fold_in(shard_key, part), GROUP_SIZE)

    def one_shard(one_key):
        tok_key, cold_key, swap_key = jax.random.split(one_key, 3)
        tok_rank = jax.random.permutation(tok_key, TOKENS_DEV)
        cold_mix = jax.random.permutation(cold_key, cold_ids)
        first_pick = hot_ids[tok_rank % HOT_COUNT]
        second_pick = cold_mix[tok_rank % (EXPERTS - HOT_COUNT)]
        swapped = jax.random.randint(swap_key, (TOKENS_DEV,), 0, 2) == 1
        return jnp.stack([jnp.where(swapped, second_pick, first_pick), jnp.where(swapped, first_pick, second_pick)], axis=1)

    return jax.vmap(one_shard)(shard_keys).reshape(BATCH_ROWS, TOP_K).astype(jnp.int32)


def draw_experts(weight_key, row_count, col_count):
    expert_keys = jax.random.split(weight_key, EXPERTS)
    return lax.map(lambda one_key: (jax.random.normal(one_key, (row_count, col_count), jnp.float32) * row_count ** -0.5).astype(jnp.bfloat16), expert_keys)


def setup_inputs(seed: int = 0, part: int = 0) -> dict:
    base_key = jax.random.key(seed)
    hid_key, route_key, gate_key, up_key, down_key, post_key, ids_key = jax.random.split(base_key, 7)
    hidden = jax.random.normal(jax.random.fold_in(hid_key, part), (BATCH_ROWS, HIDDEN), jnp.float32).astype(jnp.bfloat16)
    router_w = jax.random.normal(route_key, (HIDDEN, EXPERTS), jnp.float32) * (0.4 * HIDDEN ** -0.5)
    w_gate = draw_experts(gate_key, HIDDEN, FFN_DIM)
    w_up = draw_experts(up_key, HIDDEN, FFN_DIM)
    w_down = draw_experts(down_key, FFN_DIM, HIDDEN)
    post_scale = jax.random.uniform(post_key, (2,), jnp.float32, jnp.array([0.5, 1.0], jnp.float32), jnp.array([1.0, 2.0], jnp.float32))
    expert_ids = draw_routing(ids_key, part)
    return {'hidden': hidden, 'router_w': router_w, 'expert_ids': expert_ids, 'w_gate': w_gate, 'w_up': w_up, 'w_down': w_down, 'post_scale': post_scale}


def reference(hidden, router_w, expert_ids, w_gate, w_up, w_down, post_scale):
    hid_wide = hidden.astype(jnp.float32)
    logits = jnp.dot(hid_wide, router_w, preferred_element_type=jnp.float32)
    router_prob = jax.nn.softmax(logits, axis=-1)
    picked = jnp.take_along_axis(router_prob, expert_ids, axis=1)
    gates = picked / jnp.sum(picked, axis=1, keepdims=True)

    def add_expert(running_sum, expert):
        hit_mask = expert_ids == expert
        tok_gate = jnp.sum(jnp.where(hit_mask, gates, 0.0), axis=1)
        chosen = jnp.any(hit_mask, axis=1)
        row_index = jnp.nonzero(chosen, size=MAX_ROWS, fill_value=0)[0]
        in_range = jnp.arange(MAX_ROWS) < jnp.sum(chosen)
        tok_rows = hidden[row_index]
        gate_in = jnp.dot(tok_rows, w_gate[expert], preferred_element_type=jnp.float32)
        up_in = jnp.dot(tok_rows, w_up[expert], preferred_element_type=jnp.float32)
        middle = (jax.nn.silu(gate_in) * up_in).astype(jnp.bfloat16)
        expert_out = jnp.dot(middle, w_down[expert], preferred_element_type=jnp.float32).astype(jnp.bfloat16)
        row_weight = jnp.where(in_range, tok_gate[row_index], 0.0)
        running_sum = running_sum.at[row_index].add(row_weight[:, None] * expert_out.astype(jnp.float32))
        return running_sum, None

    mixed, _ = lax.scan(add_expert, jnp.zeros((BATCH_ROWS, HIDDEN), jnp.float32), jnp.arange(EXPERTS))
    return (post_scale[0] * hid_wide + post_scale[1] * mixed).astype(jnp.bfloat16)
```

```python
import functools

import jax
import jax.numpy as jnp
from jax import lax
from jax.experimental import pallas as pl
from jax.experimental.pallas import tpu as pltpu
from jax.sharding import PartitionSpec as P

MESH = pl.DeviceIdType.MESH
F32, BF16, I32 = jnp.float32, jnp.bfloat16, jnp.int32
NT = (((1,), (1,)), ((), ()))


def flip(idx, mask):
    out = idx
    for bit in (1, 2, 4):
        if mask & bit:
            out = out + bit - 2 * bit * ((idx // bit) % 2)
    return out


def dev(idx):
    return (lax.axis_index('dp'), idx)


def iota(shape, dim):
    return lax.broadcasted_iota(I32, shape, dim)


CHUNKS = 4


def gather_kernel(caps, hid, ids, wrt, h_all, pos, tok, cap, ids_all, send, recv, id_send, id_recv, own_sem):
    me = lax.axis_index('ep')
    tokens, width = hid.shape
    experts = wrt.shape[0]
    owners = h_all.shape[0]
    local = experts // owners
    rows = tokens // CHUNKS
    barrier = pltpu.get_barrier_semaphore()
    for q in range(1, owners):
        pl.semaphore_signal(barrier, inc=1, device_id=dev(flip(me, q)), device_id_type=MESH)
    pl.semaphore_wait(barrier, owners - 1)

    def piece(ref, c):
        return ref.at[pl.ds(c * rows, rows)]

    def remote(src, dst, n, to):
        return pltpu.make_async_remote_copy(src_ref=src, dst_ref=dst, send_sem=send.at[n], recv_sem=recv.at[n], device_id=dev(to), device_id_type=MESH)

    xn, yn, dg, mate = flip(me, 2), flip(me, 4), flip(me, 6), flip(me, 1)
    id_copies = []
    for q in range(1, owners):
        id_copies.append(pltpu.make_async_remote_copy(src_ref=ids, dst_ref=ids_all.at[q], send_sem=id_send.at[q], recv_sem=id_recv.at[q], device_id=dev(flip(me, q)), device_id_type=MESH))
    for c in id_copies:
        c.start()
    x_order, y_order = (0, 1, 2, 3), (2, 3, 0, 1)
    to_x = {c: remote(piece(hid, c), piece(h_all.at[me], c), c, xn) for c in x_order}
    to_y = {c: remote(piece(hid, c), piece(h_all.at[me], c), 4 + c, yn) for c in y_order}
    for cx, cy in zip(x_order, y_order):
        to_x[cx].start()
        to_y[cy].start()
    to_mate = remote(hid, h_all.at[me], 24, mate)
    to_mate.start()
    own = pltpu.make_async_copy(hid, h_all.at[me], own_sem)
    own.start()

    h = hid[...]
    w = wrt[...]
    w_hi = w.astype(BF16)
    rest = w - w_hi.astype(F32)
    w_mid = rest.astype(BF16)
    w_lo = (rest - w_mid.astype(F32)).astype(BF16)
    dot = functools.partial(lax.dot_general, dimension_numbers=NT, preferred_element_type=F32)
    logits = dot(h, w_hi) + (dot(h, w_mid) + dot(h, w_lo))
    ex = jnp.exp(logits - jnp.max(logits, axis=1, keepdims=True))
    prob = ex / jnp.sum(ex, axis=1, keepdims=True)
    eye = (iota((tokens, tokens), 0) == iota((tokens, tokens), 1)).astype(F32).astype(BF16)
    own_ids = ids[...].astype(F32)
    lane = iota((tokens, experts), 1).astype(F32)
    id_col = [dot(eye, jnp.broadcast_to(own_ids[k:k + 1], (8, tokens)).astype(BF16))[:, 0:1] for k in (0, 1)]
    pick = [(id_col[k] == lane).astype(F32) for k in (0, 1)]
    g = [jnp.sum(pick[k] * prob, axis=1, keepdims=True) for k in (0, 1)]
    total = g[0] + g[1]

    for c in id_copies:
        c.wait_recv()
    ids_all[0] = ids[...]
    most = None
    for q in range(owners):
        both = ids_all[q]
        e_col = iota((experts, tokens), 0)
        hot = ((both[0:1] == e_col) | (both[1:2] == e_col)).astype(F32).astype(BF16)
        count = dot(jnp.ones((8, tokens), BF16), hot)
        most = count if most is None else jnp.maximum(most, count)
    stride = jnp.floor((most + 15.0) * (1.0 / 16.0)) * 16.0
    ea, eb = iota((experts, experts), 0), iota((experts, experts), 1)
    same = ea // local == eb // local
    plain = functools.partial(jnp.dot, preferred_element_type=F32)
    offset = plain(stride.astype(BF16), (same & (ea < eb)).astype(F32).astype(BF16))
    need = jnp.max(plain(stride.astype(BF16), same.astype(F32).astype(BF16))).astype(I32)
    branch = jnp.int32(0)
    for limit in caps[:-1]:
        branch = branch + (need > limit).astype(I32)
    cap[0] = branch
    ta, tb = iota((tokens, tokens), 0), iota((tokens, tokens), 1)
    before = (tb < ta).astype(F32).astype(BF16)
    rank = plain(before, (pick[0] + pick[1]).astype(BF16))
    place = rank + offset[0:1]
    slot = [jnp.sum(pick[k] * place, axis=1, keepdims=True) for k in (0, 1)]
    owner = [jnp.floor(id_col[k] * (1.0 / local)) for k in (0, 1)]
    wide = iota((tokens, 128), 1)
    table = jnp.zeros((tokens, 128), F32)
    for n, col in enumerate((g[0] / total, g[1] / total, owner[0], owner[1], slot[0], slot[1])):
        table = jnp.where(wide == n, col, table)
    tok[...] = table
    rows_of = [[], []]
    for s in range(owners):
        both = ids_all[flip(me, s)]
        for k in (0, 1):
            rows_of[k].append(both[k:k + 1])
    first, second = (jnp.concatenate(rows_of[k], axis=0) for k in (0, 1))
    marks = jnp.concatenate([((first == me * local + j) | (second == me * local + j)).astype(F32) for j in range(local)], axis=0)
    earlier = plain(marks.astype(BF16), (ta < tb).astype(F32).astype(BF16))
    pos[...] = jnp.where(marks > 0.5, earlier, -1.0)

    sent = [*to_x.values(), *to_y.values(), to_mate]
    relayed = []
    for cx, cy in zip(x_order, y_order):
        to_x[cx].wait_recv()
        if cx in (0, 1):
            f = remote(piece(h_all.at[xn], cx), piece(h_all.at[xn], cx), 8 + cx, yn)
            f.start()
            relayed.append((cx, f))
        m = remote(piece(h_all.at[xn], cx), piece(h_all.at[xn], cx), 12 + cx, mate)
        m.start()
        sent.append(m)
        to_y[cy].wait_recv()
        if cy in (2, 3):
            f = remote(piece(h_all.at[yn], cy), piece(h_all.at[yn], cy), 8 + cy, xn)
            f.start()
            relayed.append((cy, f))
        m = remote(piece(h_all.at[yn], cy), piece(h_all.at[yn], cy), 16 + cy, mate)
        m.start()
        sent.append(m)
    for c, f in relayed:
        f.wait_recv()
        m = remote(piece(h_all.at[dg], c), piece(h_all.at[dg], c), 20 + c, mate)
        m.start()
        sent.append(m)
        sent.append(f)
    to_mate.wait_recv()
    for m in sent[9:]:
        if not any(m is f for _, f in relayed):
            m.wait_recv()
    for m in sent:
        m.wait_send()
    for c in id_copies:
        c.wait_send()
    own.wait()


def gather_call(hidden, ids_t, wr_t, owners, caps):
    tokens, width = hidden.shape
    experts = wr_t.shape[0]
    vmem = pl.BlockSpec(memory_space=pltpu.VMEM)
    return pl.pallas_call(
        functools.partial(gather_kernel, caps),
        name='gather_tokens',
        out_shape=(
            jax.ShapeDtypeStruct((owners, tokens, width), BF16),
            jax.ShapeDtypeStruct((experts // owners * owners, tokens), F32),
            jax.ShapeDtypeStruct((tokens, 128), F32),
            jax.ShapeDtypeStruct((1,), I32),
        ),
        in_specs=[vmem, vmem, vmem],
        out_specs=(pl.BlockSpec(memory_space=pl.ANY), vmem, vmem, pl.BlockSpec(memory_space=pltpu.SMEM)),
        scratch_shapes=[
            pltpu.VMEM((owners, 2, tokens), I32),
            pltpu.SemaphoreType.DMA((25,)),
            pltpu.SemaphoreType.DMA((25,)),
            pltpu.SemaphoreType.DMA((owners,)),
            pltpu.SemaphoreType.DMA((owners,)),
            pltpu.SemaphoreType.DMA,
        ],
        compiler_params=pltpu.CompilerParams(collective_id=0, has_side_effects=True),
    )(hidden, ids_t, wr_t)


NF = 3
RING = 4


def expert_kernel(caps, branch, pos, h_all, w1, w3, w2, ret, hbuf, xbuf, w1b, w3b, w2b, hot, mid, yacc, ybuf, zero, plan, hsem, wsem, ysem, zsem):
    sources, tokens, width = h_all.shape
    local, _, ffn = w1.shape
    ft = ffn // NF
    steps = local * NF
    slots = hot.shape[0] // local

    unit = []
    for j in range(local):
        most = jnp.max(pos[pl.ds(j * sources, sources), :]).astype(I32) + 1
        unit.append((most + 15) // 16)
    for j in range(local):
        rank = jnp.int32(0)
        offset = jnp.int32(0)
        for i in range(local):
            if i != j:
                ahead = (unit[i] >= unit[j]) if i < j else (unit[i] > unit[j])
                rank = rank + ahead.astype(I32)
            if i < j:
                offset = offset + unit[i]
        plan[0, rank] = jnp.int32(j)
        plan[1, rank] = unit[j]
        plan[2, rank] = offset
    used = unit[0] + unit[1] + unit[2] + unit[3]

    def weights(t):
        e = plan[0, t // NF]
        cols = pl.ds(pl.multiple_of((t % NF) * ft, ft), ft)
        n = t % RING
        return (
            pltpu.make_async_copy(w1.at[e, :, cols], w1b.at[n], wsem.at[n, 0]),
            pltpu.make_async_copy(w3.at[e, :, cols], w3b.at[n], wsem.at[n, 1]),
            pltpu.make_async_copy(w2.at[e, cols, :], w2b.at[n], wsem.at[n, 2]),
        )

    def tokens_in(s):
        return pltpu.make_async_copy(h_all.at[s], hbuf.at[s], hsem.at[s])

    for s in range(sources):
        tokens_in(s).start()
    for t in range(RING):
        for c in weights(jnp.int32(t)):
            c.start()

    limit = jnp.int32(caps[0])
    for n in range(1, len(caps)):
        limit = jnp.where(branch[0] >= n, caps[n], limit)
    zero[...] = jnp.zeros_like(zero)
    spare = limit // 16 - used

    def fill(n):
        s, u = n // spare, n % spare
        return pltpu.make_async_copy(zero, ret.at[s, pl.ds(pl.multiple_of((used + u) * 16, 16), 16)], zsem)

    for s in range(sources):
        tokens_in(s).wait()
        for r in range(local):
            row = pos[pl.ds(plan[0, r] * sources + s, 1), :]
            match = iota((slots, tokens), 0).astype(F32) == row
            hot[pl.ds(r * slots, slots), :] = match.astype(F32).astype(BF16)

        @pl.loop(0, width // 512)
        def _(n):
            cols = pl.ds(pl.multiple_of(n * 512, 512), 512)
            part = jnp.dot(hot[...], hbuf[s, :, cols], preferred_element_type=F32).astype(BF16)
            for r in range(local):
                first = pl.multiple_of(plan[1, r] * (16 * s), 16)
                xbuf[r, pl.ds(first, slots), cols] = part[r * slots:(r + 1) * slots]

    @pl.loop(0, sources * spare)
    def _(n):
        fill(n).start()

    def out_copies(r, units):
        st = 16 * units
        first = pl.multiple_of(plan[2, r] * 16, 16)
        return [pltpu.make_async_copy(ybuf.at[r, pl.ds(s * st, st)], ret.at[s, pl.ds(first, st)], ysem) for s in range(sources)]

    @pl.loop(0, local)
    def _(r):
        @pl.loop(0, NF)
        def _(f):
            t = r * NF + f
            n = t % RING
            for c in weights(t):
                c.wait()
            for units in range(1, slots // 16 + 1):
                m = 16 * units * sources

                @pl.when(plan[1, r] == units)
                def _():
                    @pl.loop(0, ft // 256)
                    def _(i):
                        cols = pl.ds(pl.multiple_of(i * 256, 256), 256)
                        gate = jnp.dot(xbuf[r, 0:m, :], w1b[n, :, cols], preferred_element_type=F32)
                        up = jnp.dot(xbuf[r, 0:m, :], w3b[n, :, cols], preferred_element_type=F32)
                        mid[0:m, cols] = (gate * jax.nn.sigmoid(gate) * up).astype(BF16)

                    @pl.loop(0, width // 512)
                    def _(i):
                        cols = pl.ds(pl.multiple_of(i * 512, 512), 512)
                        part = jnp.dot(mid[0:m, :], w2b[n, :, cols], preferred_element_type=F32)
                        old = yacc[0:m, cols]
                        yacc[0:m, cols] = jnp.where(f == 0, 0.0, old) + part

                    @pl.when(f == NF - 1)
                    def _():
                        ybuf[r, 0:m, :] = yacc[0:m, :].astype(BF16)
                        for c in out_copies(r, units):
                            c.start()

            @pl.when(t + RING < steps)
            def _():
                for c in weights(t + RING):
                    c.start()

    @pl.loop(0, local)
    def _(r):
        for units in range(1, slots // 16 + 1):
            @pl.when(plan[1, r] == units)
            def _():
                for c in out_copies(r, units):
                    c.wait()

    @pl.loop(0, sources * spare)
    def _(n):
        fill(n).wait()


def expert_call(branch, pos, h_all, w1, w3, w2, caps):
    sources, tokens, width = h_all.shape
    local, _, ffn = w1.shape
    slots = caps[-1] // local
    ft = ffn // NF
    hbm = pl.BlockSpec(memory_space=pl.ANY)
    flops = 3 * 2 * local * slots * sources * width * ffn // 2
    return pl.pallas_call(
        functools.partial(expert_kernel, caps),
        name='experts',
        out_shape=jax.ShapeDtypeStruct((sources, caps[-1], width), BF16),
        in_specs=[pl.BlockSpec(memory_space=pltpu.SMEM), pl.BlockSpec(memory_space=pltpu.VMEM), hbm, hbm, hbm, hbm],
        out_specs=hbm,
        scratch_shapes=[
            pltpu.VMEM((sources, tokens, width), BF16),
            pltpu.VMEM((local, sources * slots + slots, width), BF16),
            pltpu.VMEM((RING, width, ft), BF16),
            pltpu.VMEM((RING, width, ft), BF16),
            pltpu.VMEM((RING, ft, width), BF16),
            pltpu.VMEM((local * slots, tokens), BF16),
            pltpu.VMEM((sources * slots, ft), BF16),
            pltpu.VMEM((sources * slots, width), F32),
            pltpu.VMEM((local, sources * slots, width), BF16),
            pltpu.VMEM((16, width), BF16),
            pltpu.SMEM((3, local), I32),
            pltpu.SemaphoreType.DMA((sources,)),
            pltpu.SemaphoreType.DMA((RING, 3)),
            pltpu.SemaphoreType.DMA,
            pltpu.SemaphoreType.DMA,
        ],
        compiler_params=pltpu.CompilerParams(vmem_limit_bytes=60 * 1024 * 1024),
        cost_estimate=pl.CostEstimate(flops=flops, bytes_accessed=3 * 2 * local * width * ffn, transcendentals=0),
    )(branch, pos, h_all, w1, w3, w2)


ORDER = (0, 1, 2, 4, 6, 3, 5, 7)


def return_kernel(cap, ret, tok, hid, scale, out, got, acc, send, recv):
    me = lax.axis_index('ep')
    owners = ret.shape[0]
    tokens, width = hid.shape
    barrier = pltpu.get_barrier_semaphore()
    for q in range(1, owners):
        pl.semaphore_signal(barrier, inc=1, device_id=dev(flip(me, q)), device_id_type=MESH)
    pl.semaphore_wait(barrier, owners - 1)
    copies = {}
    for q in ORDER[2:] + (1,):
        to = flip(me, q)
        copies[q] = pltpu.make_async_remote_copy(src_ref=ret.at[to, pl.ds(0, cap)], dst_ref=got.at[q], send_sem=send.at[q], recv_sem=recv.at[q], device_id=dev(to), device_id_type=MESH)
        copies[q].start()
    own = pltpu.make_async_copy(ret.at[me, pl.ds(0, cap)], got.at[0], recv.at[0])
    own.start()
    table = tok[...]
    lane = iota((tokens, cap), 1).astype(F32)
    for q in ORDER:
        if q == 0:
            own.wait()
        else:
            copies[q].wait_recv()
        peer = flip(me, q).astype(F32)
        hot = jnp.concatenate([((table[:, 2 + k:3 + k] == peer) & (table[:, 4 + k:5 + k] == lane)).astype(F32).astype(BF16) for k in (0, 1)], axis=0)

        @pl.loop(0, width // 256)
        def _(n):
            cols = pl.ds(pl.multiple_of(n * 256, 256), 256)
            part = jnp.dot(hot, got[q, :, cols], preferred_element_type=F32)
            acc[:, cols] = part if q == 0 else acc[:, cols] + part

    mixed = table[:, 0:1] * acc[0:tokens] + table[:, 1:2] * acc[tokens:2 * tokens]
    out[...] = (scale[0] * hid[...].astype(F32) + scale[1] * mixed).astype(BF16)
    for q in copies:
        copies[q].wait_send()


def return_call(n, cap, ret, tok, hidden, scale):
    owners, _, width = ret.shape
    tokens = hidden.shape[0]
    vmem = pl.BlockSpec(memory_space=pltpu.VMEM)
    return pl.pallas_call(
        functools.partial(return_kernel, cap),
        name=f'return_{cap}',
        out_shape=jax.ShapeDtypeStruct((tokens, width), BF16),
        in_specs=[pl.BlockSpec(memory_space=pl.ANY), vmem, vmem, pl.BlockSpec(memory_space=pltpu.SMEM)],
        out_specs=vmem,
        scratch_shapes=[
            pltpu.VMEM((owners, cap, width), BF16),
            pltpu.VMEM((2 * tokens, width), F32),
            pltpu.SemaphoreType.DMA((owners,)),
            pltpu.SemaphoreType.DMA((owners,)),
        ],
        compiler_params=pltpu.CompilerParams(collective_id=1 + n, has_side_effects=True, vmem_limit_bytes=40 * 1024 * 1024),
    )(ret, tok, hidden, scale)


def capacities(local, slots):
    full = [slots * n + 16 * (local - n) for n in range(1, local + 1)]
    return tuple(sorted({full[0] + 16, *full}))


def solution(mesh):
    owners = mesh.shape['ep']

    def local_step(hidden, router_w, expert_ids, w_gate, w_up, w_down, post_scale):
        tokens = hidden.shape[0]
        local = w_gate.shape[0]
        slots = tokens // max(1, local * owners // 8)
        caps = capacities(local, slots)
        h_all, pos, tok, branch = gather_call(hidden, expert_ids.T, router_w.T, owners, caps)
        ret = expert_call(branch, pos, h_all, w_gate, w_up, w_down, caps)
        branches = [functools.partial(return_call, n, cap) for n, cap in enumerate(caps)]
        return lax.switch(branch[0], branches, ret, tok, hidden, post_scale)

    tok_spec = P(('dp', 'ep'))
    return jax.shard_map(local_step, mesh=mesh, in_specs=(tok_spec, P(), tok_spec, P('ep'), P('ep'), P('ep'), P()), out_specs=tok_spec, check_vma=False)
```

```python
import functools

import jax
import jax.numpy as jnp
from jax import lax
from jax.experimental import pallas as pl
from jax.experimental.pallas import tpu as pltpu
from jax.sharding import PartitionSpec as P

MESH = pl.DeviceIdType.MESH
F32, BF16, I32 = jnp.float32, jnp.bfloat16, jnp.int32
NT = (((1,), (1,)), ((), ()))


def flip(idx, mask):
    out = idx
    for bit in (1, 2, 4):
        if mask & bit:
            out = out + bit - 2 * bit * ((idx // bit) % 2)
    return out


def dev(idx):
    return (lax.axis_index('dp'), idx)


def iota(shape, dim):
    return lax.broadcasted_iota(I32, shape, dim)


CHUNKS = 4
NF = 3
RING = 2


def gather_kernel(caps, hid, ids, wrt, w1, w3, w2, rows_out, pos, tok, cap, w1p, w3p, w2p, land, ids_all, send, recv, id_send, id_recv, wsem):
    me = lax.axis_index('ep')
    tokens, width = hid.shape
    experts = wrt.shape[0]
    local, owners, slots, _ = rows_out.shape
    ft = w1p.shape[2]
    rows = tokens // CHUNKS
    barrier = pltpu.get_barrier_semaphore()
    for q in range(1, owners):
        pl.semaphore_signal(barrier, inc=1, device_id=dev(flip(me, q)), device_id_type=MESH)
    pl.semaphore_wait(barrier, owners - 1)

    def piece(q, c):
        return (hid if q == 0 else land.at[q]).at[pl.ds(c * rows, rows)]

    def remote(q, c, n, to):
        return pltpu.make_async_remote_copy(src_ref=piece(q, c), dst_ref=land.at[q ^ to, pl.ds(c * rows, rows)], send_sem=send.at[n], recv_sem=recv.at[n], device_id=dev(flip(me, to)), device_id_type=MESH)

    id_copies = []
    for q in range(1, owners):
        id_copies.append(pltpu.make_async_remote_copy(src_ref=ids, dst_ref=ids_all.at[q], send_sem=id_send.at[q], recv_sem=id_recv.at[q], device_id=dev(flip(me, q)), device_id_type=MESH))
    for c in id_copies:
        c.start()
    x_order, y_order = (0, 1, 2, 3), (2, 3, 0, 1)
    to_x = {c: remote(0, c, c, 2) for c in x_order}
    to_y = {c: remote(0, c, 4 + c, 4) for c in y_order}
    for cx, cy in zip(x_order, y_order):
        to_x[cx].start()
        to_y[cy].start()
    to_mate = pltpu.make_async_remote_copy(src_ref=hid, dst_ref=land.at[1], send_sem=send.at[24], recv_sem=recv.at[24], device_id=dev(flip(me, 1)), device_id_type=MESH)
    to_mate.start()
    early = []
    for f in range(NF):
        cols = pl.ds(f * ft, ft)
        early += [
            pltpu.make_async_copy(w1.at[0, :, cols], w1p.at[f], wsem.at[f, 0]),
            pltpu.make_async_copy(w3.at[0, :, cols], w3p.at[f], wsem.at[f, 1]),
            pltpu.make_async_copy(w2.at[0, cols, :], w2p.at[f], wsem.at[f, 2]),
        ]
    for c in early:
        c.start()

    h = hid[...]
    w = wrt[...]
    w_hi = w.astype(BF16)
    rest = w - w_hi.astype(F32)
    w_mid = rest.astype(BF16)
    w_lo = (rest - w_mid.astype(F32)).astype(BF16)
    dot = functools.partial(lax.dot_general, dimension_numbers=NT, preferred_element_type=F32)
    logits = dot(h, w_hi) + (dot(h, w_mid) + dot(h, w_lo))
    ex = jnp.exp(logits - jnp.max(logits, axis=1, keepdims=True))
    prob = ex / jnp.sum(ex, axis=1, keepdims=True)
    ta, tb = iota((tokens, tokens), 0), iota((tokens, tokens), 1)
    eye = (ta == tb).astype(F32).astype(BF16)
    own_ids = ids[...].astype(F32)
    lane = iota((tokens, experts), 1).astype(F32)
    id_col = [dot(eye, jnp.broadcast_to(own_ids[k:k + 1], (8, tokens)).astype(BF16))[:, 0:1] for k in (0, 1)]
    pick = [(id_col[k] == lane).astype(F32) for k in (0, 1)]
    g = [jnp.sum(pick[k] * prob, axis=1, keepdims=True) for k in (0, 1)]
    total = g[0] + g[1]

    for c in id_copies:
        c.wait_recv()
    ids_all[0] = ids[...]
    most = None
    for q in range(owners):
        both = ids_all[q]
        e_col = iota((experts, tokens), 0)
        hot = ((both[0:1] == e_col) | (both[1:2] == e_col)).astype(F32).astype(BF16)
        count = dot(jnp.ones((8, tokens), BF16), hot)
        most = count if most is None else jnp.maximum(most, count)
    stride = jnp.floor((most + 15.0) * (1.0 / 16.0)) * 16.0
    ea, eb = iota((experts, experts), 0), iota((experts, experts), 1)
    same = ea // local == eb // local
    plain = functools.partial(jnp.dot, preferred_element_type=F32)
    offset = plain(stride.astype(BF16), (same & (ea < eb)).astype(F32).astype(BF16))
    need = jnp.max(plain(stride.astype(BF16), same.astype(F32).astype(BF16))).astype(I32)
    branch = jnp.int32(0)
    for limit in caps[:-1]:
        branch = branch + (need > limit).astype(I32)
    cap[0] = branch
    rank = plain((tb < ta).astype(F32).astype(BF16), (pick[0] + pick[1]).astype(BF16))
    place = rank + offset[0:1]
    slot = [jnp.sum(pick[k] * place, axis=1, keepdims=True) for k in (0, 1)]
    owner = [jnp.floor(id_col[k] * (1.0 / local)) for k in (0, 1)]
    wide = iota((tokens, 128), 1)
    table = jnp.zeros((tokens, 128), F32)
    for n, col in enumerate((g[0] / total, g[1] / total, owner[0], owner[1], slot[0], slot[1])):
        table = jnp.where(wide == n, col, table)
    tok[...] = table
    first, second = (jnp.concatenate([ids_all[q, k:k + 1] for q in range(owners)], axis=0) for k in (0, 1))
    marks = jnp.concatenate([((first == me * local + j) | (second == me * local + j)).astype(F32) for j in range(local)], axis=0)
    earlier = plain(marks.astype(BF16), (ta < tb).astype(F32).astype(BF16))
    pos[...] = jnp.where(marks > 0.5, earlier, -1.0)

    def pick_rows(q):
        at = iota((slots, tokens), 0).astype(F32)
        match = jnp.concatenate([(at == pos[j * owners + q:j * owners + q + 1, :]).astype(F32) for j in range(local)], axis=0).astype(BF16)

        @pl.loop(0, width // 512)
        def _(n):
            cols = pl.ds(pl.multiple_of(n * 512, 512), 512)
            block = hid[:, cols] if q == 0 else land[q, :, cols]
            part = jnp.dot(match, block, preferred_element_type=F32).astype(BF16)
            for j in range(local):
                rows_out[j, q, :, cols] = part[j * slots:(j + 1) * slots]

    sent = [*to_x.values(), *to_y.values(), to_mate]

    def pass_on(q, c, n, to):
        copy = remote(q, c, n, to)
        copy.start()
        sent.append(copy)
        return copy

    pick_rows(0)
    across, mates = {}, {2: [], 4: [], 6: []}
    for cx, cy in zip(x_order, y_order):
        to_x[cx].wait_recv()
        if cx in (0, 1):
            across[cx] = pass_on(2, cx, 8 + cx, 4)
        mates[2].append(pass_on(2, cx, 12 + cx, 1))
        to_y[cy].wait_recv()
        if cy in (2, 3):
            across[cy] = pass_on(4, cy, 8 + cy, 2)
        mates[4].append(pass_on(4, cy, 16 + cy, 1))
        if cx == 0:
            to_mate.wait_recv()
            pick_rows(1)
    for q in (2, 4):
        pick_rows(q)
    for q in (2, 4):
        for m in mates[q]:
            m.wait_recv()
        pick_rows(q + 1)
    for c in (0, 2, 1, 3):
        across[c].wait_recv()
        mates[6].append(pass_on(6, c, 20 + c, 1))
    pick_rows(6)
    for m in mates[6]:
        m.wait_recv()
    pick_rows(7)
    for m in sent:
        m.wait_send()
    for c in id_copies:
        c.wait_send()
    for c in early:
        c.wait()


def gather_call(hidden, ids_t, wr_t, w1, w3, w2, owners, caps):
    tokens, width = hidden.shape
    experts = wr_t.shape[0]
    local, _, ffn = w1.shape
    slots = caps[-1] // local
    ft = ffn // NF
    vmem = pl.BlockSpec(memory_space=pltpu.VMEM)
    hbm = pl.BlockSpec(memory_space=pl.ANY)
    return pl.pallas_call(
        functools.partial(gather_kernel, caps),
        name='gather_tokens',
        out_shape=(
            pltpu.VMEM((local, owners, slots, width), BF16),
            jax.ShapeDtypeStruct((local * owners, tokens), F32),
            jax.ShapeDtypeStruct((tokens, 128), F32),
            jax.ShapeDtypeStruct((1,), I32),
            pltpu.VMEM((NF, width, ft), BF16),
            pltpu.VMEM((NF, width, ft), BF16),
            pltpu.VMEM((NF, ft, width), BF16),
        ),
        in_specs=[vmem, vmem, vmem, hbm, hbm, hbm],
        out_specs=(vmem, vmem, vmem, pl.BlockSpec(memory_space=pltpu.SMEM), vmem, vmem, vmem),
        scratch_shapes=[
            pltpu.VMEM((owners, tokens, width), BF16),
            pltpu.VMEM((owners, 2, tokens), I32),
            pltpu.SemaphoreType.DMA((25,)),
            pltpu.SemaphoreType.DMA((25,)),
            pltpu.SemaphoreType.DMA((owners,)),
            pltpu.SemaphoreType.DMA((owners,)),
            pltpu.SemaphoreType.DMA((NF, 3)),
        ],
        compiler_params=pltpu.CompilerParams(collective_id=0, has_side_effects=True, vmem_limit_bytes=20 * 1024 * 1024),
    )(hidden, ids_t, wr_t, w1, w3, w2)


def expert_kernel(caps, branch, pos, rows, w1p, w3p, w2p, w1, w3, w2, ret, w1b, w3b, w2b, mid, yacc, plan, wsem):
    local, owners, slots, width = rows.shape
    ft = w1b.shape[2]
    steps = (local - 1) * NF

    unit = []
    for j in range(local):
        most = jnp.max(pos[pl.ds(j * owners, owners), :]).astype(I32) + 1
        unit.append((most + 15) // 16)
    for j in range(local):
        rank = jnp.int32(min(j, 1))
        offset = jnp.int32(0)
        for i in range(local):
            if i > 0 and j > 0 and i != j:
                ahead = (unit[i] >= unit[j]) if i < j else (unit[i] > unit[j])
                rank = rank + ahead.astype(I32)
            if i < j:
                offset = offset + unit[i]
        plan[0, rank] = jnp.int32(j)
        plan[1, rank] = unit[j]
        plan[2, rank] = offset
    used = unit[0]
    for j in range(1, local):
        used = used + unit[j]

    def weights(t):
        e = plan[0, 1 + t // NF]
        cols = pl.ds(pl.multiple_of((t % NF) * ft, ft), ft)
        n = t % RING
        return (
            pltpu.make_async_copy(w1.at[e, :, cols], w1b.at[n], wsem.at[n, 0]),
            pltpu.make_async_copy(w3.at[e, :, cols], w3b.at[n], wsem.at[n, 1]),
            pltpu.make_async_copy(w2.at[e, cols, :], w2b.at[n], wsem.at[n, 2]),
        )

    for t in range(RING):
        for c in weights(jnp.int32(t)):
            c.start()

    limit = jnp.int32(caps[0])
    for n in range(1, len(caps)):
        limit = jnp.where(branch[0] >= n, caps[n], limit)

    @pl.loop(used, limit // 16)
    def _(n):
        blank = pl.ds(pl.multiple_of(n * 16, 16), 16)
        for q in range(owners):
            ret[q, blank, :] = jnp.zeros((16, width), BF16)

    def step(r, f, gate_w, up_w, down_w):
        e = plan[0, r]
        for units in range(1, slots // 16 + 1):
            m = 16 * units * owners

            @pl.when(plan[1, r] == units)
            def _():
                @pl.loop(0, ft // 256)
                def _(i):
                    cols = pl.ds(pl.multiple_of(i * 256, 256), 256)
                    x = rows[e, :, 0:16 * units, :].reshape(m, width)
                    gate = jnp.dot(x, gate_w[:, cols], preferred_element_type=F32)
                    up = jnp.dot(x, up_w[:, cols], preferred_element_type=F32)
                    mid[0:m, cols] = (gate * jax.nn.sigmoid(gate) * up).astype(BF16)

                @pl.loop(0, width // 512)
                def _(i):
                    cols = pl.ds(pl.multiple_of(i * 512, 512), 512)
                    part = jnp.dot(mid[0:m, :], down_w[:, cols], preferred_element_type=F32)
                    yacc[0:m, cols] = jnp.where(f == 0, 0.0, yacc[0:m, cols]) + part

                @pl.when(f == NF - 1)
                def _():
                    first = pl.multiple_of(plan[2, r] * 16, 16)
                    for q in range(owners):
                        ret[q, pl.ds(first, 16 * units), :] = yacc[q * 16 * units:(q + 1) * 16 * units, :].astype(BF16)

    @pl.loop(0, NF)
    def _(f):
        step(0, f, w1p.at[f], w3p.at[f], w2p.at[f])

    @pl.loop(0, steps)
    def _(t):
        n = t % RING
        for c in weights(t):
            c.wait()
        step(1 + t // NF, t % NF, w1b.at[n], w3b.at[n], w2b.at[n])

        @pl.when(t + RING < steps)
        def _():
            for c in weights(t + RING):
                c.start()


def expert_call(branch, pos, rows, w1p, w3p, w2p, w1, w3, w2, caps):
    local, owners, slots, width = rows.shape
    ft = w1p.shape[2]
    hbm = pl.BlockSpec(memory_space=pl.ANY)
    vmem = pl.BlockSpec(memory_space=pltpu.VMEM)
    flops = 3 * 2 * local * slots * owners * width * ft * NF // 2
    return pl.pallas_call(
        functools.partial(expert_kernel, caps),
        name='experts',
        out_shape=pltpu.VMEM((owners, caps[-1], width), BF16),
        in_specs=[pl.BlockSpec(memory_space=pltpu.SMEM), vmem, vmem, vmem, vmem, vmem, hbm, hbm, hbm],
        out_specs=vmem,
        scratch_shapes=[
            pltpu.VMEM((RING, width, ft), BF16),
            pltpu.VMEM((RING, width, ft), BF16),
            pltpu.VMEM((RING, ft, width), BF16),
            pltpu.VMEM((owners * slots, ft), BF16),
            pltpu.VMEM((owners * slots, width), F32),
            pltpu.SMEM((3, local), I32),
            pltpu.SemaphoreType.DMA((RING, 3)),
        ],
        compiler_params=pltpu.CompilerParams(vmem_limit_bytes=20 * 1024 * 1024),
        cost_estimate=pl.CostEstimate(flops=flops, bytes_accessed=3 * 2 * local * width * ft * NF, transcendentals=0),
    )(branch, pos, rows, w1p, w3p, w2p, w1, w3, w2)


ORDER = (0, 1, 2, 4, 6, 3, 5, 7)


def return_kernel(cap, ret, tok, hid, scale, out, got, acc, send, recv):
    me = lax.axis_index('ep')
    owners = ret.shape[0]
    tokens, width = hid.shape
    barrier = pltpu.get_barrier_semaphore()
    for q in range(1, owners):
        pl.semaphore_signal(barrier, inc=1, device_id=dev(flip(me, q)), device_id_type=MESH)
    pl.semaphore_wait(barrier, owners - 1)
    copies = {}
    for q in ORDER[2:] + (1,):
        copies[q] = pltpu.make_async_remote_copy(src_ref=ret.at[q, pl.ds(0, cap)], dst_ref=got.at[q], send_sem=send.at[q], recv_sem=recv.at[q], device_id=dev(flip(me, q)), device_id_type=MESH)
        copies[q].start()
    table = tok[...]
    lane = iota((tokens, cap), 1).astype(F32)
    for q in ORDER:
        if q != 0:
            copies[q].wait_recv()
        peer = flip(me, q).astype(F32)
        hot = jnp.concatenate([((table[:, 2 + k:3 + k] == peer) & (table[:, 4 + k:5 + k] == lane)).astype(F32) for k in (0, 1)], axis=0).astype(BF16)

        @pl.loop(0, width // 256)
        def _(n):
            cols = pl.ds(pl.multiple_of(n * 256, 256), 256)
            block = ret[0, 0:cap, cols] if q == 0 else got[q, :, cols]
            part = jnp.dot(hot, block, preferred_element_type=F32)
            acc[:, cols] = part if q == 0 else acc[:, cols] + part

    mixed = table[:, 0:1] * acc[0:tokens] + table[:, 1:2] * acc[tokens:2 * tokens]
    out[...] = (scale[0] * hid[...].astype(F32) + scale[1] * mixed).astype(BF16)
    for q in copies:
        copies[q].wait_send()


def return_call(n, cap, ret, tok, hidden, scale):
    owners, _, width = ret.shape
    tokens = hidden.shape[0]
    vmem = pl.BlockSpec(memory_space=pltpu.VMEM)
    return pl.pallas_call(
        functools.partial(return_kernel, cap),
        name=f'return_{cap}',
        out_shape=jax.ShapeDtypeStruct((tokens, width), BF16),
        in_specs=[vmem, vmem, vmem, pl.BlockSpec(memory_space=pltpu.SMEM)],
        out_specs=vmem,
        scratch_shapes=[
            pltpu.VMEM((owners, cap, width), BF16),
            pltpu.VMEM((2 * tokens, width), F32),
            pltpu.SemaphoreType.DMA((owners,)),
            pltpu.SemaphoreType.DMA((owners,)),
        ],
        compiler_params=pltpu.CompilerParams(collective_id=1 + n, has_side_effects=True, vmem_limit_bytes=24 * 1024 * 1024),
    )(ret, tok, hidden, scale)


def capacities(local, slots):
    full = [slots * n + 16 * (local - n) for n in range(1, local + 1)]
    return tuple(sorted({full[0] + 16, *full}))


def solution(mesh):
    owners = mesh.shape['ep']

    def local_step(hidden, router_w, expert_ids, w_gate, w_up, w_down, post_scale):
        tokens = hidden.shape[0]
        local = w_gate.shape[0]
        slots = tokens // max(1, local * owners // 8)
        caps = capacities(local, slots)
        rows, pos, tok, branch, w1p, w3p, w2p = gather_call(hidden, expert_ids.T, router_w.T, w_gate, w_up, w_down, owners, caps)
        ret = expert_call(branch, pos, rows, w1p, w3p, w2p, w_gate, w_up, w_down, caps)
        branches = [functools.partial(return_call, n, cap) for n, cap in enumerate(caps)]
        return lax.switch(branch[0], branches, ret, tok, hidden, post_scale)

    tok_spec = P(('dp', 'ep'))
    return jax.shard_map(local_step, mesh=mesh, in_specs=(tok_spec, P(), tok_spec, P('ep'), P('ep'), P('ep'), P()), out_specs=tok_spec, check_vma=False)
```

```python
import functools

import jax
import jax.numpy as jnp
from jax import lax
from jax.experimental import pallas as pl
from jax.experimental.pallas import tpu as pltpu
from jax.sharding import PartitionSpec as P

MESH = pl.DeviceIdType.MESH
F32, BF16, I32 = jnp.float32, jnp.bfloat16, jnp.int32
NT = (((1,), (1,)), ((), ()))


def flip(idx, mask):
    out = idx
    for bit in (1, 2, 4):
        if mask & bit:
            out = out + bit - 2 * bit * ((idx // bit) % 2)
    return out


def dev(idx):
    return (lax.axis_index('dp'), idx)


def iota(shape, dim):
    return lax.broadcasted_iota(I32, shape, dim)


CHUNKS = 4
NF = 3
RING = 4


def gather_kernel(caps, hid, ids, wrt, w1, w3, w2, rows_out, pos, tok, cap, w1p, w3p, w2p, land, ids_all, send, recv, id_send, id_recv, wsem):
    me = lax.axis_index('ep')
    tokens, width = hid.shape
    experts = wrt.shape[0]
    local, owners, slots, _ = rows_out.shape
    ft = w1p.shape[2]
    rows = tokens // CHUNKS
    barrier = pltpu.get_barrier_semaphore()
    for q in range(1, owners):
        pl.semaphore_signal(barrier, inc=1, device_id=dev(flip(me, q)), device_id_type=MESH)
    pl.semaphore_wait(barrier, owners - 1)

    def piece(q, c):
        return (hid if q == 0 else land.at[q]).at[pl.ds(c * rows, rows)]

    def remote(q, c, n, to):
        return pltpu.make_async_remote_copy(src_ref=piece(q, c), dst_ref=land.at[q ^ to, pl.ds(c * rows, rows)], send_sem=send.at[n], recv_sem=recv.at[n], device_id=dev(flip(me, to)), device_id_type=MESH)

    id_copies = []
    for q in range(1, owners):
        id_copies.append(pltpu.make_async_remote_copy(src_ref=ids, dst_ref=ids_all.at[q], send_sem=id_send.at[q], recv_sem=id_recv.at[q], device_id=dev(flip(me, q)), device_id_type=MESH))
    for c in id_copies:
        c.start()
    x_order, y_order = (0, 1, 2, 3), (2, 3, 0, 1)
    to_x = {c: remote(0, c, c, 2) for c in x_order}
    to_y = {c: remote(0, c, 4 + c, 4) for c in y_order}
    for cx, cy in zip(x_order, y_order):
        to_x[cx].start()
        to_y[cy].start()
    to_mate = pltpu.make_async_remote_copy(src_ref=hid, dst_ref=land.at[1], send_sem=send.at[24], recv_sem=recv.at[24], device_id=dev(flip(me, 1)), device_id_type=MESH)
    to_mate.start()
    early = []
    for t in range(RING):
        e, cols = t // NF, pl.ds(t % NF * ft, ft)
        early += [
            pltpu.make_async_copy(w1.at[e, :, cols], w1p.at[t], wsem.at[t, 0]),
            pltpu.make_async_copy(w3.at[e, :, cols], w3p.at[t], wsem.at[t, 1]),
            pltpu.make_async_copy(w2.at[e, cols, :], w2p.at[t], wsem.at[t, 2]),
        ]
    for c in early:
        c.start()

    h = hid[...]
    w = wrt[...]
    w_hi = w.astype(BF16)
    rest = w - w_hi.astype(F32)
    w_mid = rest.astype(BF16)
    w_lo = (rest - w_mid.astype(F32)).astype(BF16)
    dot = functools.partial(lax.dot_general, dimension_numbers=NT, preferred_element_type=F32)
    logits = dot(h, w_hi) + (dot(h, w_mid) + dot(h, w_lo))
    ex = jnp.exp(logits - jnp.max(logits, axis=1, keepdims=True))
    prob = ex / jnp.sum(ex, axis=1, keepdims=True)
    ta, tb = iota((tokens, tokens), 0), iota((tokens, tokens), 1)
    eye = (ta == tb).astype(F32).astype(BF16)
    own_ids = ids[...].astype(F32)
    lane = iota((tokens, experts), 1).astype(F32)
    id_col = [dot(eye, jnp.broadcast_to(own_ids[k:k + 1], (8, tokens)).astype(BF16))[:, 0:1] for k in (0, 1)]
    pick = [(id_col[k] == lane).astype(F32) for k in (0, 1)]
    g = [jnp.sum(pick[k] * prob, axis=1, keepdims=True) for k in (0, 1)]
    total = g[0] + g[1]

    for c in id_copies:
        c.wait_recv()
    ids_all[0] = ids[...]
    most = None
    for q in range(owners):
        both = ids_all[q]
        e_col = iota((experts, tokens), 0)
        hot = ((both[0:1] == e_col) | (both[1:2] == e_col)).astype(F32).astype(BF16)
        count = dot(jnp.ones((8, tokens), BF16), hot)
        most = count if most is None else jnp.maximum(most, count)
    stride = jnp.where(most > 32.0, float(slots), jnp.where(most > 16.0, 32.0, 16.0))
    ea, eb = iota((experts, experts), 0), iota((experts, experts), 1)
    same = ea // local == eb // local
    plain = functools.partial(jnp.dot, preferred_element_type=F32)
    offset = plain(stride.astype(BF16), (same & (ea < eb)).astype(F32).astype(BF16))
    need = jnp.max(plain(stride.astype(BF16), same.astype(F32).astype(BF16))).astype(I32)
    branch = jnp.int32(0)
    for limit in caps[:-1]:
        branch = branch + (need > limit).astype(I32)
    cap[0] = branch
    rank = plain((tb < ta).astype(F32).astype(BF16), (pick[0] + pick[1]).astype(BF16))
    place = rank + offset[0:1]
    slot = [jnp.sum(pick[k] * place, axis=1, keepdims=True) for k in (0, 1)]
    owner = [jnp.floor(id_col[k] * (1.0 / local)) for k in (0, 1)]
    wide = iota((tokens, 128), 1)
    table = jnp.zeros((tokens, 128), F32)
    for n, col in enumerate((g[0] / total, g[1] / total, owner[0], owner[1], slot[0], slot[1])):
        table = jnp.where(wide == n, col, table)
    tok[...] = table
    first, second = (jnp.concatenate([ids_all[q, k:k + 1] for q in range(owners)], axis=0) for k in (0, 1))
    marks = jnp.concatenate([((first == me * local + j) | (second == me * local + j)).astype(F32) for j in range(local)], axis=0)
    earlier = plain(marks.astype(BF16), (ta < tb).astype(F32).astype(BF16))
    pos[...] = jnp.where(marks > 0.5, earlier, -1.0)

    def pick_rows(q):
        at = iota((slots, tokens), 0).astype(F32)
        match = jnp.concatenate([(at == pos[j * owners + q:j * owners + q + 1, :]).astype(F32) for j in range(local)], axis=0).astype(BF16)

        @pl.loop(0, width // 512)
        def _(n):
            cols = pl.ds(pl.multiple_of(n * 512, 512), 512)
            block = hid[:, cols] if q == 0 else land[q, :, cols]
            part = jnp.dot(match, block, preferred_element_type=F32).astype(BF16)
            for j in range(local):
                rows_out[j, q, :, cols] = part[j * slots:(j + 1) * slots]

    sent = [*to_x.values(), *to_y.values(), to_mate]

    def pass_on(q, c, n, to):
        copy = remote(q, c, n, to)
        copy.start()
        sent.append(copy)
        return copy

    pick_rows(0)
    across, mates = {}, {2: [], 4: [], 6: []}
    for cx, cy in zip(x_order, y_order):
        to_x[cx].wait_recv()
        if cx in (0, 1):
            across[cx] = pass_on(2, cx, 8 + cx, 4)
        mates[2].append(pass_on(2, cx, 12 + cx, 1))
        to_y[cy].wait_recv()
        if cy in (2, 3):
            across[cy] = pass_on(4, cy, 8 + cy, 2)
        mates[4].append(pass_on(4, cy, 16 + cy, 1))
        if cx == 0:
            to_mate.wait_recv()
            pick_rows(1)
    for q in (2, 4):
        pick_rows(q)
    for q in (2, 4):
        for m in mates[q]:
            m.wait_recv()
        pick_rows(q + 1)
    for c in (0, 2, 1, 3):
        across[c].wait_recv()
        mates[6].append(pass_on(6, c, 20 + c, 1))
    pick_rows(6)
    for m in mates[6]:
        m.wait_recv()
    pick_rows(7)
    for m in sent:
        m.wait_send()
    for c in id_copies:
        c.wait_send()
    for c in early:
        c.wait()


def gather_call(hidden, ids_t, wr_t, w1, w3, w2, owners, caps):
    tokens, width = hidden.shape
    experts = wr_t.shape[0]
    local, _, ffn = w1.shape
    slots = caps[-1] // local
    ft = ffn // NF
    vmem = pl.BlockSpec(memory_space=pltpu.VMEM)
    hbm = pl.BlockSpec(memory_space=pl.ANY)
    return pl.pallas_call(
        functools.partial(gather_kernel, caps),
        name='gather_tokens',
        out_shape=(
            pltpu.VMEM((local, owners, slots, width), BF16),
            jax.ShapeDtypeStruct((local * owners, tokens), F32),
            jax.ShapeDtypeStruct((tokens, 128), F32),
            jax.ShapeDtypeStruct((1,), I32),
            pltpu.VMEM((RING, width, ft), BF16),
            pltpu.VMEM((RING, width, ft), BF16),
            pltpu.VMEM((RING, ft, width), BF16),
        ),
        in_specs=[vmem, vmem, vmem, hbm, hbm, hbm],
        out_specs=(vmem, vmem, vmem, pl.BlockSpec(memory_space=pltpu.SMEM), vmem, vmem, vmem),
        scratch_shapes=[
            pltpu.VMEM((owners, tokens, width), BF16),
            pltpu.VMEM((owners, 2, tokens), I32),
            pltpu.SemaphoreType.DMA((25,)),
            pltpu.SemaphoreType.DMA((25,)),
            pltpu.SemaphoreType.DMA((owners,)),
            pltpu.SemaphoreType.DMA((owners,)),
            pltpu.SemaphoreType.DMA((RING, 3)),
        ],
        compiler_params=pltpu.CompilerParams(collective_id=0, has_side_effects=True, vmem_limit_bytes=11 * 1024 * 1024),
    )(hidden, ids_t, wr_t, w1, w3, w2)


def expert_kernel(caps, branch, pos, rows, _w1b, _w3b, _w2b, w1, w3, w2, ret, w1b, w3b, w2b, mid, yacc, plan, wsem):
    local, owners, slots, width = rows.shape
    ft = w1b.shape[2]
    steps = local * NF
    fixed = (RING + NF - 1) // NF

    size = []
    for j in range(local):
        most = jnp.max(pos[pl.ds(j * owners, owners), :]).astype(I32) + 1
        size.append(jnp.where(most > 32, slots, jnp.where(most > 16, 32, 16)))
    for j in range(local):
        rank = jnp.int32(min(j, fixed))
        offset = jnp.int32(0)
        for i in range(local):
            if i >= fixed and j >= fixed and i != j:
                ahead = (size[i] >= size[j]) if i < j else (size[i] > size[j])
                rank = rank + ahead.astype(I32)
            if i < j:
                offset = offset + size[i]
        plan[0, rank] = jnp.int32(j)
        plan[1, rank] = size[j]
        plan[2, rank] = offset
    used = size[0]
    for j in range(1, local):
        used = used + size[j]

    def weights(t):
        e = plan[0, t // NF]
        cols = pl.ds(pl.multiple_of((t % NF) * ft, ft), ft)
        n = t % RING
        return (
            pltpu.make_async_copy(w1.at[e, :, cols], w1b.at[n], wsem.at[n, 0]),
            pltpu.make_async_copy(w3.at[e, :, cols], w3b.at[n], wsem.at[n, 1]),
            pltpu.make_async_copy(w2.at[e, cols, :], w2b.at[n], wsem.at[n, 2]),
        )

    limit = jnp.int32(caps[0])
    for n in range(1, len(caps)):
        limit = jnp.where(branch[0] >= n, caps[n], limit)

    @pl.loop(used // 16, limit // 16)
    def _(n):
        blank = pl.ds(pl.multiple_of(n * 16, 16), 16)
        for q in range(owners):
            ret[q, blank, :] = jnp.zeros((16, width), BF16)

    @pl.loop(0, steps)
    def _(t):
        r, f, n = t // NF, t % NF, t % RING
        e = plan[0, r]

        @pl.when(t >= RING)
        def _():
            for c in weights(t):
                c.wait()

        for size in (16, 32, slots):
            m = size * owners

            @pl.when(plan[1, r] == size)
            def _():
                x = rows[e, :, 0:size, :].reshape(m, width)
                for c in range(0, ft, 256):
                    gate = jnp.dot(x, w1b[n, :, c:c + 256], preferred_element_type=F32)
                    up = jnp.dot(x, w3b[n, :, c:c + 256], preferred_element_type=F32)
                    mid[0:m, c:c + 256] = (gate * jax.nn.sigmoid(gate) * up).astype(BF16)
                for c in range(0, width, 512):
                    part = jnp.dot(mid[0:m, :], w2b[n, :, c:c + 512], preferred_element_type=F32)
                    yacc[0:m, c:c + 512] = jnp.where(f == 0, 0.0, yacc[0:m, c:c + 512]) + part

                @pl.when(f == NF - 1)
                def _():
                    first = pl.multiple_of(plan[2, r], 16)
                    for q in range(owners):
                        ret[q, pl.ds(first, size), :] = yacc[q * size:(q + 1) * size, :].astype(BF16)

        @pl.when(t + RING < steps)
        def _():
            for c in weights(t + RING):
                c.start()


def expert_call(branch, pos, rows, w1p, w3p, w2p, w1, w3, w2, caps):
    local, owners, slots, width = rows.shape
    ft = w1p.shape[2]
    hbm = pl.BlockSpec(memory_space=pl.ANY)
    vmem = pl.BlockSpec(memory_space=pltpu.VMEM)
    flops = 3 * 2 * local * slots * owners * width * ft * NF // 2
    return pl.pallas_call(
        functools.partial(expert_kernel, caps),
        name='experts',
        out_shape=(
            pltpu.VMEM((owners, caps[-1], width), BF16),
            pltpu.VMEM(w1p.shape, BF16),
            pltpu.VMEM(w3p.shape, BF16),
            pltpu.VMEM(w2p.shape, BF16),
        ),
        in_specs=[pl.BlockSpec(memory_space=pltpu.SMEM), vmem, vmem, vmem, vmem, vmem, hbm, hbm, hbm],
        out_specs=(vmem, vmem, vmem, vmem),
        input_output_aliases={3: 1, 4: 2, 5: 3},
        scratch_shapes=[
            pltpu.VMEM((owners * slots, ft), BF16),
            pltpu.VMEM((owners * slots, width), F32),
            pltpu.SMEM((3, local), I32),
            pltpu.SemaphoreType.DMA((RING, 3)),
        ],
        compiler_params=pltpu.CompilerParams(vmem_limit_bytes=12 * 1024 * 1024),
        cost_estimate=pl.CostEstimate(flops=flops, bytes_accessed=3 * 2 * local * width * ft * NF, transcendentals=0),
    )(branch, pos, rows, w1p, w3p, w2p, w1, w3, w2)[0]


ORDER = (0, 1, 2, 4, 6, 3, 5, 7)


def return_kernel(cap, ret, tok, hid, scale, out, got, acc, send, recv):
    me = lax.axis_index('ep')
    owners = ret.shape[0]
    tokens, width = hid.shape
    barrier = pltpu.get_barrier_semaphore()
    for q in range(1, owners):
        pl.semaphore_signal(barrier, inc=1, device_id=dev(flip(me, q)), device_id_type=MESH)
    pl.semaphore_wait(barrier, owners - 1)
    copies = {}
    for q in ORDER[2:] + (1,):
        copies[q] = pltpu.make_async_remote_copy(src_ref=ret.at[q, pl.ds(0, cap)], dst_ref=got.at[q], send_sem=send.at[q], recv_sem=recv.at[q], device_id=dev(flip(me, q)), device_id_type=MESH)
        copies[q].start()
    table = tok[...]
    lane = iota((tokens, cap), 1).astype(F32)
    for q in ORDER:
        if q != 0:
            copies[q].wait_recv()
        peer = flip(me, q).astype(F32)
        hot = jnp.concatenate([((table[:, 2 + k:3 + k] == peer) & (table[:, 4 + k:5 + k] == lane)).astype(F32) for k in (0, 1)], axis=0).astype(BF16)

        @pl.loop(0, width // 256)
        def _(n):
            cols = pl.ds(pl.multiple_of(n * 256, 256), 256)
            block = ret[0, 0:cap, cols] if q == 0 else got[q, :, cols]
            part = jnp.dot(hot, block, preferred_element_type=F32)
            acc[:, cols] = part if q == 0 else acc[:, cols] + part

    mixed = table[:, 0:1] * acc[0:tokens] + table[:, 1:2] * acc[tokens:2 * tokens]
    out[...] = (scale[0] * hid[...].astype(F32) + scale[1] * mixed).astype(BF16)
    for q in copies:
        copies[q].wait_send()


def return_call(n, cap, ret, tok, hidden, scale):
    owners, _, width = ret.shape
    tokens = hidden.shape[0]
    vmem = pl.BlockSpec(memory_space=pltpu.VMEM)
    return pl.pallas_call(
        functools.partial(return_kernel, cap),
        name=f'return_{cap}',
        out_shape=jax.ShapeDtypeStruct((tokens, width), BF16),
        in_specs=[vmem, vmem, vmem, pl.BlockSpec(memory_space=pltpu.SMEM)],
        out_specs=vmem,
        scratch_shapes=[
            pltpu.VMEM((owners, cap, width), BF16),
            pltpu.VMEM((2 * tokens, width), F32),
            pltpu.SemaphoreType.DMA((owners,)),
            pltpu.SemaphoreType.DMA((owners,)),
        ],
        compiler_params=pltpu.CompilerParams(collective_id=1 + n, has_side_effects=True, vmem_limit_bytes=14 * 1024 * 1024),
    )(ret, tok, hidden, scale)


def capacities(local, slots):
    full = [slots * n + 16 * (local - n) for n in range(1, local + 1)]
    return tuple(sorted({full[0] + 16, *full}))


def solution(mesh):
    owners = mesh.shape['ep']

    def local_step(hidden, router_w, expert_ids, w_gate, w_up, w_down, post_scale):
        tokens = hidden.shape[0]
        local = w_gate.shape[0]
        slots = tokens // max(1, local * owners // 8)
        caps = capacities(local, slots)
        rows, pos, tok, branch, w1p, w3p, w2p = gather_call(hidden, expert_ids.T, router_w.T, w_gate, w_up, w_down, owners, caps)
        ret = expert_call(branch, pos, rows, w1p, w3p, w2p, w_gate, w_up, w_down, caps)
        branches = [functools.partial(return_call, n, cap) for n, cap in enumerate(caps)]
        return lax.switch(branch[0], branches, ret, tok, hidden, post_scale)

    tok_spec = P(('dp', 'ep'))
    return jax.shard_map(local_step, mesh=mesh, in_specs=(tok_spec, P(), tok_spec, P('ep'), P('ep'), P('ep'), P()), out_specs=tok_spec, check_vma=False)
```

```python
import functools

import jax
import jax.numpy as jnp
from jax import lax
from jax.experimental import pallas as pl
from jax.experimental.pallas import tpu as pltpu
from jax.sharding import PartitionSpec as P

MESH = pl.DeviceIdType.MESH
F32, BF16, I32 = jnp.float32, jnp.bfloat16, jnp.int32
NT = (((1,), (1,)), ((), ()))


def flip(idx, mask):
    out = idx
    for bit in (1, 2, 4):
        if mask & bit:
            out = out + bit - 2 * bit * ((idx // bit) % 2)
    return out


def dev(idx):
    return (lax.axis_index('dp'), idx)


def iota(shape, dim):
    return lax.broadcasted_iota(I32, shape, dim)


CHUNKS = 4
NF = 3
RING = 4


def gather_kernel(caps, hid, ids, wrt, w1, w3, w2, rows_out, pos, tok, goal, cap, w1p, w3p, w2p, land, ids_all, send, recv, id_send, id_recv, wsem):
    me = lax.axis_index('ep')
    tokens, width = hid.shape
    experts = wrt.shape[0]
    local, owners, slots, _ = rows_out.shape
    ft = w1p.shape[2]
    rows = tokens // CHUNKS
    barrier = pltpu.get_barrier_semaphore()
    for q in range(1, owners):
        pl.semaphore_signal(barrier, inc=1, device_id=dev(flip(me, q)), device_id_type=MESH)
    pl.semaphore_wait(barrier, owners - 1)

    def piece(q, c):
        return (hid if q == 0 else land.at[q]).at[pl.ds(c * rows, rows)]

    def remote(q, c, n, to):
        return pltpu.make_async_remote_copy(src_ref=piece(q, c), dst_ref=land.at[q ^ to, pl.ds(c * rows, rows)], send_sem=send.at[n], recv_sem=recv.at[n], device_id=dev(flip(me, to)), device_id_type=MESH)

    id_copies = []
    for q in range(1, owners):
        id_copies.append(pltpu.make_async_remote_copy(src_ref=ids, dst_ref=ids_all.at[q], send_sem=id_send.at[q], recv_sem=id_recv.at[q], device_id=dev(flip(me, q)), device_id_type=MESH))
    for c in id_copies:
        c.start()
    x_order, y_order = (0, 1, 2, 3), (2, 3, 0, 1)
    to_x = {c: remote(0, c, c, 2) for c in x_order}
    to_y = {c: remote(0, c, 4 + c, 4) for c in y_order}
    for cx, cy in zip(x_order, y_order):
        to_x[cx].start()
        to_y[cy].start()
    to_mate = pltpu.make_async_remote_copy(src_ref=hid, dst_ref=land.at[1], send_sem=send.at[24], recv_sem=recv.at[24], device_id=dev(flip(me, 1)), device_id_type=MESH)
    to_mate.start()
    early = []
    for t in range(RING):
        e, cols = t // NF, pl.ds(t % NF * ft, ft)
        early += [
            pltpu.make_async_copy(w1.at[e, :, cols], w1p.at[t], wsem.at[t, 0]),
            pltpu.make_async_copy(w3.at[e, :, cols], w3p.at[t], wsem.at[t, 1]),
            pltpu.make_async_copy(w2.at[e, cols, :], w2p.at[t], wsem.at[t, 2]),
        ]
    for c in early:
        c.start()

    h = hid[...]
    w = wrt[...]
    w_hi = w.astype(BF16)
    rest = w - w_hi.astype(F32)
    w_mid = rest.astype(BF16)
    w_lo = (rest - w_mid.astype(F32)).astype(BF16)
    dot = functools.partial(lax.dot_general, dimension_numbers=NT, preferred_element_type=F32)
    logits = dot(h, w_hi) + (dot(h, w_mid) + dot(h, w_lo))
    ex = jnp.exp(logits - jnp.max(logits, axis=1, keepdims=True))
    prob = ex / jnp.sum(ex, axis=1, keepdims=True)
    ta, tb = iota((tokens, tokens), 0), iota((tokens, tokens), 1)
    eye = (ta == tb).astype(F32).astype(BF16)
    own_ids = ids[...].astype(F32)
    lane = iota((tokens, experts), 1).astype(F32)
    id_col = [dot(eye, jnp.broadcast_to(own_ids[k:k + 1], (8, tokens)).astype(BF16))[:, 0:1] for k in (0, 1)]
    pick = [(id_col[k] == lane).astype(F32) for k in (0, 1)]
    g = [jnp.sum(pick[k] * prob, axis=1, keepdims=True) for k in (0, 1)]
    total = g[0] + g[1]

    for c in id_copies:
        c.wait_recv()
    ids_all[0] = ids[...]
    counts = []
    for q in range(owners):
        both = ids_all[q]
        e_col = iota((experts, tokens), 0)
        hot = ((both[0:1] == e_col) | (both[1:2] == e_col)).astype(F32).astype(BF16)
        counts.append(dot(jnp.ones((8, tokens), BF16), hot))
    most = functools.reduce(jnp.maximum, counts)
    count = jnp.concatenate([c[0:1] for c in counts], axis=0)
    stride = jnp.where(most > 32.0, float(slots), jnp.where(most > 16.0, 32.0, 16.0))
    mark = lambda mask: mask.astype(F32).astype(BF16)
    plain = functools.partial(jnp.dot, preferred_element_type=F32)
    ea, eb = iota((experts, experts), 0), iota((experts, experts), 1)
    same, same_chip = ea // local == eb // local, ea // (2 * local) == eb // (2 * local)
    offset = plain(stride.astype(BF16), mark(same & (ea < eb)))
    need = jnp.max(plain(stride.astype(BF16), mark(same))).astype(I32)
    need_chip = jnp.max(plain(count.astype(BF16), mark(same_chip))).astype(I32)
    branch = jnp.int32(0)
    for limit, limit_chip in caps[:-1]:
        branch = branch + ((need > limit) | (need_chip > limit_chip)).astype(I32)
    cap[0] = branch
    rank = plain(mark(tb < ta), (pick[0] + pick[1]).astype(BF16))
    chip_first = plain(count.astype(BF16), mark(same_chip & (ea < eb)))[0:1]
    slot = [jnp.sum(pick[k] * (rank + offset[0:1]), axis=1, keepdims=True) for k in (0, 1)]
    packed = [jnp.sum(pick[k] * (rank + chip_first), axis=1, keepdims=True) for k in (0, 1)]
    owner = [jnp.floor(id_col[k] * (1.0 / local)) for k in (0, 1)]
    wide = iota((tokens, 128), 1)
    table = jnp.zeros((tokens, 128), F32)
    for n, col in enumerate((g[0] / total, g[1] / total, *owner, *slot, *packed)):
        table = jnp.where(wide == n, col, table)
    tok[...] = table

    e_row, n_col = iota((experts, 128), 0), iota((experts, 128), 1)
    e_of = jnp.where(n_col < local, me * local + n_col, flip(me, 1) * local + n_col - local)
    used = n_col < 2 * local
    held = plain(count.astype(BF16), mark(used & (e_row == e_of)))
    start = plain(count.astype(BF16), mark(used & (e_row // (2 * local) == me // 2) & (e_row < e_of)))
    base = plain(stride.astype(BF16), mark(used & (e_row // local == e_of // local) & (e_row < e_of)))
    lane_of = iota((owners, goal.shape[1]), 1)
    where_to = jnp.full((owners, goal.shape[1]), -1.0, F32)
    for n in range(2 * local):
        at = (lane_of - (n // local) * (goal.shape[1] // 2)).astype(F32) - base[0:1, n:n + 1]
        where_to = jnp.where((at >= 0.0) & (at < held[:, n:n + 1]), at + start[:, n:n + 1], where_to)
    goal[...] = where_to

    first, second = (jnp.concatenate([ids_all[q, k:k + 1] for q in range(owners)], axis=0) for k in (0, 1))
    marks = jnp.concatenate([((first == me * local + j) | (second == me * local + j)).astype(F32) for j in range(local)], axis=0)
    earlier = plain(marks.astype(BF16), (ta < tb).astype(F32).astype(BF16))
    pos[...] = jnp.where(marks > 0.5, earlier, -1.0)

    def pick_rows(q):
        at = iota((slots, tokens), 0).astype(F32)
        match = jnp.concatenate([(at == pos[j * owners + q:j * owners + q + 1, :]).astype(F32) for j in range(local)], axis=0).astype(BF16)

        @pl.loop(0, width // 512)
        def _(n):
            cols = pl.ds(pl.multiple_of(n * 512, 512), 512)
            block = hid[:, cols] if q == 0 else land[q, :, cols]
            part = jnp.dot(match, block, preferred_element_type=F32).astype(BF16)
            for j in range(local):
                rows_out[j, q, :, cols] = part[j * slots:(j + 1) * slots]

    sent = [*to_x.values(), *to_y.values(), to_mate]

    def pass_on(q, c, n, to):
        copy = remote(q, c, n, to)
        copy.start()
        sent.append(copy)
        return copy

    pick_rows(0)
    across, mates = {}, {2: [], 4: [], 6: []}
    for cx, cy in zip(x_order, y_order):
        to_x[cx].wait_recv()
        if cx in (0, 1):
            across[cx] = pass_on(2, cx, 8 + cx, 4)
        mates[2].append(pass_on(2, cx, 12 + cx, 1))
        to_y[cy].wait_recv()
        if cy in (2, 3):
            across[cy] = pass_on(4, cy, 8 + cy, 2)
        mates[4].append(pass_on(4, cy, 16 + cy, 1))
        if cx == 0:
            to_mate.wait_recv()
            pick_rows(1)
    for q in (2, 4):
        pick_rows(q)
    for q in (2, 4):
        for m in mates[q]:
            m.wait_recv()
        pick_rows(q + 1)
    for c in (0, 2, 1, 3):
        across[c].wait_recv()
        mates[6].append(pass_on(6, c, 20 + c, 1))
    pick_rows(6)
    for m in mates[6]:
        m.wait_recv()
    pick_rows(7)
    for m in sent:
        m.wait_send()
    for c in id_copies:
        c.wait_send()
    for c in early:
        c.wait()


def gather_call(hidden, ids_t, wr_t, w1, w3, w2, owners, caps):
    tokens, width = hidden.shape
    experts = wr_t.shape[0]
    local, _, ffn = w1.shape
    slots = caps[-1][0] // local
    ft = ffn // NF
    vmem = pl.BlockSpec(memory_space=pltpu.VMEM)
    hbm = pl.BlockSpec(memory_space=pl.ANY)
    return pl.pallas_call(
        functools.partial(gather_kernel, caps),
        name='gather_tokens',
        out_shape=(
            pltpu.VMEM((local, owners, slots, width), BF16),
            jax.ShapeDtypeStruct((local * owners, tokens), F32),
            jax.ShapeDtypeStruct((tokens, 128), F32),
            jax.ShapeDtypeStruct((owners, 2 * local * slots), F32),
            jax.ShapeDtypeStruct((1,), I32),
            pltpu.VMEM((RING, width, ft), BF16),
            pltpu.VMEM((RING, width, ft), BF16),
            pltpu.VMEM((RING, ft, width), BF16),
        ),
        in_specs=[vmem, vmem, vmem, hbm, hbm, hbm],
        out_specs=(vmem, vmem, vmem, vmem, pl.BlockSpec(memory_space=pltpu.SMEM), vmem, vmem, vmem),
        scratch_shapes=[
            pltpu.VMEM((owners, tokens, width), BF16),
            pltpu.VMEM((owners, 2, tokens), I32),
            pltpu.SemaphoreType.DMA((25,)),
            pltpu.SemaphoreType.DMA((25,)),
            pltpu.SemaphoreType.DMA((owners,)),
            pltpu.SemaphoreType.DMA((owners,)),
            pltpu.SemaphoreType.DMA((RING, 3)),
        ],
        compiler_params=pltpu.CompilerParams(collective_id=0, has_side_effects=True, vmem_limit_bytes=11 * 1024 * 1024),
    )(hidden, ids_t, wr_t, w1, w3, w2)


def expert_kernel(caps, branch, pos, rows, _w1b, _w3b, _w2b, w1, w3, w2, ret, w1b, w3b, w2b, mid, yacc, plan, wsem):
    local, owners, slots, width = rows.shape
    ft = w1b.shape[2]
    steps = local * NF
    fixed = (RING + NF - 1) // NF

    size = []
    for j in range(local):
        most = jnp.max(pos[pl.ds(j * owners, owners), :]).astype(I32) + 1
        size.append(jnp.where(most > 32, slots, jnp.where(most > 16, 32, 16)))
    for j in range(local):
        rank = jnp.int32(min(j, fixed))
        offset = jnp.int32(0)
        for i in range(local):
            if i >= fixed and j >= fixed and i != j:
                ahead = (size[i] >= size[j]) if i < j else (size[i] > size[j])
                rank = rank + ahead.astype(I32)
            if i < j:
                offset = offset + size[i]
        plan[0, rank] = jnp.int32(j)
        plan[1, rank] = size[j]
        plan[2, rank] = offset
    used = size[0]
    for j in range(1, local):
        used = used + size[j]

    def weights(t):
        e = plan[0, t // NF]
        cols = pl.ds(pl.multiple_of((t % NF) * ft, ft), ft)
        n = t % RING
        return (
            pltpu.make_async_copy(w1.at[e, :, cols], w1b.at[n], wsem.at[n, 0]),
            pltpu.make_async_copy(w3.at[e, :, cols], w3b.at[n], wsem.at[n, 1]),
            pltpu.make_async_copy(w2.at[e, cols, :], w2b.at[n], wsem.at[n, 2]),
        )

    limit = jnp.int32(caps[0][0])
    for n in range(1, len(caps)):
        limit = jnp.where(branch[0] >= n, caps[n][0], limit)

    @pl.loop(used // 16, limit // 16)
    def _(n):
        blank = pl.ds(pl.multiple_of(n * 16, 16), 16)
        for q in range(owners):
            ret[q, blank, :] = jnp.zeros((16, width), BF16)

    @pl.loop(0, steps)
    def _(t):
        r, f, n = t // NF, t % NF, t % RING
        e = plan[0, r]

        @pl.when(t >= RING)
        def _():
            for c in weights(t):
                c.wait()

        for size in (16, 32, slots):
            m = size * owners

            @pl.when(plan[1, r] == size)
            def _():
                x = rows[e, :, 0:size, :].reshape(m, width)
                for c in range(0, ft, 256):
                    gate = jnp.dot(x, w1b[n, :, c:c + 256], preferred_element_type=F32)
                    up = jnp.dot(x, w3b[n, :, c:c + 256], preferred_element_type=F32)
                    mid[0:m, c:c + 256] = (gate * jax.nn.sigmoid(gate) * up).astype(BF16)
                for c in range(0, width, 512):
                    part = jnp.dot(mid[0:m, :], w2b[n, :, c:c + 512], preferred_element_type=F32)
                    yacc[0:m, c:c + 512] = jnp.where(f == 0, 0.0, yacc[0:m, c:c + 512]) + part

                @pl.when(f == NF - 1)
                def _():
                    first = pl.multiple_of(plan[2, r], 16)
                    for q in range(owners):
                        ret[q, pl.ds(first, size), :] = yacc[q * size:(q + 1) * size, :].astype(BF16)

        @pl.when(t + RING < steps)
        def _():
            for c in weights(t + RING):
                c.start()


def expert_call(branch, pos, rows, w1p, w3p, w2p, w1, w3, w2, caps):
    local, owners, slots, width = rows.shape
    ft = w1p.shape[2]
    hbm = pl.BlockSpec(memory_space=pl.ANY)
    vmem = pl.BlockSpec(memory_space=pltpu.VMEM)
    flops = 3 * 2 * local * slots * owners * width * ft * NF // 2
    return pl.pallas_call(
        functools.partial(expert_kernel, caps),
        name='experts',
        out_shape=(
            pltpu.VMEM((owners, caps[-1][0], width), BF16),
            pltpu.VMEM(w1p.shape, BF16),
            pltpu.VMEM(w3p.shape, BF16),
            pltpu.VMEM(w2p.shape, BF16),
        ),
        in_specs=[pl.BlockSpec(memory_space=pltpu.SMEM), vmem, vmem, vmem, vmem, vmem, hbm, hbm, hbm],
        out_specs=(vmem, vmem, vmem, vmem),
        input_output_aliases={3: 1, 4: 2, 5: 3},
        scratch_shapes=[
            pltpu.VMEM((owners * slots, ft), BF16),
            pltpu.VMEM((owners * slots, width), F32),
            pltpu.SMEM((3, local), I32),
            pltpu.SemaphoreType.DMA((RING, 3)),
        ],
        compiler_params=pltpu.CompilerParams(vmem_limit_bytes=12 * 1024 * 1024),
        cost_estimate=pl.CostEstimate(flops=flops, bytes_accessed=3 * 2 * local * width * ft * NF, transcendentals=0),
    )(branch, pos, rows, w1p, w3p, w2p, w1, w3, w2)[0]


REMOTE = (2, 4, 6)


def return_kernel(cap, chip_cap, ret, tok, goal, hid, scale, out, half, pack, got, acc, send, recv, half_send, half_recv):
    me = lax.axis_index('ep')
    tokens, width = hid.shape
    lanes = goal.shape[1] // 2
    barrier = pltpu.get_barrier_semaphore()
    for q in (1, *REMOTE):
        pl.semaphore_signal(barrier, inc=1, device_id=dev(flip(me, q)), device_id_type=MESH)
    pl.semaphore_wait(barrier, 1 + len(REMOTE))
    halves, copies = {}, {}
    for q in (*REMOTE, 0):
        halves[q] = pltpu.make_async_remote_copy(src_ref=ret.at[q + 1, pl.ds(0, cap)], dst_ref=half.at[q // 2], send_sem=half_send.at[q // 2], recv_sem=half_recv.at[q // 2], device_id=dev(flip(me, 1)), device_id_type=MESH)
        halves[q].start()

    for q in REMOTE:
        row = iota((chip_cap, cap), 0).astype(F32)
        mine = (row == goal[q:q + 1, 0:cap]).astype(F32).astype(BF16)
        theirs = (row == goal[q:q + 1, lanes:lanes + cap]).astype(F32).astype(BF16)
        halves[q].wait_recv()
        for c in range(0, width, 512):
            part = jnp.dot(mine, ret[q, 0:cap, c:c + 512], preferred_element_type=F32)
            part = part + jnp.dot(theirs, half[q // 2, :, c:c + 512], preferred_element_type=F32)
            pack[q // 2 - 1, :, c:c + 512] = part.astype(BF16)
        copies[q] = pltpu.make_async_remote_copy(src_ref=pack.at[q // 2 - 1], dst_ref=got.at[q // 2 - 1], send_sem=send.at[q // 2 - 1], recv_sem=recv.at[q // 2 - 1], device_id=dev(flip(me, q)), device_id_type=MESH)
        copies[q].start()

    table = tok[...]

    def chosen(column, peer, at, count):
        lane = iota((tokens, count), 1).astype(F32)
        return jnp.concatenate([((column[k] == peer) & (table[:, at + k:at + k + 1] == lane)).astype(F32) for k in (0, 1)], axis=0).astype(BF16)

    owner = [table[:, 2 + k:3 + k] for k in (0, 1)]
    chip = [jnp.floor(o * 0.5) for o in owner]

    def add(pick, block, fresh):
        for c in range(0, width, 512):
            part = jnp.dot(pick, block(c), preferred_element_type=F32)
            acc[:, c:c + 512] = part if fresh else acc[:, c:c + 512] + part

    add(chosen(owner, me.astype(F32), 4, cap), lambda c: ret[0, 0:cap, c:c + 512], True)
    pick = chosen(owner, flip(me, 1).astype(F32), 4, cap)
    halves[0].wait_recv()
    add(pick, lambda c: half[0, :, c:c + 512], False)
    for q in REMOTE:
        pick = chosen(chip, (flip(me, q) // 2).astype(F32), 6, chip_cap)
        copies[q].wait_recv()
        add(pick, lambda c: got[q // 2 - 1, :, c:c + 512], False)

    mixed = table[:, 0:1] * acc[0:tokens] + table[:, 1:2] * acc[tokens:2 * tokens]
    out[...] = (scale[0] * hid[...].astype(F32) + scale[1] * mixed).astype(BF16)
    for copy in (*halves.values(), *copies.values()):
        copy.wait_send()


def return_call(n, caps, ret, tok, goal, hidden, scale):
    owners, _, width = ret.shape
    tokens = hidden.shape[0]
    cap, chip_cap = caps
    vmem = pl.BlockSpec(memory_space=pltpu.VMEM)
    return pl.pallas_call(
        functools.partial(return_kernel, cap, chip_cap),
        name=f'return_{cap}_{chip_cap}',
        out_shape=jax.ShapeDtypeStruct((tokens, width), BF16),
        in_specs=[vmem, vmem, vmem, vmem, pl.BlockSpec(memory_space=pltpu.SMEM)],
        out_specs=vmem,
        scratch_shapes=[
            pltpu.VMEM((owners // 2, cap, width), BF16),
            pltpu.VMEM((len(REMOTE), chip_cap, width), BF16),
            pltpu.VMEM((len(REMOTE), chip_cap, width), BF16),
            pltpu.VMEM((2 * tokens, width), F32),
            pltpu.SemaphoreType.DMA((len(REMOTE),)),
            pltpu.SemaphoreType.DMA((len(REMOTE),)),
            pltpu.SemaphoreType.DMA((owners // 2,)),
            pltpu.SemaphoreType.DMA((owners // 2,)),
        ],
        compiler_params=pltpu.CompilerParams(collective_id=1 + n, has_side_effects=True, vmem_limit_bytes=24 * 1024 * 1024),
    )(ret, tok, goal, hidden, scale)


def capacities(local, slots):
    full = [slots * n + 16 * (local - n) for n in range(1, local + 1)]
    chip = [2 * slots + 8 + (slots - 8) * n for n in range(local - 1)] + [5 * slots]
    return (*zip(full, chip), (local * slots, 2 * local * slots))


def solution(mesh):
    owners = mesh.shape['ep']

    def local_step(hidden, router_w, expert_ids, w_gate, w_up, w_down, post_scale):
        tokens = hidden.shape[0]
        local = w_gate.shape[0]
        slots = tokens // max(1, local * owners // 8)
        caps = capacities(local, slots)
        rows, pos, tok, goal, branch, w1p, w3p, w2p = gather_call(hidden, expert_ids.T, router_w.T, w_gate, w_up, w_down, owners, caps)
        ret = expert_call(branch, pos, rows, w1p, w3p, w2p, w_gate, w_up, w_down, caps)
        branches = [functools.partial(return_call, n, cap) for n, cap in enumerate(caps)]
        return lax.switch(branch[0], branches, ret, tok, goal, hidden, post_scale)

    tok_spec = P(('dp', 'ep'))
    return jax.shard_map(local_step, mesh=mesh, in_specs=(tok_spec, P(), tok_spec, P('ep'), P('ep'), P('ep'), P()), out_specs=tok_spec, check_vma=False)
```

```python
import functools

import jax
import jax.numpy as jnp
from jax import lax
from jax.experimental import pallas as pl
from jax.experimental.pallas import tpu as pltpu
from jax.sharding import PartitionSpec as P

MESH = pl.DeviceIdType.MESH
F32, BF16, I32 = jnp.float32, jnp.bfloat16, jnp.int32
NT = (((1,), (1,)), ((), ()))


def flip(idx, mask):
    out = idx
    for bit in (1, 2, 4):
        if mask & bit:
            out = out + bit - 2 * bit * ((idx // bit) % 2)
    return out


def dev(idx):
    return (lax.axis_index('dp'), idx)


def iota(shape, dim):
    return lax.broadcasted_iota(I32, shape, dim)


CHUNKS = 4
NF = 3
RING = 4


def gather_kernel(caps, hid_in, ids_in, wrt_in, w1, w3, w2, rows_out, tok, goal, plan, w1p, w3p, w2p, hid, ids, wrt, pos, land, ids_all, send, recv, id_send, id_recv, wsem, in_sem):
    me = lax.axis_index('ep')
    own = [pltpu.make_async_copy(src, dst, in_sem.at[n]) for n, (src, dst) in enumerate(((hid_in, hid), (ids_in, ids), (wrt_in, wrt)))]
    for c in own:
        c.start()
    tokens, width = hid.shape
    experts = wrt.shape[0]
    local, owners, slots, _ = rows_out.shape
    ft = w1p.shape[2]
    rows = tokens // CHUNKS
    barrier = pltpu.get_barrier_semaphore()
    for q in range(1, owners):
        pl.semaphore_signal(barrier, inc=1, device_id=dev(flip(me, q)), device_id_type=MESH)
    pl.semaphore_wait(barrier, owners - 1)
    own[0].wait()
    own[1].wait()

    def piece(q, c):
        return (hid if q == 0 else land.at[q]).at[pl.ds(c * rows, rows)]

    def remote(q, c, n, to):
        return pltpu.make_async_remote_copy(src_ref=piece(q, c), dst_ref=land.at[q ^ to, pl.ds(c * rows, rows)], send_sem=send.at[n], recv_sem=recv.at[n], device_id=dev(flip(me, to)), device_id_type=MESH)

    id_copies = []
    for q in range(1, owners):
        id_copies.append(pltpu.make_async_remote_copy(src_ref=ids, dst_ref=ids_all.at[q], send_sem=id_send.at[q], recv_sem=id_recv.at[q], device_id=dev(flip(me, q)), device_id_type=MESH))
    for c in id_copies:
        c.start()
    x_order, y_order = (0, 1, 2, 3), (2, 3, 0, 1)
    to_x = {c: remote(0, c, c, 2) for c in x_order}
    to_y = {c: remote(0, c, 4 + c, 4) for c in y_order}
    for cx, cy in zip(x_order, y_order):
        to_x[cx].start()
        to_y[cy].start()
    to_mate = pltpu.make_async_remote_copy(src_ref=hid, dst_ref=land.at[1], send_sem=send.at[24], recv_sem=recv.at[24], device_id=dev(flip(me, 1)), device_id_type=MESH)
    to_mate.start()
    early = []
    for t in range(RING):
        e, cols = t // NF, pl.ds(t % NF * ft, ft)
        early += [
            pltpu.make_async_copy(w1.at[e, :, cols], w1p.at[t], wsem.at[t, 0]),
            pltpu.make_async_copy(w3.at[e, :, cols], w3p.at[t], wsem.at[t, 1]),
            pltpu.make_async_copy(w2.at[e, cols, :], w2p.at[t], wsem.at[t, 2]),
        ]
    for c in early:
        c.start()

    own[2].wait()
    h = hid[...]
    w = wrt[...]
    w_hi = w.astype(BF16)
    rest = w - w_hi.astype(F32)
    w_mid = rest.astype(BF16)
    w_lo = (rest - w_mid.astype(F32)).astype(BF16)
    dot = functools.partial(lax.dot_general, dimension_numbers=NT, preferred_element_type=F32)
    logits = dot(h, w_hi) + (dot(h, w_mid) + dot(h, w_lo))
    ex = jnp.exp(logits - jnp.max(logits, axis=1, keepdims=True))
    prob = ex / jnp.sum(ex, axis=1, keepdims=True)
    ta, tb = iota((tokens, tokens), 0), iota((tokens, tokens), 1)
    eye = (ta == tb).astype(F32).astype(BF16)
    own_ids = ids[...].astype(F32)
    lane = iota((tokens, experts), 1).astype(F32)
    id_col = [dot(eye, jnp.broadcast_to(own_ids[k:k + 1], (8, tokens)).astype(BF16))[:, 0:1] for k in (0, 1)]
    pick = [(id_col[k] == lane).astype(F32) for k in (0, 1)]
    g = [jnp.sum(pick[k] * prob, axis=1, keepdims=True) for k in (0, 1)]
    total = g[0] + g[1]

    for c in id_copies:
        c.wait_recv()
    ids_all[0] = ids[...]
    counts = []
    for q in range(owners):
        both = ids_all[q]
        e_col = iota((experts, tokens), 0)
        hot = ((both[0:1] == e_col) | (both[1:2] == e_col)).astype(F32).astype(BF16)
        counts.append(dot(jnp.ones((8, tokens), BF16), hot))
    most = functools.reduce(jnp.maximum, counts)
    count = jnp.concatenate([c[0:1] for c in counts], axis=0)
    stride = jnp.where(most > 32.0, float(slots), jnp.where(most > 16.0, 32.0, 16.0))
    mark = lambda mask: mask.astype(F32).astype(BF16)
    plain = functools.partial(jnp.dot, preferred_element_type=F32)
    ea, eb = iota((experts, experts), 0), iota((experts, experts), 1)
    same, same_chip = ea // local == eb // local, ea // (2 * local) == eb // (2 * local)
    offset = plain(stride.astype(BF16), mark(same & (ea < eb)))
    need = jnp.max(plain(stride.astype(BF16), mark(same))).astype(I32)
    need_chip = jnp.max(plain(count.astype(BF16), mark(same_chip))).astype(I32)
    branch = jnp.int32(0)
    for limit, limit_chip in caps[:-1]:
        branch = branch + ((need > limit) | (need_chip > limit_chip)).astype(I32)
    plan[0] = branch
    rank = plain(mark(tb < ta), (pick[0] + pick[1]).astype(BF16))
    chip_first = plain(count.astype(BF16), mark(same_chip & (ea < eb)))[0:1]
    slot = [jnp.sum(pick[k] * (rank + offset[0:1]), axis=1, keepdims=True) for k in (0, 1)]
    packed = [jnp.sum(pick[k] * (rank + chip_first), axis=1, keepdims=True) for k in (0, 1)]
    owner = [jnp.floor(id_col[k] * (1.0 / local)) for k in (0, 1)]
    wide = iota((tokens, 128), 1)
    table = jnp.zeros((tokens, 128), F32)
    for n, col in enumerate((g[0] / total, g[1] / total, *owner, *slot, *packed)):
        table = jnp.where(wide == n, col, table)
    tok[...] = table

    e_row, n_col = iota((experts, 128), 0), iota((experts, 128), 1)
    e_of = jnp.where(n_col < local, me * local + n_col, flip(me, 1) * local + n_col - local)
    used = n_col < 2 * local
    held = plain(count.astype(BF16), mark(used & (e_row == e_of)))
    start = plain(count.astype(BF16), mark(used & (e_row // (2 * local) == me // 2) & (e_row < e_of)))
    base = plain(stride.astype(BF16), mark(used & (e_row // local == e_of // local) & (e_row < e_of)))
    base_size = plain(stride.astype(BF16), mark(used & (e_row == e_of)))
    lane_of = iota((owners, goal.shape[1]), 1)
    where_to = jnp.full((owners, goal.shape[1]), -1.0, F32)
    for n in range(2 * local):
        at = (lane_of - (n // local) * (goal.shape[1] // 2)).astype(F32) - base[0:1, n:n + 1]
        where_to = jnp.where((at >= 0.0) & (at < held[:, n:n + 1]), at + start[:, n:n + 1], where_to)
    goal[...] = where_to

    first, second = (jnp.concatenate([ids_all[q, k:k + 1] for q in range(owners)], axis=0) for k in (0, 1))
    marks = jnp.concatenate([((first == me * local + j) | (second == me * local + j)).astype(F32) for j in range(local)], axis=0)
    earlier = plain(marks.astype(BF16), (ta < tb).astype(F32).astype(BF16))
    pos[...] = jnp.where(marks > 0.5, earlier, -1.0)
    for j in range(local):
        plan[1 + j] = jnp.max(base_size[:, j:j + 1]).astype(I32)

    def pick_rows(q):
        at = iota((slots, tokens), 0).astype(F32)
        match = jnp.concatenate([(at == pos[j * owners + q:j * owners + q + 1, :]).astype(F32) for j in range(local)], axis=0).astype(BF16)

        @pl.loop(0, width // 512)
        def _(n):
            cols = pl.ds(pl.multiple_of(n * 512, 512), 512)
            block = hid[:, cols] if q == 0 else land[q, :, cols]
            part = jnp.dot(match, block, preferred_element_type=F32).astype(BF16)
            for j in range(local):
                rows_out[j, q, :, cols] = part[j * slots:(j + 1) * slots]

    sent = [*to_x.values(), *to_y.values(), to_mate]

    def pass_on(q, c, n, to):
        copy = remote(q, c, n, to)
        copy.start()
        sent.append(copy)
        return copy

    pick_rows(0)
    across, mates = {}, {2: [], 4: [], 6: []}
    for cx, cy in zip(x_order, y_order):
        to_x[cx].wait_recv()
        if cx in (0, 1):
            across[cx] = pass_on(2, cx, 8 + cx, 4)
        mates[2].append(pass_on(2, cx, 12 + cx, 1))
        to_y[cy].wait_recv()
        if cy in (2, 3):
            across[cy] = pass_on(4, cy, 8 + cy, 2)
        mates[4].append(pass_on(4, cy, 16 + cy, 1))
        if cx == 0:
            to_mate.wait_recv()
            pick_rows(1)
    for q in (2, 4):
        pick_rows(q)
    for q in (2, 4):
        for m in mates[q]:
            m.wait_recv()
        pick_rows(q + 1)
    for c in (0, 2, 1, 3):
        across[c].wait_recv()
        mates[6].append(pass_on(6, c, 20 + c, 1))
    pick_rows(6)
    for m in mates[6]:
        m.wait_recv()
    pick_rows(7)
    for m in sent:
        m.wait_send()
    for c in id_copies:
        c.wait_send()
    for c in early:
        c.wait()


def gather_call(hidden, ids_t, wr_t, w1, w3, w2, owners, caps):
    tokens, width = hidden.shape
    experts = wr_t.shape[0]
    local, _, ffn = w1.shape
    slots = caps[-1][0] // local
    ft = ffn // NF
    vmem = pl.BlockSpec(memory_space=pltpu.VMEM)
    hbm = pl.BlockSpec(memory_space=pl.ANY)
    return pl.pallas_call(
        functools.partial(gather_kernel, caps),
        name='gather_tokens',
        out_shape=(
            pltpu.VMEM((local, owners, slots, width), BF16),
            jax.ShapeDtypeStruct((tokens, 128), F32),
            jax.ShapeDtypeStruct((owners, 2 * local * slots), F32),
            jax.ShapeDtypeStruct((1 + local,), I32),
            pltpu.VMEM((RING, width, ft), BF16),
            pltpu.VMEM((RING, width, ft), BF16),
            pltpu.VMEM((RING, ft, width), BF16),
        ),
        in_specs=[hbm, *[pl.BlockSpec(memory_space=pltpu.HBM)] * 2, hbm, hbm, hbm],
        out_specs=(vmem, vmem, vmem, pl.BlockSpec(memory_space=pltpu.SMEM), vmem, vmem, vmem),
        scratch_shapes=[
            pltpu.VMEM((tokens, width), BF16),
            pltpu.VMEM((2, tokens), I32),
            pltpu.VMEM((experts, width), F32),
            pltpu.VMEM((local * owners, tokens), F32),
            pltpu.VMEM((owners, tokens, width), BF16),
            pltpu.VMEM((owners, 2, tokens), I32),
            pltpu.SemaphoreType.DMA((25,)),
            pltpu.SemaphoreType.DMA((25,)),
            pltpu.SemaphoreType.DMA((owners,)),
            pltpu.SemaphoreType.DMA((owners,)),
            pltpu.SemaphoreType.DMA((RING, 3)),
            pltpu.SemaphoreType.DMA((3,)),
        ],
        compiler_params=pltpu.CompilerParams(collective_id=0, has_side_effects=True, vmem_limit_bytes=11 * 1024 * 1024),
    )(hidden, *(pltpu.with_memory_space_constraint(x, pltpu.HBM) for x in (ids_t, wr_t)), w1, w3, w2)


def expert_kernel(caps, sizes, rows, _w1b, _w3b, _w2b, w1, w3, w2, ret, w1b, w3b, w2b, mid, yacc, plan, wsem):
    local, owners, slots, width = rows.shape
    ft = w1b.shape[2]
    steps = local * NF
    fixed = (RING + NF - 1) // NF

    size = [sizes[1 + j] for j in range(local)]
    for j in range(local):
        rank = jnp.int32(min(j, fixed))
        offset = jnp.int32(0)
        for i in range(local):
            if i >= fixed and j >= fixed and i != j:
                ahead = (size[i] >= size[j]) if i < j else (size[i] > size[j])
                rank = rank + ahead.astype(I32)
            if i < j:
                offset = offset + size[i]
        plan[0, rank] = jnp.int32(j)
        plan[1, rank] = size[j]
        plan[2, rank] = offset
    used = size[0]
    for j in range(1, local):
        used = used + size[j]

    def weights(t):
        e = plan[0, t // NF]
        cols = pl.ds(pl.multiple_of((t % NF) * ft, ft), ft)
        n = t % RING
        return (
            pltpu.make_async_copy(w1.at[e, :, cols], w1b.at[n], wsem.at[n, 0]),
            pltpu.make_async_copy(w3.at[e, :, cols], w3b.at[n], wsem.at[n, 1]),
            pltpu.make_async_copy(w2.at[e, cols, :], w2b.at[n], wsem.at[n, 2]),
        )

    limit = jnp.int32(caps[0][0])
    for n in range(1, len(caps)):
        limit = jnp.where(sizes[0] >= n, caps[n][0], limit)

    @pl.loop(used // 16, limit // 16)
    def _(n):
        blank = pl.ds(pl.multiple_of(n * 16, 16), 16)
        for q in range(owners):
            ret[q, blank, :] = jnp.zeros((16, width), BF16)

    @pl.loop(0, steps)
    def _(t):
        r, f, n = t // NF, t % NF, t % RING
        e = plan[0, r]

        @pl.when(t >= RING)
        def _():
            for c in weights(t):
                c.wait()

        for size in (16, 32, slots):
            m = size * owners

            @pl.when(plan[1, r] == size)
            def _():
                x = rows[e, :, 0:size, :].reshape(m, width)
                for c in range(0, ft, 256):
                    gate = jnp.dot(x, w1b[n, :, c:c + 256], preferred_element_type=F32)
                    up = jnp.dot(x, w3b[n, :, c:c + 256], preferred_element_type=F32)
                    mid[0:m, c:c + 256] = (gate * jax.nn.sigmoid(gate) * up).astype(BF16)
                for c in range(0, width, 512):
                    part = jnp.dot(mid[0:m, :], w2b[n, :, c:c + 512], preferred_element_type=F32)
                    yacc[0:m, c:c + 512] = jnp.where(f == 0, 0.0, yacc[0:m, c:c + 512]) + part

                @pl.when(f == NF - 1)
                def _():
                    first = pl.multiple_of(plan[2, r], 16)
                    for q in range(owners):
                        ret[q, pl.ds(first, size), :] = yacc[q * size:(q + 1) * size, :].astype(BF16)

        @pl.when(t + RING < steps)
        def _():
            for c in weights(t + RING):
                c.start()


def expert_call(sizes, rows, w1p, w3p, w2p, w1, w3, w2, caps):
    local, owners, slots, width = rows.shape
    ft = w1p.shape[2]
    hbm = pl.BlockSpec(memory_space=pl.ANY)
    vmem = pl.BlockSpec(memory_space=pltpu.VMEM)
    flops = 3 * 2 * local * slots * owners * width * ft * NF // 2
    return pl.pallas_call(
        functools.partial(expert_kernel, caps),
        name='experts',
        out_shape=(
            pltpu.VMEM((owners, caps[-1][0], width), BF16),
            pltpu.VMEM(w1p.shape, BF16),
            pltpu.VMEM(w3p.shape, BF16),
            pltpu.VMEM(w2p.shape, BF16),
        ),
        in_specs=[pl.BlockSpec(memory_space=pltpu.SMEM), vmem, vmem, vmem, vmem, hbm, hbm, hbm],
        out_specs=(vmem, vmem, vmem, vmem),
        input_output_aliases={2: 1, 3: 2, 4: 3},
        scratch_shapes=[
            pltpu.VMEM((owners * slots, ft), BF16),
            pltpu.VMEM((owners * slots, width), F32),
            pltpu.SMEM((3, local), I32),
            pltpu.SemaphoreType.DMA((RING, 3)),
        ],
        compiler_params=pltpu.CompilerParams(vmem_limit_bytes=12 * 1024 * 1024),
        cost_estimate=pl.CostEstimate(flops=flops, bytes_accessed=3 * 2 * local * width * ft * NF, transcendentals=0),
    )(sizes, rows, w1p, w3p, w2p, w1, w3, w2)[0]


REMOTE = (2, 4, 6)


def return_kernel(cap, chip_cap, ret, tok, goal, hid, scale, out, half, pack, got, acc, send, recv, half_send, half_recv):
    me = lax.axis_index('ep')
    tokens, width = hid.shape
    lanes = goal.shape[1] // 2
    barrier = pltpu.get_barrier_semaphore()
    for q in (1, *REMOTE):
        pl.semaphore_signal(barrier, inc=1, device_id=dev(flip(me, q)), device_id_type=MESH)
    pl.semaphore_wait(barrier, 1 + len(REMOTE))
    halves, copies = {}, {}
    for q in (*REMOTE, 0):
        halves[q] = pltpu.make_async_remote_copy(src_ref=ret.at[q + 1, pl.ds(0, cap)], dst_ref=half.at[q // 2], send_sem=half_send.at[q // 2], recv_sem=half_recv.at[q // 2], device_id=dev(flip(me, 1)), device_id_type=MESH)
        halves[q].start()

    for q in REMOTE:
        row = iota((chip_cap, cap), 0).astype(F32)
        mine = (row == goal[q:q + 1, 0:cap]).astype(F32).astype(BF16)
        theirs = (row == goal[q:q + 1, lanes:lanes + cap]).astype(F32).astype(BF16)
        halves[q].wait_recv()
        for c in range(0, width, 512):
            part = jnp.dot(mine, ret[q, 0:cap, c:c + 512], preferred_element_type=F32)
            part = part + jnp.dot(theirs, half[q // 2, :, c:c + 512], preferred_element_type=F32)
            pack[q // 2 - 1, :, c:c + 512] = part.astype(BF16)
        copies[q] = pltpu.make_async_remote_copy(src_ref=pack.at[q // 2 - 1], dst_ref=got.at[q // 2 - 1], send_sem=send.at[q // 2 - 1], recv_sem=recv.at[q // 2 - 1], device_id=dev(flip(me, q)), device_id_type=MESH)
        copies[q].start()

    table = tok[...]

    def chosen(column, peer, at, count):
        lane = iota((tokens, count), 1).astype(F32)
        return jnp.concatenate([((column[k] == peer) & (table[:, at + k:at + k + 1] == lane)).astype(F32) for k in (0, 1)], axis=0).astype(BF16)

    owner = [table[:, 2 + k:3 + k] for k in (0, 1)]
    chip = [jnp.floor(o * 0.5) for o in owner]

    def add(pick, block, fresh):
        for c in range(0, width, 512):
            part = jnp.dot(pick, block(c), preferred_element_type=F32)
            acc[:, c:c + 512] = part if fresh else acc[:, c:c + 512] + part

    add(chosen(owner, me.astype(F32), 4, cap), lambda c: ret[0, 0:cap, c:c + 512], True)
    pick = chosen(owner, flip(me, 1).astype(F32), 4, cap)
    halves[0].wait_recv()
    add(pick, lambda c: half[0, :, c:c + 512], False)
    for q in REMOTE:
        pick = chosen(chip, (flip(me, q) // 2).astype(F32), 6, chip_cap)
        copies[q].wait_recv()
        add(pick, lambda c: got[q // 2 - 1, :, c:c + 512], False)

    mixed = table[:, 0:1] * acc[0:tokens] + table[:, 1:2] * acc[tokens:2 * tokens]
    out[...] = (scale[0] * hid[...].astype(F32) + scale[1] * mixed).astype(BF16)
    for copy in (*halves.values(), *copies.values()):
        copy.wait_send()


def return_call(n, caps, ret, tok, goal, hidden, scale):
    owners, _, width = ret.shape
    tokens = hidden.shape[0]
    cap, chip_cap = caps
    vmem = pl.BlockSpec(memory_space=pltpu.VMEM)
    return pl.pallas_call(
        functools.partial(return_kernel, cap, chip_cap),
        name=f'return_{cap}_{chip_cap}',
        out_shape=jax.ShapeDtypeStruct((tokens, width), BF16),
        in_specs=[vmem, vmem, vmem, vmem, pl.BlockSpec(memory_space=pltpu.SMEM)],
        out_specs=vmem,
        scratch_shapes=[
            pltpu.VMEM((owners // 2, cap, width), BF16),
            pltpu.VMEM((len(REMOTE), chip_cap, width), BF16),
            pltpu.VMEM((len(REMOTE), chip_cap, width), BF16),
            pltpu.VMEM((2 * tokens, width), F32),
            pltpu.SemaphoreType.DMA((len(REMOTE),)),
            pltpu.SemaphoreType.DMA((len(REMOTE),)),
            pltpu.SemaphoreType.DMA((owners // 2,)),
            pltpu.SemaphoreType.DMA((owners // 2,)),
        ],
        compiler_params=pltpu.CompilerParams(collective_id=1 + n, has_side_effects=True, vmem_limit_bytes=24 * 1024 * 1024),
    )(ret, tok, goal, hidden, scale)


def capacities(local, slots):
    full = [slots * n + 16 * (local - n) for n in range(1, local + 1)]
    chip = [2 * slots + 8 + (slots - 8) * n for n in range(local - 1)] + [5 * slots]
    return (*zip(full, chip), (local * slots, 2 * local * slots))


def solution(mesh):
    owners = mesh.shape['ep']

    def local_step(hidden, router_w, expert_ids, w_gate, w_up, w_down, post_scale):
        tokens = hidden.shape[0]
        local = w_gate.shape[0]
        slots = tokens // max(1, local * owners // 8)
        caps = capacities(local, slots)
        rows, tok, goal, sizes, w1p, w3p, w2p = gather_call(hidden, expert_ids.T, router_w.T, w_gate, w_up, w_down, owners, caps)
        ret = expert_call(sizes, rows, w1p, w3p, w2p, w_gate, w_up, w_down, caps)
        branches = [functools.partial(return_call, n, cap) for n, cap in enumerate(caps)]
        return lax.switch(sizes[0], branches, ret, tok, goal, hidden, post_scale)

    tok_spec = P(('dp', 'ep'))
    return jax.shard_map(local_step, mesh=mesh, in_specs=(tok_spec, P(), tok_spec, P('ep'), P('ep'), P('ep'), P()), out_specs=tok_spec, check_vma=False)
```

```python
import functools

import jax
import jax.numpy as jnp
from jax import lax
from jax.experimental import pallas as pl
from jax.experimental.pallas import tpu as pltpu
from jax.sharding import PartitionSpec as P

MESH = pl.DeviceIdType.MESH
F32, BF16, I32 = jnp.float32, jnp.bfloat16, jnp.int32
NT = (((1,), (1,)), ((), ()))


def flip(idx, mask):
    out = idx
    for bit in (1, 2, 4):
        if mask & bit:
            out = out + bit - 2 * bit * ((idx // bit) % 2)
    return out


def dev(idx):
    return (lax.axis_index('dp'), idx)


def iota(shape, dim):
    return lax.broadcasted_iota(I32, shape, dim)


CHUNKS = 4
NF = 3
RING = 4


def gather_kernel(caps, hid_in, ids_in, wrt_in, w1, w3, w2, rows_out, y_own, tok, goal, plan, w1p, w3p, w2p, hid, ids, wrt, pos, mid, yacc, land, ids_all, send, recv, id_send, id_recv, wsem, in_sem):
    me = lax.axis_index('ep')
    own = [pltpu.make_async_copy(src, dst, in_sem.at[n]) for n, (src, dst) in enumerate(((hid_in, hid), (ids_in, ids), (wrt_in, wrt)))]
    for c in own:
        c.start()
    local, owners, slots, _ = rows_out.shape
    ft = w1p.shape[2]
    steps = local * NF

    def weights(t):
        e, n = local - 1 - t // NF, t % RING
        cols = pl.ds(pl.multiple_of((t % NF) * ft, ft), ft)
        return (
            pltpu.make_async_copy(w1.at[e, :, cols], w1p.at[n], wsem.at[n, 0]),
            pltpu.make_async_copy(w3.at[e, :, cols], w3p.at[n], wsem.at[n, 1]),
            pltpu.make_async_copy(w2.at[e, cols, :], w2p.at[n], wsem.at[n, 2]),
        )

    for t in range(RING):
        for c in weights(t):
            c.start()
    tokens, width = hid.shape
    experts = wrt.shape[0]
    rows = tokens // CHUNKS
    barrier = pltpu.get_barrier_semaphore()
    for q in range(1, owners):
        pl.semaphore_signal(barrier, inc=1, device_id=dev(flip(me, q)), device_id_type=MESH)
    pl.semaphore_wait(barrier, owners - 1)
    own[0].wait()
    own[1].wait()

    def piece(q, c):
        return (hid if q == 0 else land.at[q]).at[pl.ds(c * rows, rows)]

    def remote(q, c, n, to):
        return pltpu.make_async_remote_copy(src_ref=piece(q, c), dst_ref=land.at[q ^ to, pl.ds(c * rows, rows)], send_sem=send.at[n], recv_sem=recv.at[n], device_id=dev(flip(me, to)), device_id_type=MESH)

    id_copies = []
    for q in range(1, owners):
        id_copies.append(pltpu.make_async_remote_copy(src_ref=ids, dst_ref=ids_all.at[q], send_sem=id_send.at[q], recv_sem=id_recv.at[q], device_id=dev(flip(me, q)), device_id_type=MESH))
    for c in id_copies:
        c.start()
    x_order, y_order = (0, 1, 2, 3), (2, 3, 0, 1)
    to_x = {c: remote(0, c, c, 2) for c in x_order}
    to_y = {c: remote(0, c, 4 + c, 4) for c in y_order}
    for cx, cy in zip(x_order, y_order):
        to_x[cx].start()
        to_y[cy].start()
    to_mate = pltpu.make_async_remote_copy(src_ref=hid, dst_ref=land.at[1], send_sem=send.at[24], recv_sem=recv.at[24], device_id=dev(flip(me, 1)), device_id_type=MESH)
    to_mate.start()

    own[2].wait()
    h = hid[...]
    w = wrt[...]
    w_hi = w.astype(BF16)
    rest = w - w_hi.astype(F32)
    w_mid = rest.astype(BF16)
    w_lo = (rest - w_mid.astype(F32)).astype(BF16)
    dot = functools.partial(lax.dot_general, dimension_numbers=NT, preferred_element_type=F32)
    logits = dot(h, w_hi) + (dot(h, w_mid) + dot(h, w_lo))
    ex = jnp.exp(logits - jnp.max(logits, axis=1, keepdims=True))
    prob = ex / jnp.sum(ex, axis=1, keepdims=True)
    ta, tb = iota((tokens, tokens), 0), iota((tokens, tokens), 1)
    eye = (ta == tb).astype(F32).astype(BF16)
    own_ids = ids[...].astype(F32)
    lane = iota((tokens, experts), 1).astype(F32)
    id_col = [dot(eye, jnp.broadcast_to(own_ids[k:k + 1], (8, tokens)).astype(BF16))[:, 0:1] for k in (0, 1)]
    pick = [(id_col[k] == lane).astype(F32) for k in (0, 1)]
    g = [jnp.sum(pick[k] * prob, axis=1, keepdims=True) for k in (0, 1)]
    total = g[0] + g[1]

    for c in id_copies:
        c.wait_recv()
    ids_all[0] = ids[...]
    counts = []
    for q in range(owners):
        both = ids_all[q]
        e_col = iota((experts, tokens), 0)
        hot = ((both[0:1] == e_col) | (both[1:2] == e_col)).astype(F32).astype(BF16)
        counts.append(dot(jnp.ones((8, tokens), BF16), hot))
    most = functools.reduce(jnp.maximum, counts)
    count = jnp.concatenate([c[0:1] for c in counts], axis=0)
    stride = jnp.where(most > 32.0, float(slots), jnp.where(most > 16.0, 32.0, 16.0))
    mark = lambda mask: mask.astype(F32).astype(BF16)
    plain = functools.partial(jnp.dot, preferred_element_type=F32)
    ea, eb = iota((experts, experts), 0), iota((experts, experts), 1)
    same, same_chip = ea // local == eb // local, ea // (2 * local) == eb // (2 * local)
    offset = plain(stride.astype(BF16), mark(same & (ea < eb)))
    need = jnp.max(plain(stride.astype(BF16), mark(same))).astype(I32)
    need_chip = jnp.max(plain(count.astype(BF16), mark(same_chip))).astype(I32)
    branch = jnp.int32(0)
    for limit, limit_chip in caps[:-1]:
        branch = branch + ((need > limit) | (need_chip > limit_chip)).astype(I32)
    plan[0] = branch
    rank = plain(mark(tb < ta), (pick[0] + pick[1]).astype(BF16))
    chip_first = plain(count.astype(BF16), mark(same_chip & (ea < eb)))[0:1]
    slot = [jnp.sum(pick[k] * (rank + offset[0:1]), axis=1, keepdims=True) for k in (0, 1)]
    packed = [jnp.sum(pick[k] * (rank + chip_first), axis=1, keepdims=True) for k in (0, 1)]
    owner = [jnp.floor(id_col[k] * (1.0 / local)) for k in (0, 1)]
    wide = iota((tokens, 128), 1)
    table = jnp.zeros((tokens, 128), F32)
    for n, col in enumerate((g[0] / total, g[1] / total, *owner, *slot, *packed)):
        table = jnp.where(wide == n, col, table)
    tok[...] = table

    e_row, n_col = iota((experts, 128), 0), iota((experts, 128), 1)
    e_of = jnp.where(n_col < local, me * local + n_col, flip(me, 1) * local + n_col - local)
    used = n_col < 2 * local
    held = plain(count.astype(BF16), mark(used & (e_row == e_of)))
    start = plain(count.astype(BF16), mark(used & (e_row // (2 * local) == me // 2) & (e_row < e_of)))
    base = plain(stride.astype(BF16), mark(used & (e_row // local == e_of // local) & (e_row < e_of)))
    base_size = plain(stride.astype(BF16), mark(used & (e_row == e_of)))
    lane_of = iota((owners, goal.shape[1]), 1)
    where_to = jnp.full((owners, goal.shape[1]), -1.0, F32)
    for n in range(2 * local):
        at = (lane_of - (n // local) * (goal.shape[1] // 2)).astype(F32) - base[0:1, n:n + 1]
        where_to = jnp.where((at >= 0.0) & (at < held[:, n:n + 1]), at + start[:, n:n + 1], where_to)
    goal[...] = where_to

    first, second = (jnp.concatenate([ids_all[q, k:k + 1] for q in range(owners)], axis=0) for k in (0, 1))
    marks = jnp.concatenate([((first == me * local + j) | (second == me * local + j)).astype(F32) for j in range(local)], axis=0)
    earlier = plain(marks.astype(BF16), (ta < tb).astype(F32).astype(BF16))
    pos[...] = jnp.where(marks > 0.5, earlier, -1.0)
    for j in range(local):
        plan[1 + j] = jnp.max(base_size[:, j:j + 1]).astype(I32)

    def pick_rows(q):
        at = iota((slots, tokens), 0).astype(F32)
        match = jnp.concatenate([(at == pos[j * owners + q:j * owners + q + 1, :]).astype(F32) for j in range(local)], axis=0).astype(BF16)

        @pl.loop(0, width // 512)
        def _(n):
            cols = pl.ds(pl.multiple_of(n * 512, 512), 512)
            block = hid[:, cols] if q == 0 else land[q, :, cols]
            part = jnp.dot(match, block, preferred_element_type=F32).astype(BF16)
            for j in range(local):
                rows_out[j, q, :, cols] = part[j * slots:(j + 1) * slots]

    def own_steps(first, last):
        @pl.loop(first, last)
        def _(t):
            e, f, n = local - 1 - t // NF, t % NF, t % RING
            for c in weights(t):
                c.wait()
            x = rows_out[e, 0:2, :, :].reshape(2 * slots, width)
            for c in range(0, ft, 256):
                gate = jnp.dot(x, w1p[n, :, c:c + 256], preferred_element_type=F32)
                up = jnp.dot(x, w3p[n, :, c:c + 256], preferred_element_type=F32)
                mid[:, c:c + 256] = (gate * jax.nn.sigmoid(gate) * up).astype(BF16)
            for c in range(0, width, 512):
                part = jnp.dot(mid[...], w2p[n, :, c:c + 512], preferred_element_type=F32)
                yacc[:, c:c + 512] = jnp.where(f == 0, 0.0, yacc[:, c:c + 512]) + part

            @pl.when(f == NF - 1)
            def _():
                for q in (0, 1):
                    y_own[e, q, :, :] = yacc[q * slots:(q + 1) * slots, :].astype(BF16)

            @pl.when(t + RING < steps)
            def _():
                for c in weights(t + RING):
                    c.start()

    sent = [*to_x.values(), *to_y.values(), to_mate]

    def pass_on(q, c, n, to):
        copy = remote(q, c, n, to)
        copy.start()
        sent.append(copy)
        return copy

    pick_rows(0)
    to_mate.wait_recv()
    pick_rows(1)
    across, mates = {}, {2: [], 4: [], 6: []}
    for n, (cx, cy) in enumerate(zip(x_order, y_order)):
        if n < NF:
            own_steps(n * steps // 4, (n + 1) * steps // 4)
        to_x[cx].wait_recv()
        if cx in (0, 1):
            across[cx] = pass_on(2, cx, 8 + cx, 4)
        mates[2].append(pass_on(2, cx, 12 + cx, 1))
        to_y[cy].wait_recv()
        if cy in (2, 3):
            across[cy] = pass_on(4, cy, 8 + cy, 2)
        mates[4].append(pass_on(4, cy, 16 + cy, 1))
    for q in (2, 4):
        pick_rows(q)
    for q in (2, 4):
        for m in mates[q]:
            m.wait_recv()
        pick_rows(q + 1)
    own_steps(3 * steps // 4, steps)
    for c in (0, 2, 1, 3):
        across[c].wait_recv()
        mates[6].append(pass_on(6, c, 20 + c, 1))
    pick_rows(6)
    for m in mates[6]:
        m.wait_recv()
    pick_rows(7)
    for m in sent:
        m.wait_send()
    for c in id_copies:
        c.wait_send()


def gather_call(hidden, ids_t, wr_t, w1, w3, w2, owners, caps):
    tokens, width = hidden.shape
    experts = wr_t.shape[0]
    local, _, ffn = w1.shape
    slots = caps[-1][0] // local
    ft = ffn // NF
    vmem = pl.BlockSpec(memory_space=pltpu.VMEM)
    hbm = pl.BlockSpec(memory_space=pl.ANY)
    return pl.pallas_call(
        functools.partial(gather_kernel, caps),
        name='gather_tokens',
        out_shape=(
            pltpu.VMEM((local, owners, slots, width), BF16),
            pltpu.VMEM((local, 2, slots, width), BF16),
            jax.ShapeDtypeStruct((tokens, 128), F32),
            jax.ShapeDtypeStruct((owners, 2 * local * slots), F32),
            jax.ShapeDtypeStruct((1 + local,), I32),
            pltpu.VMEM((RING, width, ft), BF16),
            pltpu.VMEM((RING, width, ft), BF16),
            pltpu.VMEM((RING, ft, width), BF16),
        ),
        in_specs=[hbm, *[pl.BlockSpec(memory_space=pltpu.HBM)] * 2, hbm, hbm, hbm],
        out_specs=(vmem, vmem, vmem, vmem, pl.BlockSpec(memory_space=pltpu.SMEM), vmem, vmem, vmem),
        scratch_shapes=[
            pltpu.VMEM((tokens, width), BF16),
            pltpu.VMEM((2, tokens), I32),
            pltpu.VMEM((experts, width), F32),
            pltpu.VMEM((local * owners, tokens), F32),
            pltpu.VMEM((2 * slots, ft), BF16),
            pltpu.VMEM((2 * slots, width), F32),
            pltpu.VMEM((owners, tokens, width), BF16),
            pltpu.VMEM((owners, 2, tokens), I32),
            pltpu.SemaphoreType.DMA((25,)),
            pltpu.SemaphoreType.DMA((25,)),
            pltpu.SemaphoreType.DMA((owners,)),
            pltpu.SemaphoreType.DMA((owners,)),
            pltpu.SemaphoreType.DMA((RING, 3)),
            pltpu.SemaphoreType.DMA((3,)),
        ],
        compiler_params=pltpu.CompilerParams(collective_id=0, has_side_effects=True, vmem_limit_bytes=13 * 1024 * 1024),
    )(hidden, *(pltpu.with_memory_space_constraint(x, pltpu.HBM) for x in (ids_t, wr_t)), w1, w3, w2)


def expert_kernel(caps, sizes, rows, y_own, _w1b, _w3b, _w2b, w1, w3, w2, ret, w1b, w3b, w2b, mid, yacc, plan, wsem):
    local, owners, slots, width = rows.shape
    ft = w1b.shape[2]
    steps = local * NF
    fixed = (RING + NF - 1) // NF

    size = [sizes[1 + j] for j in range(local)]
    for j in range(local):
        rank = jnp.int32(min(j, fixed))
        offset = jnp.int32(0)
        for i in range(local):
            if i >= fixed and j >= fixed and i != j:
                ahead = (size[i] >= size[j]) if i < j else (size[i] > size[j])
                rank = rank + ahead.astype(I32)
            if i < j:
                offset = offset + size[i]
        plan[0, rank] = jnp.int32(j)
        plan[1, rank] = size[j]
        plan[2, rank] = offset
    used = size[0]
    for j in range(1, local):
        used = used + size[j]

    def part_of(t):
        turn = jnp.where(t < NF, 0, 2 * NF - RING)
        return (t % NF + turn) % NF

    def weights(t):
        e = plan[0, t // NF]
        cols = pl.ds(pl.multiple_of(part_of(t) * ft, ft), ft)
        n = (t + steps - NF) % RING
        return (
            pltpu.make_async_copy(w1.at[e, :, cols], w1b.at[n], wsem.at[n, 0]),
            pltpu.make_async_copy(w3.at[e, :, cols], w3b.at[n], wsem.at[n, 1]),
            pltpu.make_async_copy(w2.at[e, cols, :], w2b.at[n], wsem.at[n, 2]),
        )

    limit = jnp.int32(caps[0][0])
    for n in range(1, len(caps)):
        limit = jnp.where(sizes[0] >= n, caps[n][0], limit)

    @pl.loop(used // 16, limit // 16)
    def _(n):
        blank = pl.ds(pl.multiple_of(n * 16, 16), 16)
        for q in range(owners):
            ret[q, blank, :] = jnp.zeros((16, width), BF16)

    @pl.loop(0, steps)
    def _(t):
        r, f, n = t // NF, t % NF, (t + steps - NF) % RING
        e = plan[0, r]

        @pl.when(t >= RING)
        def _():
            for c in weights(t):
                c.wait()

        for size in (16, 32, slots):
            m = size * (owners - 2)

            @pl.when(plan[1, r] == size)
            def _():
                x = rows[e, 2:owners, 0:size, :].reshape(m, width)
                for c in range(0, ft, 256):
                    gate = jnp.dot(x, w1b[n, :, c:c + 256], preferred_element_type=F32)
                    up = jnp.dot(x, w3b[n, :, c:c + 256], preferred_element_type=F32)
                    mid[0:m, c:c + 256] = (gate * jax.nn.sigmoid(gate) * up).astype(BF16)
                for c in range(0, width, 512):
                    part = jnp.dot(mid[0:m, :], w2b[n, :, c:c + 512], preferred_element_type=F32)
                    yacc[0:m, c:c + 512] = jnp.where(f == 0, 0.0, yacc[0:m, c:c + 512]) + part

                @pl.when(f == NF - 1)
                def _():
                    first = pl.multiple_of(plan[2, r], 16)
                    for q in (0, 1):
                        ret[q, pl.ds(first, size), :] = y_own[e, q, 0:size, :]
                    for q in range(2, owners):
                        ret[q, pl.ds(first, size), :] = yacc[(q - 2) * size:(q - 1) * size, :].astype(BF16)

        @pl.when(t + RING < steps)
        def _():
            for c in weights(t + RING):
                c.start()


def expert_call(sizes, rows, y_own, w1p, w3p, w2p, w1, w3, w2, caps):
    local, owners, slots, width = rows.shape
    ft = w1p.shape[2]
    hbm = pl.BlockSpec(memory_space=pl.ANY)
    vmem = pl.BlockSpec(memory_space=pltpu.VMEM)
    flops = 3 * 2 * local * slots * owners * width * ft * NF // 2
    return pl.pallas_call(
        functools.partial(expert_kernel, caps),
        name='experts',
        out_shape=(
            pltpu.VMEM((owners, caps[-1][0], width), BF16),
            pltpu.VMEM(w1p.shape, BF16),
            pltpu.VMEM(w3p.shape, BF16),
            pltpu.VMEM(w2p.shape, BF16),
        ),
        in_specs=[pl.BlockSpec(memory_space=pltpu.SMEM), vmem, vmem, vmem, vmem, vmem, hbm, hbm, hbm],
        out_specs=(vmem, vmem, vmem, vmem),
        input_output_aliases={3: 1, 4: 2, 5: 3},
        scratch_shapes=[
            pltpu.VMEM(((owners - 2) * slots, ft), BF16),
            pltpu.VMEM(((owners - 2) * slots, width), F32),
            pltpu.SMEM((3, local), I32),
            pltpu.SemaphoreType.DMA((RING, 3)),
        ],
        compiler_params=pltpu.CompilerParams(vmem_limit_bytes=12 * 1024 * 1024),
        cost_estimate=pl.CostEstimate(flops=flops, bytes_accessed=3 * 2 * local * width * ft * NF, transcendentals=0),
    )(sizes, rows, y_own, w1p, w3p, w2p, w1, w3, w2)[0]


REMOTE = (2, 4, 6)


def return_kernel(cap, chip_cap, ret, tok, goal, hid, scale, out, half, pack, got, acc, send, recv, half_send, half_recv):
    me = lax.axis_index('ep')
    tokens, width = hid.shape
    lanes = goal.shape[1] // 2
    barrier = pltpu.get_barrier_semaphore()
    for q in (1, *REMOTE):
        pl.semaphore_signal(barrier, inc=1, device_id=dev(flip(me, q)), device_id_type=MESH)
    pl.semaphore_wait(barrier, 1 + len(REMOTE))
    halves, copies = {}, {}
    for q in (*REMOTE, 0):
        halves[q] = pltpu.make_async_remote_copy(src_ref=ret.at[q + 1, pl.ds(0, cap)], dst_ref=half.at[q // 2], send_sem=half_send.at[q // 2], recv_sem=half_recv.at[q // 2], device_id=dev(flip(me, 1)), device_id_type=MESH)
        halves[q].start()

    for q in REMOTE:
        row = iota((chip_cap, cap), 0).astype(F32)
        mine = (row == goal[q:q + 1, 0:cap]).astype(F32).astype(BF16)
        theirs = (row == goal[q:q + 1, lanes:lanes + cap]).astype(F32).astype(BF16)
        halves[q].wait_recv()
        for c in range(0, width, 512):
            part = jnp.dot(mine, ret[q, 0:cap, c:c + 512], preferred_element_type=F32)
            part = part + jnp.dot(theirs, half[q // 2, :, c:c + 512], preferred_element_type=F32)
            pack[q // 2 - 1, :, c:c + 512] = part.astype(BF16)
        copies[q] = pltpu.make_async_remote_copy(src_ref=pack.at[q // 2 - 1], dst_ref=got.at[q // 2 - 1], send_sem=send.at[q // 2 - 1], recv_sem=recv.at[q // 2 - 1], device_id=dev(flip(me, q)), device_id_type=MESH)
        copies[q].start()

    table = tok[...]

    def chosen(column, peer, at, count):
        lane = iota((tokens, count), 1).astype(F32)
        return jnp.concatenate([((column[k] == peer) & (table[:, at + k:at + k + 1] == lane)).astype(F32) for k in (0, 1)], axis=0).astype(BF16)

    owner = [table[:, 2 + k:3 + k] for k in (0, 1)]
    chip = [jnp.floor(o * 0.5) for o in owner]

    def add(pick, block, fresh):
        for c in range(0, width, 512):
            part = jnp.dot(pick, block(c), preferred_element_type=F32)
            acc[:, c:c + 512] = part if fresh else acc[:, c:c + 512] + part

    add(chosen(owner, me.astype(F32), 4, cap), lambda c: ret[0, 0:cap, c:c + 512], True)
    pick = chosen(owner, flip(me, 1).astype(F32), 4, cap)
    halves[0].wait_recv()
    add(pick, lambda c: half[0, :, c:c + 512], False)
    for q in REMOTE:
        pick = chosen(chip, (flip(me, q) // 2).astype(F32), 6, chip_cap)
        copies[q].wait_recv()
        add(pick, lambda c: got[q // 2 - 1, :, c:c + 512], False)

    mixed = table[:, 0:1] * acc[0:tokens] + table[:, 1:2] * acc[tokens:2 * tokens]
    out[...] = (scale[0] * hid[...].astype(F32) + scale[1] * mixed).astype(BF16)
    for copy in (*halves.values(), *copies.values()):
        copy.wait_send()


def return_call(n, caps, ret, tok, goal, hidden, scale):
    owners, _, width = ret.shape
    tokens = hidden.shape[0]
    cap, chip_cap = caps
    vmem = pl.BlockSpec(memory_space=pltpu.VMEM)
    return pl.pallas_call(
        functools.partial(return_kernel, cap, chip_cap),
        name=f'return_{cap}_{chip_cap}',
        out_shape=jax.ShapeDtypeStruct((tokens, width), BF16),
        in_specs=[vmem, vmem, vmem, vmem, pl.BlockSpec(memory_space=pltpu.SMEM)],
        out_specs=vmem,
        scratch_shapes=[
            pltpu.VMEM((owners // 2, cap, width), BF16),
            pltpu.VMEM((len(REMOTE), chip_cap, width), BF16),
            pltpu.VMEM((len(REMOTE), chip_cap, width), BF16),
            pltpu.VMEM((2 * tokens, width), F32),
            pltpu.SemaphoreType.DMA((len(REMOTE),)),
            pltpu.SemaphoreType.DMA((len(REMOTE),)),
            pltpu.SemaphoreType.DMA((owners // 2,)),
            pltpu.SemaphoreType.DMA((owners // 2,)),
        ],
        compiler_params=pltpu.CompilerParams(collective_id=1 + n, has_side_effects=True, vmem_limit_bytes=24 * 1024 * 1024),
    )(ret, tok, goal, hidden, scale)


def capacities(local, slots):
    full = [slots * n + 16 * (local - n) for n in range(1, local + 1)]
    chip = [2 * slots + 8 + (slots - 8) * n for n in range(local - 1)] + [5 * slots]
    return (*zip(full, chip), (local * slots, 2 * local * slots))


def solution(mesh):
    owners = mesh.shape['ep']

    def local_step(hidden, router_w, expert_ids, w_gate, w_up, w_down, post_scale):
        tokens = hidden.shape[0]
        local = w_gate.shape[0]
        slots = tokens // max(1, local * owners // 8)
        caps = capacities(local, slots)
        rows, y_own, tok, goal, sizes, w1p, w3p, w2p = gather_call(hidden, expert_ids.T, router_w.T, w_gate, w_up, w_down, owners, caps)
        ret = expert_call(sizes, rows, y_own, w1p, w3p, w2p, w_gate, w_up, w_down, caps)
        branches = [functools.partial(return_call, n, cap) for n, cap in enumerate(caps)]
        return lax.switch(sizes[0], branches, ret, tok, goal, hidden, post_scale)

    tok_spec = P(('dp', 'ep'))
    return jax.shard_map(local_step, mesh=mesh, in_specs=(tok_spec, P(), tok_spec, P('ep'), P('ep'), P('ep'), P()), out_specs=tok_spec, check_vma=False)
```

```python
import functools

import jax
import jax.numpy as jnp
from jax import lax
from jax.experimental import pallas as pl
from jax.experimental.pallas import tpu as pltpu
from jax.sharding import PartitionSpec as P

MESH = pl.DeviceIdType.MESH
F32, BF16, I32 = jnp.float32, jnp.bfloat16, jnp.int32
NT = (((1,), (1,)), ((), ()))


def flip(idx, mask):
    out = idx
    for bit in (1, 2, 4):
        if mask & bit:
            out = out + bit - 2 * bit * ((idx // bit) % 2)
    return out


def dev(idx):
    return (lax.axis_index('dp'), idx)


def iota(shape, dim):
    return lax.broadcasted_iota(I32, shape, dim)


def weight_copies(w1, w3, w2, w1b, w3b, w2b, sem, e, f, n):
    ft = w1b.shape[2]
    cols = pl.ds(pl.multiple_of(f * ft, ft), ft)
    return (
        pltpu.make_async_copy(w1.at[e, :, cols], w1b.at[n], sem.at[n, 0]),
        pltpu.make_async_copy(w3.at[e, :, cols], w3b.at[n], sem.at[n, 1]),
        pltpu.make_async_copy(w2.at[e, cols, :], w2b.at[n], sem.at[n, 2]),
    )


def ffn_part(x, w1b, w3b, w2b, n, mid, yacc, fresh, m):
    for c in range(0, w1b.shape[2], 256):
        gate = jnp.dot(x, w1b[n, :, c:c + 256], preferred_element_type=F32)
        up = jnp.dot(x, w3b[n, :, c:c + 256], preferred_element_type=F32)
        mid[0:m, c:c + 256] = (gate * jax.nn.sigmoid(gate) * up).astype(BF16)
    for c in range(0, w2b.shape[2], 512):
        part = jnp.dot(mid[0:m, :], w2b[n, :, c:c + 512], preferred_element_type=F32)
        yacc[0:m, c:c + 512] = jnp.where(fresh, 0.0, yacc[0:m, c:c + 512]) + part


CHUNKS = 4
NF = 3
RING = 4
LATE_RING = 2
LATE = 2


def gather_kernel(caps, hid_in, ids_in, wrt_in, w1, w3, w2, near, far, y_own, tok, goal, plan, w1p, w3p, w2p, hid, ids, wrt, pos, mid, yacc, land, ids_all, send, recv, id_send, id_recv, wsem, in_sem):
    me = lax.axis_index('ep')
    own = [pltpu.make_async_copy(src, dst, in_sem.at[n]) for n, (src, dst) in enumerate(((hid_in, hid), (ids_in, ids), (wrt_in, wrt)))]
    for c in own:
        c.start()
    local, _, slots, _ = near.shape
    owners = 2 + far.shape[1]
    steps = (local - LATE) * NF

    def weights(t):
        return weight_copies(w1, w3, w2, w1p, w3p, w2p, wsem, local - 1 - t // NF, t % NF, t % RING)

    for t in range(RING):
        for c in weights(t):
            c.start()
    tokens, width = hid.shape
    experts = wrt.shape[0]
    rows = tokens // CHUNKS
    barrier = pltpu.get_barrier_semaphore()
    for q in range(1, owners):
        pl.semaphore_signal(barrier, inc=1, device_id=dev(flip(me, q)), device_id_type=MESH)
    pl.semaphore_wait(barrier, owners - 1)
    own[0].wait()
    own[1].wait()

    def piece(q, c):
        return (hid if q == 0 else land.at[q]).at[pl.ds(c * rows, rows)]

    def remote(q, c, n, to):
        return pltpu.make_async_remote_copy(src_ref=piece(q, c), dst_ref=land.at[q ^ to, pl.ds(c * rows, rows)], send_sem=send.at[n], recv_sem=recv.at[n], device_id=dev(flip(me, to)), device_id_type=MESH)

    id_copies = []
    for q in range(1, owners):
        id_copies.append(pltpu.make_async_remote_copy(src_ref=ids, dst_ref=ids_all.at[q], send_sem=id_send.at[q], recv_sem=id_recv.at[q], device_id=dev(flip(me, q)), device_id_type=MESH))
    for c in id_copies:
        c.start()
    x_order, y_order = (0, 1, 2, 3), (2, 3, 0, 1)
    to_x = {c: remote(0, c, c, 2) for c in x_order}
    to_y = {c: remote(0, c, 4 + c, 4) for c in y_order}
    for cx, cy in zip(x_order, y_order):
        to_x[cx].start()
        to_y[cy].start()
    to_mate = pltpu.make_async_remote_copy(src_ref=hid, dst_ref=land.at[1], send_sem=send.at[24], recv_sem=recv.at[24], device_id=dev(flip(me, 1)), device_id_type=MESH)
    to_mate.start()

    own[2].wait()
    h = hid[...]
    w = wrt[...]
    w_hi = w.astype(BF16)
    rest = w - w_hi.astype(F32)
    w_mid = rest.astype(BF16)
    w_lo = (rest - w_mid.astype(F32)).astype(BF16)
    dot = functools.partial(lax.dot_general, dimension_numbers=NT, preferred_element_type=F32)
    logits = dot(h, w_hi) + (dot(h, w_mid) + dot(h, w_lo))
    ex = jnp.exp(logits - jnp.max(logits, axis=1, keepdims=True))
    prob = ex / jnp.sum(ex, axis=1, keepdims=True)
    ta, tb = iota((tokens, tokens), 0), iota((tokens, tokens), 1)
    eye = (ta == tb).astype(F32).astype(BF16)
    own_ids = ids[...].astype(F32)
    lane = iota((tokens, experts), 1).astype(F32)
    id_col = [dot(eye, jnp.broadcast_to(own_ids[k:k + 1], (8, tokens)).astype(BF16))[:, 0:1] for k in (0, 1)]
    pick = [(id_col[k] == lane).astype(F32) for k in (0, 1)]
    g = [jnp.sum(pick[k] * prob, axis=1, keepdims=True) for k in (0, 1)]
    total = g[0] + g[1]

    for c in id_copies:
        c.wait_recv()
    ids_all[0] = ids[...]
    counts = []
    for q in range(owners):
        both = ids_all[q]
        e_col = iota((experts, tokens), 0)
        hot = ((both[0:1] == e_col) | (both[1:2] == e_col)).astype(F32).astype(BF16)
        counts.append(dot(jnp.ones((8, tokens), BF16), hot))
    most = functools.reduce(jnp.maximum, counts)
    count = jnp.concatenate([c[0:1] for c in counts], axis=0)
    stride = jnp.where(most > 32.0, float(slots), jnp.where(most > 16.0, 32.0, 16.0))
    mark = lambda mask: mask.astype(F32).astype(BF16)
    plain = functools.partial(jnp.dot, preferred_element_type=F32)
    ea, eb = iota((experts, experts), 0), iota((experts, experts), 1)
    same, same_chip = ea // local == eb // local, ea // (2 * local) == eb // (2 * local)
    offset = plain(stride.astype(BF16), mark(same & (ea < eb)))
    need = jnp.max(plain(stride.astype(BF16), mark(same))).astype(I32)
    need_chip = jnp.max(plain(count.astype(BF16), mark(same_chip))).astype(I32)
    branch = jnp.int32(0)
    for limit, limit_chip in caps[:-1]:
        branch = branch + ((need > limit) | (need_chip > limit_chip)).astype(I32)
    plan[0] = branch
    rank = plain(mark(tb < ta), (pick[0] + pick[1]).astype(BF16))
    chip_first = plain(count.astype(BF16), mark(same_chip & (ea < eb)))[0:1]
    local_of = lane - jnp.floor(lane * (1.0 / local)) * local
    late_place = jnp.where(local_of < LATE, local_of * slots + rank, -1.0)
    late = [jnp.sum(pick[k] * late_place, axis=1, keepdims=True) for k in (0, 1)]
    slot = [jnp.sum(pick[k] * (rank + offset[0:1]), axis=1, keepdims=True) for k in (0, 1)]
    packed = [jnp.sum(pick[k] * (rank + chip_first), axis=1, keepdims=True) for k in (0, 1)]
    owner = [jnp.floor(id_col[k] * (1.0 / local)) for k in (0, 1)]
    wide = iota((tokens, 128), 1)
    table = jnp.zeros((tokens, 128), F32)
    for n, col in enumerate((g[0] / total, g[1] / total, *owner, *slot, *packed, *late)):
        table = jnp.where(wide == n, col, table)
    tok[...] = table

    e_row, n_col = iota((experts, 128), 0), iota((experts, 128), 1)
    e_of = jnp.where(n_col < local, me * local + n_col, flip(me, 1) * local + n_col - local)
    used = n_col < 2 * local
    held = plain(count.astype(BF16), mark(used & (e_row == e_of)))
    start = plain(count.astype(BF16), mark(used & (e_row // (2 * local) == me // 2) & (e_row < e_of)))
    base = plain(stride.astype(BF16), mark(used & (e_row // local == e_of // local) & (e_row < e_of)))
    base_size = plain(stride.astype(BF16), mark(used & (e_row == e_of)))
    lane_of = iota((owners, goal.shape[1]), 1)
    where_to = jnp.full((owners, goal.shape[1]), -1.0, F32)
    for n in range(2 * local):
        at = (lane_of - (n // local) * (goal.shape[1] // 2)).astype(F32) - base[0:1, n:n + 1]
        where_to = jnp.where((at >= 0.0) & (at < held[:, n:n + 1]), at + start[:, n:n + 1], where_to)
    goal[...] = where_to

    first, second = (jnp.concatenate([ids_all[q, k:k + 1] for q in range(owners)], axis=0) for k in (0, 1))
    marks = jnp.concatenate([((first == me * local + j) | (second == me * local + j)).astype(F32) for j in range(local)], axis=0)
    earlier = plain(marks.astype(BF16), (ta < tb).astype(F32).astype(BF16))
    pos[...] = jnp.where(marks > 0.5, earlier, -1.0)
    for j in range(local):
        plan[1 + j] = jnp.max(base_size[:, j:j + 1]).astype(I32)

    def pick_rows(q):
        at = iota((slots, tokens), 0).astype(F32)
        match = jnp.concatenate([(at == pos[j * owners + q:j * owners + q + 1, :]).astype(F32) for j in range(local)], axis=0).astype(BF16)

        @pl.loop(0, width // 512)
        def _(n):
            cols = pl.ds(pl.multiple_of(n * 512, 512), 512)
            block = hid[:, cols] if q == 0 else land[q, :, cols]
            part = jnp.dot(match, block, preferred_element_type=F32).astype(BF16)
            for j in range(local):
                to = near.at[j, q] if q < 2 else far.at[j, q - 2]
                to[:, cols] = part[j * slots:(j + 1) * slots]

    def own_steps(first, last):
        @pl.loop(first, last)
        def _(t):
            e, f, n = local - 1 - t // NF, t % NF, t % RING
            for c in weights(t):
                c.wait()
            x = near[e, :, :, :].reshape(2 * slots, width)
            ffn_part(x, w1p, w3p, w2p, n, mid, yacc, f == 0, 2 * slots)

            @pl.when(f == NF - 1)
            def _():
                for q in (0, 1):
                    y_own[e - LATE, q, :, :] = yacc[q * slots:(q + 1) * slots, :].astype(BF16)

            @pl.when(t + RING < steps)
            def _():
                for c in weights(t + RING):
                    c.start()

    sent = [*to_x.values(), *to_y.values(), to_mate]

    def pass_on(q, c, n, to):
        copy = remote(q, c, n, to)
        copy.start()
        sent.append(copy)
        return copy

    pick_rows(0)
    to_mate.wait_recv()
    pick_rows(1)
    across, mates = {}, {2: [], 4: [], 6: []}
    for n, (cx, cy) in enumerate(zip(x_order, y_order)):
        if n < 2:
            own_steps(n * steps // 2, (n + 1) * steps // 2)
        to_x[cx].wait_recv()
        if cx in (0, 1):
            across[cx] = pass_on(2, cx, 8 + cx, 4)
        mates[2].append(pass_on(2, cx, 12 + cx, 1))
        to_y[cy].wait_recv()
        if cy in (2, 3):
            across[cy] = pass_on(4, cy, 8 + cy, 2)
        mates[4].append(pass_on(4, cy, 16 + cy, 1))
    for q in (2, 4):
        pick_rows(q)
    for q in (2, 4):
        for m in mates[q]:
            m.wait_recv()
        pick_rows(q + 1)
    for c in (0, 2, 1, 3):
        across[c].wait_recv()
        mates[6].append(pass_on(6, c, 20 + c, 1))
    pick_rows(6)
    for m in mates[6]:
        m.wait_recv()
    pick_rows(7)
    for m in sent:
        m.wait_send()
    for c in id_copies:
        c.wait_send()


def gather_call(hidden, ids_t, wr_t, w1, w3, w2, owners, caps):
    tokens, width = hidden.shape
    experts = wr_t.shape[0]
    local, _, ffn = w1.shape
    slots = caps[-1][0] // local
    ft = ffn // NF
    vmem = pl.BlockSpec(memory_space=pltpu.VMEM)
    hbm = pl.BlockSpec(memory_space=pl.ANY)
    return pl.pallas_call(
        functools.partial(gather_kernel, caps),
        name='gather_tokens',
        out_shape=(
            pltpu.VMEM((local, 2, slots, width), BF16),
            pltpu.VMEM((local, owners - 2, slots, width), BF16),
            pltpu.VMEM((local - LATE, 2, slots, width), BF16),
            jax.ShapeDtypeStruct((tokens, 128), F32),
            jax.ShapeDtypeStruct((owners, 2 * local * slots), F32),
            jax.ShapeDtypeStruct((1 + local,), I32),
            pltpu.VMEM((RING, width, ft), BF16),
            pltpu.VMEM((RING, width, ft), BF16),
            pltpu.VMEM((RING, ft, width), BF16),
        ),
        in_specs=[hbm, *[pl.BlockSpec(memory_space=pltpu.HBM)] * 2, hbm, hbm, hbm],
        out_specs=(vmem, vmem, vmem, vmem, vmem, pl.BlockSpec(memory_space=pltpu.SMEM), vmem, vmem, vmem),
        scratch_shapes=[
            pltpu.VMEM((tokens, width), BF16),
            pltpu.VMEM((2, tokens), I32),
            pltpu.VMEM((experts, width), F32),
            pltpu.VMEM((local * owners, tokens), F32),
            pltpu.VMEM((2 * slots, ft), BF16),
            pltpu.VMEM((2 * slots, width), F32),
            pltpu.VMEM((owners, tokens, width), BF16),
            pltpu.VMEM((owners, 2, tokens), I32),
            pltpu.SemaphoreType.DMA((25,)),
            pltpu.SemaphoreType.DMA((25,)),
            pltpu.SemaphoreType.DMA((owners,)),
            pltpu.SemaphoreType.DMA((owners,)),
            pltpu.SemaphoreType.DMA((RING, 3)),
            pltpu.SemaphoreType.DMA((3,)),
        ],
        compiler_params=pltpu.CompilerParams(collective_id=0, has_side_effects=True, vmem_limit_bytes=13 * 1024 * 1024),
    )(hidden, *(pltpu.with_memory_space_constraint(x, pltpu.HBM) for x in (ids_t, wr_t)), w1, w3, w2)


def expert_kernel(caps, sizes, rows, y_own, _w1b, _w3b, _w2b, w1, w3, w2, ret, w1b, w3b, w2b, mid, yacc, plan, wsem):
    local, distant, slots, width = rows.shape
    owners = distant + 2
    steps = local * NF
    done = (local - LATE) * NF

    size = [sizes[1 + j] for j in range(local)]
    for j in range(local):
        rank = jnp.int32(j - LATE if j >= LATE else local - LATE)
        offset = jnp.int32(0)
        for i in range(local):
            if i < LATE and j < LATE and i != j:
                ahead = (size[i] >= size[j]) if i < j else (size[i] > size[j])
                rank = rank + ahead.astype(I32)
            if i < j:
                offset = offset + size[i]
        plan[0, rank] = jnp.int32(j)
        plan[1, rank] = size[j]
        plan[2, rank] = offset
    used = size[0]
    for j in range(1, local):
        used = used + size[j]

    def part_of(t):
        turn = jnp.where(t < NF, 0, 2 * NF - RING)
        return (t % NF + turn) % NF

    def weights(t):
        return weight_copies(w1, w3, w2, w1b, w3b, w2b, wsem, plan[0, t // NF], part_of(t), (t + done - NF) % RING)

    limit = jnp.int32(caps[0][0])
    for n in range(1, len(caps)):
        limit = jnp.where(sizes[0] >= n, caps[n][0], limit)

    @pl.loop(used // 16, limit // 16)
    def _(n):
        blank = pl.ds(pl.multiple_of(n * 16, 16), 16)
        for q in range(owners):
            ret[q, blank, :] = jnp.zeros((16, width), BF16)

    @pl.loop(0, steps)
    def _(t):
        r, f, n = t // NF, t % NF, (t + done - NF) % RING
        e = plan[0, r]

        @pl.when(t >= RING)
        def _():
            for c in weights(t):
                c.wait()

        for size in (16, 32, slots):
            m = size * distant

            @pl.when(plan[1, r] == size)
            def _():
                x = rows[e, :, 0:size, :].reshape(m, width)
                ffn_part(x, w1b, w3b, w2b, n, mid, yacc, f == 0, m)

                @pl.when(f == NF - 1)
                def _():
                    first = pl.multiple_of(plan[2, r], 16)
                    for q in (0, 1):
                        mine = y_own[jnp.maximum(e - LATE, 0), q, 0:size, :]
                        ret[q, pl.ds(first, size), :] = jnp.where(e >= LATE, mine, jnp.zeros_like(mine))
                    for q in range(2, owners):
                        ret[q, pl.ds(first, size), :] = yacc[(q - 2) * size:(q - 1) * size, :].astype(BF16)

        @pl.when(t + RING < steps)
        def _():
            for c in weights(t + RING):
                c.start()


def expert_call(sizes, rows, y_own, w1p, w3p, w2p, w1, w3, w2, caps):
    local, distant, slots, width = rows.shape
    owners = distant + 2
    ft = w1p.shape[2]
    hbm = pl.BlockSpec(memory_space=pl.ANY)
    vmem = pl.BlockSpec(memory_space=pltpu.VMEM)
    flops = 3 * 2 * local * slots * owners * width * ft * NF // 2
    return pl.pallas_call(
        functools.partial(expert_kernel, caps),
        name='experts',
        out_shape=(
            pltpu.VMEM((owners, caps[-1][0], width), BF16),
            pltpu.VMEM(w1p.shape, BF16),
            pltpu.VMEM(w3p.shape, BF16),
            pltpu.VMEM(w2p.shape, BF16),
        ),
        in_specs=[pl.BlockSpec(memory_space=pltpu.SMEM), vmem, vmem, vmem, vmem, vmem, hbm, hbm, hbm],
        out_specs=(vmem, vmem, vmem, vmem),
        input_output_aliases={3: 1, 4: 2, 5: 3},
        scratch_shapes=[
            pltpu.VMEM((distant * slots, ft), BF16),
            pltpu.VMEM((distant * slots, width), F32),
            pltpu.SMEM((3, local), I32),
            pltpu.SemaphoreType.DMA((RING, 3)),
        ],
        compiler_params=pltpu.CompilerParams(vmem_limit_bytes=12 * 1024 * 1024),
        cost_estimate=pl.CostEstimate(flops=flops, bytes_accessed=3 * 2 * local * width * ft * NF, transcendentals=0),
    )(sizes, rows, y_own, w1p, w3p, w2p, w1, w3, w2)[0]


REMOTE = (2, 4, 6)


def return_kernel(cap, chip_cap, ret, near, tok, goal, hid, scale, w1, w3, w2, out, half, pack, got, acc, late, late_half, mid, yacc, w1b, w3b, w2b, send, recv, half_send, half_recv, wsem):
    me = lax.axis_index('ep')
    slots = near.shape[2]
    steps = LATE * NF

    def weights(t):
        return weight_copies(w1, w3, w2, w1b, w3b, w2b, wsem, t // NF, t % NF, t % LATE_RING)

    for t in range(LATE_RING):
        for c in weights(t):
            c.start()
    tokens, width = hid.shape
    lanes = goal.shape[1] // 2
    barrier = pltpu.get_barrier_semaphore()
    for q in (1, *REMOTE):
        pl.semaphore_signal(barrier, inc=1, device_id=dev(flip(me, q)), device_id_type=MESH)
    pl.semaphore_wait(barrier, 1 + len(REMOTE))
    halves, copies = {}, {}
    for q in (*REMOTE, 0):
        halves[q] = pltpu.make_async_remote_copy(src_ref=ret.at[q + 1, pl.ds(0, cap)], dst_ref=half.at[q // 2], send_sem=half_send.at[q // 2], recv_sem=half_recv.at[q // 2], device_id=dev(flip(me, 1)), device_id_type=MESH)
        halves[q].start()

    for q in REMOTE:
        row = iota((chip_cap, cap), 0).astype(F32)
        mine = (row == goal[q:q + 1, 0:cap]).astype(F32).astype(BF16)
        theirs = (row == goal[q:q + 1, lanes:lanes + cap]).astype(F32).astype(BF16)
        halves[q].wait_recv()
        for c in range(0, width, 512):
            part = jnp.dot(mine, ret[q, 0:cap, c:c + 512], preferred_element_type=F32)
            part = part + jnp.dot(theirs, half[q // 2, :, c:c + 512], preferred_element_type=F32)
            pack[q // 2 - 1, :, c:c + 512] = part.astype(BF16)
        copies[q] = pltpu.make_async_remote_copy(src_ref=pack.at[q // 2 - 1], dst_ref=got.at[q // 2 - 1], send_sem=send.at[q // 2 - 1], recv_sem=recv.at[q // 2 - 1], device_id=dev(flip(me, q)), device_id_type=MESH)
        copies[q].start()

    table = tok[...]

    def chosen(column, peer, at, count):
        lane = iota((tokens, count), 1).astype(F32)
        return jnp.concatenate([((column[k] == peer) & (table[:, at + k:at + k + 1] == lane)).astype(F32) for k in (0, 1)], axis=0).astype(BF16)

    owner = [table[:, 2 + k:3 + k] for k in (0, 1)]
    chip = [jnp.floor(o * 0.5) for o in owner]

    def add(pick, block, fresh):
        for c in range(0, width, 512):
            part = jnp.dot(pick, block(c), preferred_element_type=F32)
            acc[:, c:c + 512] = part if fresh else acc[:, c:c + 512] + part

    add(chosen(owner, me.astype(F32), 4, cap), lambda c: ret[0, 0:cap, c:c + 512], True)
    pick = chosen(owner, flip(me, 1).astype(F32), 4, cap)
    halves[0].wait_recv()
    add(pick, lambda c: half[0, :, c:c + 512], False)

    @pl.loop(0, steps)
    def _(t):
        e, f, n = t // NF, t % NF, t % LATE_RING
        for c in weights(t):
            c.wait()
        ffn_part(near[e, :, :, :].reshape(2 * slots, width), w1b, w3b, w2b, n, mid, yacc, f == 0, 2 * slots)

        @pl.when(f == NF - 1)
        def _():
            for q in (0, 1):
                late[q, pl.ds(pl.multiple_of(e * slots, slots), slots), :] = yacc[q * slots:(q + 1) * slots, :].astype(BF16)

        @pl.when(t + LATE_RING < steps)
        def _():
            for c in weights(t + LATE_RING):
                c.start()

    swap = pltpu.make_async_remote_copy(src_ref=late.at[1], dst_ref=late_half, send_sem=half_send.at[4], recv_sem=half_recv.at[4], device_id=dev(flip(me, 1)), device_id_type=MESH)
    swap.start()
    add(chosen(owner, me.astype(F32), 8, LATE * slots), lambda c: late[0, :, c:c + 512], False)
    pick = chosen(owner, flip(me, 1).astype(F32), 8, LATE * slots)
    swap.wait_recv()
    add(pick, lambda c: late_half[:, c:c + 512], False)
    for q in REMOTE:
        pick = chosen(chip, (flip(me, q) // 2).astype(F32), 6, chip_cap)
        copies[q].wait_recv()
        add(pick, lambda c: got[q // 2 - 1, :, c:c + 512], False)

    mixed = table[:, 0:1] * acc[0:tokens] + table[:, 1:2] * acc[tokens:2 * tokens]
    out[...] = (scale[0] * hid[...].astype(F32) + scale[1] * mixed).astype(BF16)
    for copy in (*halves.values(), *copies.values(), swap):
        copy.wait_send()


def return_call(n, caps, ret, near, tok, goal, hidden, scale, w1, w3, w2):
    owners, _, width = ret.shape
    slots, ft = near.shape[2], w1.shape[2] // NF
    tokens = hidden.shape[0]
    cap, chip_cap = caps
    vmem = pl.BlockSpec(memory_space=pltpu.VMEM)
    return pl.pallas_call(
        functools.partial(return_kernel, cap, chip_cap),
        name=f'return_{cap}_{chip_cap}',
        out_shape=jax.ShapeDtypeStruct((tokens, width), BF16),
        in_specs=[vmem, vmem, vmem, vmem, vmem, pl.BlockSpec(memory_space=pltpu.SMEM), *[pl.BlockSpec(memory_space=pl.ANY)] * 3],
        out_specs=vmem,
        scratch_shapes=[
            pltpu.VMEM((owners // 2, cap, width), BF16),
            pltpu.VMEM((len(REMOTE), chip_cap, width), BF16),
            pltpu.VMEM((len(REMOTE), chip_cap, width), BF16),
            pltpu.VMEM((2 * tokens, width), F32),
            pltpu.VMEM((2, LATE * slots, width), BF16),
            pltpu.VMEM((LATE * slots, width), BF16),
            pltpu.VMEM((2 * slots, ft), BF16),
            pltpu.VMEM((2 * slots, width), F32),
            pltpu.VMEM((LATE_RING, width, ft), BF16),
            pltpu.VMEM((LATE_RING, width, ft), BF16),
            pltpu.VMEM((LATE_RING, ft, width), BF16),
            pltpu.SemaphoreType.DMA((len(REMOTE),)),
            pltpu.SemaphoreType.DMA((len(REMOTE),)),
            pltpu.SemaphoreType.DMA((owners // 2 + 1,)),
            pltpu.SemaphoreType.DMA((owners // 2 + 1,)),
            pltpu.SemaphoreType.DMA((LATE_RING, 3)),
        ],
        compiler_params=pltpu.CompilerParams(collective_id=1 + n, has_side_effects=True, vmem_limit_bytes=34 * 1024 * 1024),
    )(ret, near, tok, goal, hidden, scale, w1, w3, w2)


def capacities(local, slots):
    full = [slots * n + 16 * (local - n) for n in range(1, local + 1)]
    chip = [2 * slots + 8 + (slots - 8) * n for n in range(local - 1)]
    return (*zip(full, chip), (local * slots, 2 * local * slots))


def solution(mesh):
    owners = mesh.shape['ep']

    def local_step(hidden, router_w, expert_ids, w_gate, w_up, w_down, post_scale):
        tokens = hidden.shape[0]
        local = w_gate.shape[0]
        slots = tokens // max(1, local * owners // 8)
        caps = capacities(local, slots)
        near, far, y_own, tok, goal, sizes, w1p, w3p, w2p = gather_call(hidden, expert_ids.T, router_w.T, w_gate, w_up, w_down, owners, caps)
        ret = expert_call(sizes, far, y_own, w1p, w3p, w2p, w_gate, w_up, w_down, caps)
        branches = [functools.partial(return_call, n, cap) for n, cap in enumerate(caps)]
        return lax.switch(sizes[0], branches, ret, near, tok, goal, hidden, post_scale, w_gate, w_up, w_down)

    tok_spec = P(('dp', 'ep'))
    return jax.shard_map(local_step, mesh=mesh, in_specs=(tok_spec, P(), tok_spec, P('ep'), P('ep'), P('ep'), P()), out_specs=tok_spec, check_vma=False)
```

```python
import functools

import jax
import jax.numpy as jnp
from jax import lax
from jax.experimental import pallas as pl
from jax.experimental.pallas import tpu as pltpu
from jax.sharding import PartitionSpec as P

MESH = pl.DeviceIdType.MESH
F32, BF16, I32 = jnp.float32, jnp.bfloat16, jnp.int32
NT = (((1,), (1,)), ((), ()))


def flip(idx, mask):
    out = idx
    for bit in (1, 2, 4):
        if mask & bit:
            out = out + bit - 2 * bit * ((idx // bit) % 2)
    return out


def dev(idx):
    return (lax.axis_index('dp'), idx)


def iota(shape, dim):
    return lax.broadcasted_iota(I32, shape, dim)


def weight_copies(w1, w3, w2, w1b, w3b, w2b, sem, e, f, n):
    ft = w1b.shape[2]
    cols = pl.ds(pl.multiple_of(f * ft, ft), ft)
    return (
        pltpu.make_async_copy(w1.at[e, :, cols], w1b.at[n], sem.at[n, 0]),
        pltpu.make_async_copy(w3.at[e, :, cols], w3b.at[n], sem.at[n, 1]),
        pltpu.make_async_copy(w2.at[e, cols, :], w2b.at[n], sem.at[n, 2]),
    )


def ffn_part(x, w1b, w3b, w2b, n, mid, yacc, fresh, m):
    for c in range(0, w1b.shape[2], 256):
        gate = jnp.dot(x, w1b[n, :, c:c + 256], preferred_element_type=F32)
        up = jnp.dot(x, w3b[n, :, c:c + 256], preferred_element_type=F32)
        mid[0:m, c:c + 256] = (gate * jax.nn.sigmoid(gate) * up).astype(BF16)
    for c in range(0, w2b.shape[2], 512):
        part = jnp.dot(mid[0:m, :], w2b[n, :, c:c + 512], preferred_element_type=F32)
        yacc[0:m, c:c + 512] = jnp.where(fresh, 0.0, yacc[0:m, c:c + 512]) + part


CHUNKS = 4
NF = 3
RING = 4
LATE_RING = 2
LATE = 2


def gather_kernel(caps, hid_in, ids_in, wrt_in, w1, w3, w2, near, far, y_own, tok, goal, plan, w1p, w3p, w2p, hid, ids, wrt, pos, mid, yacc, land, ids_all, send, recv, id_send, id_recv, wsem, in_sem):
    me = lax.axis_index('ep')
    own = [pltpu.make_async_copy(src, dst, in_sem.at[n]) for n, (src, dst) in enumerate(((hid_in, hid), (ids_in, ids), (wrt_in, wrt)))]
    for c in own:
        c.start()
    local, _, slots, _ = near.shape
    owners = 2 + far.shape[1]
    steps = (local - LATE) * NF

    def weights(t):
        return weight_copies(w1, w3, w2, w1p, w3p, w2p, wsem, local - 1 - t // NF, t % NF, t % RING)

    tokens, width = hid.shape
    experts = wrt.shape[0]
    rows = tokens // CHUNKS
    barrier = pltpu.get_barrier_semaphore()
    for q in range(1, owners):
        pl.semaphore_signal(barrier, inc=1, device_id=dev(flip(me, q)), device_id_type=MESH)
    pl.semaphore_wait(barrier, owners - 1)
    own[0].wait()
    own[1].wait()

    def piece(q, c):
        return (hid if q == 0 else land.at[q]).at[pl.ds(c * rows, rows)]

    def remote(q, c, n, to):
        return pltpu.make_async_remote_copy(src_ref=piece(q, c), dst_ref=land.at[q ^ to, pl.ds(c * rows, rows)], send_sem=send.at[n], recv_sem=recv.at[n], device_id=dev(flip(me, to)), device_id_type=MESH)

    id_copies = []
    for q in range(1, owners):
        id_copies.append(pltpu.make_async_remote_copy(src_ref=ids, dst_ref=ids_all.at[q], send_sem=id_send.at[q], recv_sem=id_recv.at[q], device_id=dev(flip(me, q)), device_id_type=MESH))
    for c in id_copies:
        c.start()
    x_order, y_order = (0, 1, 2, 3), (2, 3, 0, 1)
    to_x = {c: remote(0, c, c, 2) for c in x_order}
    to_y = {c: remote(0, c, 4 + c, 4) for c in y_order}
    for cx, cy in zip(x_order, y_order):
        to_x[cx].start()
        to_y[cy].start()
    to_mate = pltpu.make_async_remote_copy(src_ref=hid, dst_ref=land.at[1], send_sem=send.at[24], recv_sem=recv.at[24], device_id=dev(flip(me, 1)), device_id_type=MESH)
    to_mate.start()
    for t in range(RING):
        for c in weights(t):
            c.start()

    own[2].wait()
    h = hid[...]
    w = wrt[...]
    w_hi = w.astype(BF16)
    rest = w - w_hi.astype(F32)
    w_mid = rest.astype(BF16)
    w_lo = (rest - w_mid.astype(F32)).astype(BF16)
    dot = functools.partial(lax.dot_general, dimension_numbers=NT, preferred_element_type=F32)
    logits = dot(h, w_hi) + (dot(h, w_mid) + dot(h, w_lo))
    ex = jnp.exp(logits - jnp.max(logits, axis=1, keepdims=True))
    prob = ex / jnp.sum(ex, axis=1, keepdims=True)
    ta, tb = iota((tokens, tokens), 0), iota((tokens, tokens), 1)
    eye = (ta == tb).astype(F32).astype(BF16)
    own_ids = ids[...].astype(F32)
    lane = iota((tokens, experts), 1).astype(F32)
    id_col = [dot(eye, jnp.broadcast_to(own_ids[k:k + 1], (8, tokens)).astype(BF16))[:, 0:1] for k in (0, 1)]
    pick = [(id_col[k] == lane).astype(F32) for k in (0, 1)]
    g = [jnp.sum(pick[k] * prob, axis=1, keepdims=True) for k in (0, 1)]
    total = g[0] + g[1]

    for c in id_copies:
        c.wait_recv()
    ids_all[0] = ids[...]
    counts = []
    for q in range(owners):
        both = ids_all[q]
        e_col = iota((experts, tokens), 0)
        hot = ((both[0:1] == e_col) | (both[1:2] == e_col)).astype(F32).astype(BF16)
        counts.append(dot(jnp.ones((8, tokens), BF16), hot))
    most = functools.reduce(jnp.maximum, counts)
    count = jnp.concatenate([c[0:1] for c in counts], axis=0)
    stride = jnp.where(most > 32.0, float(slots), jnp.where(most > 16.0, 32.0, 16.0))
    mark = lambda mask: mask.astype(F32).astype(BF16)
    plain = functools.partial(jnp.dot, preferred_element_type=F32)
    ea, eb = iota((experts, experts), 0), iota((experts, experts), 1)
    same, same_chip = ea // local == eb // local, ea // (2 * local) == eb // (2 * local)
    offset = plain(stride.astype(BF16), mark(same & (ea < eb)))
    need = jnp.max(plain(stride.astype(BF16), mark(same))).astype(I32)
    need_chip = jnp.max(plain(count.astype(BF16), mark(same_chip))).astype(I32)
    branch = jnp.int32(0)
    for limit, limit_chip in caps[:-1]:
        branch = branch + ((need > limit) | (need_chip > limit_chip)).astype(I32)
    plan[0] = branch
    rank = plain(mark(tb < ta), (pick[0] + pick[1]).astype(BF16))
    chip_first = plain(count.astype(BF16), mark(same_chip & (ea < eb)))[0:1]
    local_of = lane - jnp.floor(lane * (1.0 / local)) * local
    late_place = jnp.where(local_of < LATE, local_of * slots + rank, -1.0)
    late = [jnp.sum(pick[k] * late_place, axis=1, keepdims=True) for k in (0, 1)]
    slot = [jnp.sum(pick[k] * (rank + offset[0:1]), axis=1, keepdims=True) for k in (0, 1)]
    packed = [jnp.sum(pick[k] * (rank + chip_first), axis=1, keepdims=True) for k in (0, 1)]
    owner = [jnp.floor(id_col[k] * (1.0 / local)) for k in (0, 1)]
    wide = iota((tokens, 128), 1)
    table = jnp.zeros((tokens, 128), F32)
    for n, col in enumerate((g[0] / total, g[1] / total, *owner, *slot, *packed, *late)):
        table = jnp.where(wide == n, col, table)
    tok[...] = table

    e_row, n_col = iota((experts, 128), 0), iota((experts, 128), 1)
    e_of = jnp.where(n_col < local, me * local + n_col, flip(me, 1) * local + n_col - local)
    used = n_col < 2 * local
    held = plain(count.astype(BF16), mark(used & (e_row == e_of)))
    start = plain(count.astype(BF16), mark(used & (e_row // (2 * local) == me // 2) & (e_row < e_of)))
    base = plain(stride.astype(BF16), mark(used & (e_row // local == e_of // local) & (e_row < e_of)))
    base_size = plain(stride.astype(BF16), mark(used & (e_row == e_of)))
    lane_of = iota((owners, goal.shape[1]), 1)
    where_to = jnp.full((owners, goal.shape[1]), -1.0, F32)
    for n in range(2 * local):
        at = (lane_of - (n // local) * (goal.shape[1] // 2)).astype(F32) - base[0:1, n:n + 1]
        where_to = jnp.where((at >= 0.0) & (at < held[:, n:n + 1]), at + start[:, n:n + 1], where_to)
    goal[...] = where_to

    first, second = (jnp.concatenate([ids_all[q, k:k + 1] for q in range(owners)], axis=0) for k in (0, 1))
    marks = jnp.concatenate([((first == me * local + j) | (second == me * local + j)).astype(F32) for j in range(local)], axis=0)
    earlier = plain(marks.astype(BF16), (ta < tb).astype(F32).astype(BF16))
    pos[...] = jnp.where(marks > 0.5, earlier, -1.0)
    for j in range(local):
        plan[1 + j] = jnp.max(base_size[:, j:j + 1]).astype(I32)

    def pick_rows(q):
        at = iota((slots, tokens), 0).astype(F32)
        match = jnp.concatenate([(at == pos[j * owners + q:j * owners + q + 1, :]).astype(F32) for j in range(local)], axis=0).astype(BF16)

        @pl.loop(0, width // 512)
        def _(n):
            cols = pl.ds(pl.multiple_of(n * 512, 512), 512)
            block = hid[:, cols] if q == 0 else land[q, :, cols]
            part = jnp.dot(match, block, preferred_element_type=F32).astype(BF16)
            for j in range(local):
                to = near.at[j, q] if q < 2 else far.at[j, q - 2]
                to[:, cols] = part[j * slots:(j + 1) * slots]

    def own_steps(first, last):
        @pl.loop(first, last)
        def _(t):
            e, f, n = local - 1 - t // NF, t % NF, t % RING
            for c in weights(t):
                c.wait()
            x = near[e, :, :, :].reshape(2 * slots, width)
            ffn_part(x, w1p, w3p, w2p, n, mid, yacc, f == 0, 2 * slots)

            @pl.when(f == NF - 1)
            def _():
                for q in (0, 1):
                    y_own[e - LATE, q, :, :] = yacc[q * slots:(q + 1) * slots, :].astype(BF16)

            @pl.when(t + RING < steps)
            def _():
                for c in weights(t + RING):
                    c.start()

    sent = [*to_x.values(), *to_y.values(), to_mate]

    def pass_on(q, c, n, to):
        copy = remote(q, c, n, to)
        copy.start()
        sent.append(copy)
        return copy

    pick_rows(0)
    to_mate.wait_recv()
    pick_rows(1)
    across, mates = {}, {2: [], 4: [], 6: []}
    for n, (cx, cy) in enumerate(zip(x_order, y_order)):
        if n < 2:
            own_steps(n * steps // 2, (n + 1) * steps // 2)
        to_x[cx].wait_recv()
        if cx in (0, 1):
            across[cx] = pass_on(2, cx, 8 + cx, 4)
        mates[2].append(pass_on(2, cx, 12 + cx, 1))
        to_y[cy].wait_recv()
        if cy in (2, 3):
            across[cy] = pass_on(4, cy, 8 + cy, 2)
        mates[4].append(pass_on(4, cy, 16 + cy, 1))
    for q in (2, 4):
        pick_rows(q)
    for q in (2, 4):
        for m in mates[q]:
            m.wait_recv()
        pick_rows(q + 1)
    for c in (0, 2, 1, 3):
        across[c].wait_recv()
        mates[6].append(pass_on(6, c, 20 + c, 1))
    pick_rows(6)
    for m in mates[6]:
        m.wait_recv()
    pick_rows(7)
    for m in sent:
        m.wait_send()
    for c in id_copies:
        c.wait_send()


def gather_call(hidden, ids_t, wr_t, w1, w3, w2, owners, caps):
    tokens, width = hidden.shape
    experts = wr_t.shape[0]
    local, _, ffn = w1.shape
    slots = caps[-1][0] // local
    ft = ffn // NF
    vmem = pl.BlockSpec(memory_space=pltpu.VMEM)
    hbm = pl.BlockSpec(memory_space=pl.ANY)
    return pl.pallas_call(
        functools.partial(gather_kernel, caps),
        name='gather_tokens',
        out_shape=(
            pltpu.VMEM((local, 2, slots, width), BF16),
            pltpu.VMEM((local, owners - 2, slots, width), BF16),
            pltpu.VMEM((local - LATE, 2, slots, width), BF16),
            jax.ShapeDtypeStruct((tokens, 128), F32),
            jax.ShapeDtypeStruct((owners, 2 * local * slots), F32),
            jax.ShapeDtypeStruct((1 + local,), I32),
            pltpu.VMEM((RING, width, ft), BF16),
            pltpu.VMEM((RING, width, ft), BF16),
            pltpu.VMEM((RING, ft, width), BF16),
        ),
        in_specs=[hbm, *[pl.BlockSpec(memory_space=pltpu.HBM)] * 2, hbm, hbm, hbm],
        out_specs=(vmem, vmem, vmem, vmem, vmem, pl.BlockSpec(memory_space=pltpu.SMEM), vmem, vmem, vmem),
        scratch_shapes=[
            pltpu.VMEM((tokens, width), BF16),
            pltpu.VMEM((2, tokens), I32),
            pltpu.VMEM((experts, width), F32),
            pltpu.VMEM((local * owners, tokens), F32),
            pltpu.VMEM((2 * slots, ft), BF16),
            pltpu.VMEM((2 * slots, width), F32),
            pltpu.VMEM((owners, tokens, width), BF16),
            pltpu.VMEM((owners, 2, tokens), I32),
            pltpu.SemaphoreType.DMA((25,)),
            pltpu.SemaphoreType.DMA((25,)),
            pltpu.SemaphoreType.DMA((owners,)),
            pltpu.SemaphoreType.DMA((owners,)),
            pltpu.SemaphoreType.DMA((RING, 3)),
            pltpu.SemaphoreType.DMA((3,)),
        ],
        compiler_params=pltpu.CompilerParams(collective_id=0, has_side_effects=True, vmem_limit_bytes=13 * 1024 * 1024),
    )(hidden, *(pltpu.with_memory_space_constraint(x, pltpu.HBM) for x in (ids_t, wr_t)), w1, w3, w2)


def expert_kernel(caps, sizes, rows, y_own, _w1b, _w3b, _w2b, w1, w3, w2, ret, w1b, w3b, w2b, mid, yacc, plan, wsem):
    local, distant, slots, width = rows.shape
    owners = distant + 2
    steps = local * NF
    done = (local - LATE) * NF

    size = [sizes[1 + j] for j in range(local)]
    for j in range(local):
        rank = jnp.int32(j - LATE if j >= LATE else local - LATE)
        offset = jnp.int32(0)
        for i in range(local):
            if i < LATE and j < LATE and i != j:
                ahead = (size[i] >= size[j]) if i < j else (size[i] > size[j])
                rank = rank + ahead.astype(I32)
            if i < j:
                offset = offset + size[i]
        plan[0, rank] = jnp.int32(j)
        plan[1, rank] = size[j]
        plan[2, rank] = offset
    used = size[0]
    for j in range(1, local):
        used = used + size[j]

    def part_of(t):
        turn = jnp.where(t < NF, 0, 2 * NF - RING)
        return (t % NF + turn) % NF

    def weights(t):
        return weight_copies(w1, w3, w2, w1b, w3b, w2b, wsem, plan[0, t // NF], part_of(t), (t + done - NF) % RING)

    limit = jnp.int32(caps[0][0])
    for n in range(1, len(caps)):
        limit = jnp.where(sizes[0] >= n, caps[n][0], limit)

    @pl.loop(used // 16, limit // 16)
    def _(n):
        blank = pl.ds(pl.multiple_of(n * 16, 16), 16)
        for q in range(owners):
            ret[q, blank, :] = jnp.zeros((16, width), BF16)

    @pl.loop(0, steps)
    def _(t):
        r, f, n = t // NF, t % NF, (t + done - NF) % RING
        e = plan[0, r]

        @pl.when(t >= RING)
        def _():
            for c in weights(t):
                c.wait()

        for size in (16, 32, slots):
            m = size * distant

            @pl.when(plan[1, r] == size)
            def _():
                x = rows[e, :, 0:size, :].reshape(m, width)
                ffn_part(x, w1b, w3b, w2b, n, mid, yacc, f == 0, m)

                @pl.when(f == NF - 1)
                def _():
                    first = pl.multiple_of(plan[2, r], 16)
                    for q in (0, 1):
                        mine = y_own[jnp.maximum(e - LATE, 0), q, 0:size, :]
                        ret[q, pl.ds(first, size), :] = jnp.where(e >= LATE, mine, jnp.zeros_like(mine))
                    for q in range(2, owners):
                        ret[q, pl.ds(first, size), :] = yacc[(q - 2) * size:(q - 1) * size, :].astype(BF16)

        @pl.when(t + RING < steps)
        def _():
            for c in weights(t + RING):
                c.start()


def expert_call(sizes, rows, y_own, w1p, w3p, w2p, w1, w3, w2, caps):
    local, distant, slots, width = rows.shape
    owners = distant + 2
    ft = w1p.shape[2]
    hbm = pl.BlockSpec(memory_space=pl.ANY)
    vmem = pl.BlockSpec(memory_space=pltpu.VMEM)
    flops = 3 * 2 * local * slots * owners * width * ft * NF // 2
    return pl.pallas_call(
        functools.partial(expert_kernel, caps),
        name='experts',
        out_shape=(
            pltpu.VMEM((owners, caps[-1][0], width), BF16),
            pltpu.VMEM(w1p.shape, BF16),
            pltpu.VMEM(w3p.shape, BF16),
            pltpu.VMEM(w2p.shape, BF16),
        ),
        in_specs=[pl.BlockSpec(memory_space=pltpu.SMEM), vmem, vmem, vmem, vmem, vmem, hbm, hbm, hbm],
        out_specs=(vmem, vmem, vmem, vmem),
        input_output_aliases={3: 1, 4: 2, 5: 3},
        scratch_shapes=[
            pltpu.VMEM((distant * slots, ft), BF16),
            pltpu.VMEM((distant * slots, width), F32),
            pltpu.SMEM((3, local), I32),
            pltpu.SemaphoreType.DMA((RING, 3)),
        ],
        compiler_params=pltpu.CompilerParams(vmem_limit_bytes=12 * 1024 * 1024),
        cost_estimate=pl.CostEstimate(flops=flops, bytes_accessed=3 * 2 * local * width * ft * NF, transcendentals=0),
    )(sizes, rows, y_own, w1p, w3p, w2p, w1, w3, w2)[0]


REMOTE = (2, 4, 6)


def return_kernel(cap, chip_cap, ret, near, tok, goal, hid, scale, w1, w3, w2, out, half, pack, got, acc, late, late_half, mid, yacc, w1b, w3b, w2b, send, recv, half_send, half_recv, wsem):
    me = lax.axis_index('ep')
    slots = near.shape[2]
    steps = LATE * NF

    def weights(t):
        return weight_copies(w1, w3, w2, w1b, w3b, w2b, wsem, t // NF, t % NF, t % LATE_RING)

    tokens, width = hid.shape
    lanes = goal.shape[1] // 2
    barrier = pltpu.get_barrier_semaphore()
    for q in (1, *REMOTE):
        pl.semaphore_signal(barrier, inc=1, device_id=dev(flip(me, q)), device_id_type=MESH)
    pl.semaphore_wait(barrier, 1 + len(REMOTE))
    halves, copies = {}, {}
    for q in (*REMOTE, 0):
        halves[q] = pltpu.make_async_remote_copy(src_ref=ret.at[q + 1, pl.ds(0, cap)], dst_ref=half.at[q // 2], send_sem=half_send.at[q // 2], recv_sem=half_recv.at[q // 2], device_id=dev(flip(me, 1)), device_id_type=MESH)
        halves[q].start()

    for q in REMOTE:
        row = iota((chip_cap, cap), 0).astype(F32)
        mine = (row == goal[q:q + 1, 0:cap]).astype(F32).astype(BF16)
        theirs = (row == goal[q:q + 1, lanes:lanes + cap]).astype(F32).astype(BF16)
        halves[q].wait_recv()
        for c in range(0, width, 512):
            part = jnp.dot(mine, ret[q, 0:cap, c:c + 512], preferred_element_type=F32)
            part = part + jnp.dot(theirs, half[q // 2, :, c:c + 512], preferred_element_type=F32)
            pack[q // 2 - 1, :, c:c + 512] = part.astype(BF16)
        copies[q] = pltpu.make_async_remote_copy(src_ref=pack.at[q // 2 - 1], dst_ref=got.at[q // 2 - 1], send_sem=send.at[q // 2 - 1], recv_sem=recv.at[q // 2 - 1], device_id=dev(flip(me, q)), device_id_type=MESH)
        copies[q].start()

    for t in range(LATE_RING):
        for c in weights(t):
            c.start()
    table = tok[...]

    def chosen(column, peer, at, count):
        lane = iota((tokens, count), 1).astype(F32)
        return jnp.concatenate([((column[k] == peer) & (table[:, at + k:at + k + 1] == lane)).astype(F32) for k in (0, 1)], axis=0).astype(BF16)

    owner = [table[:, 2 + k:3 + k] for k in (0, 1)]
    chip = [jnp.floor(o * 0.5) for o in owner]

    def add(pick, block, fresh):
        for c in range(0, width, 512):
            part = jnp.dot(pick, block(c), preferred_element_type=F32)
            acc[:, c:c + 512] = part if fresh else acc[:, c:c + 512] + part

    add(chosen(owner, me.astype(F32), 4, cap), lambda c: ret[0, 0:cap, c:c + 512], True)
    pick = chosen(owner, flip(me, 1).astype(F32), 4, cap)
    halves[0].wait_recv()
    add(pick, lambda c: half[0, :, c:c + 512], False)

    @pl.loop(0, steps)
    def _(t):
        e, f, n = t // NF, t % NF, t % LATE_RING
        for c in weights(t):
            c.wait()
        ffn_part(near[e, :, :, :].reshape(2 * slots, width), w1b, w3b, w2b, n, mid, yacc, f == 0, 2 * slots)

        @pl.when(f == NF - 1)
        def _():
            for q in (0, 1):
                late[q, pl.ds(pl.multiple_of(e * slots, slots), slots), :] = yacc[q * slots:(q + 1) * slots, :].astype(BF16)

        @pl.when(t + LATE_RING < steps)
        def _():
            for c in weights(t + LATE_RING):
                c.start()

    swap = pltpu.make_async_remote_copy(src_ref=late.at[1], dst_ref=late_half, send_sem=half_send.at[4], recv_sem=half_recv.at[4], device_id=dev(flip(me, 1)), device_id_type=MESH)
    swap.start()
    add(chosen(owner, me.astype(F32), 8, LATE * slots), lambda c: late[0, :, c:c + 512], False)
    pick = chosen(owner, flip(me, 1).astype(F32), 8, LATE * slots)
    swap.wait_recv()
    add(pick, lambda c: late_half[:, c:c + 512], False)
    for q in REMOTE:
        pick = chosen(chip, (flip(me, q) // 2).astype(F32), 6, chip_cap)
        copies[q].wait_recv()
        add(pick, lambda c: got[q // 2 - 1, :, c:c + 512], False)

    mixed = table[:, 0:1] * acc[0:tokens] + table[:, 1:2] * acc[tokens:2 * tokens]
    out[...] = (scale[0] * hid[...].astype(F32) + scale[1] * mixed).astype(BF16)
    for copy in (*halves.values(), *copies.values(), swap):
        copy.wait_send()


def return_call(n, caps, ret, near, tok, goal, hidden, scale, w1, w3, w2):
    owners, _, width = ret.shape
    slots, ft = near.shape[2], w1.shape[2] // NF
    tokens = hidden.shape[0]
    cap, chip_cap = caps
    vmem = pl.BlockSpec(memory_space=pltpu.VMEM)
    return pl.pallas_call(
        functools.partial(return_kernel, cap, chip_cap),
        name=f'return_{cap}_{chip_cap}',
        out_shape=jax.ShapeDtypeStruct((tokens, width), BF16),
        in_specs=[vmem, vmem, vmem, vmem, vmem, pl.BlockSpec(memory_space=pltpu.SMEM), *[pl.BlockSpec(memory_space=pl.ANY)] * 3],
        out_specs=vmem,
        scratch_shapes=[
            pltpu.VMEM((owners // 2, cap, width), BF16),
            pltpu.VMEM((len(REMOTE), chip_cap, width), BF16),
            pltpu.VMEM((len(REMOTE), chip_cap, width), BF16),
            pltpu.VMEM((2 * tokens, width), F32),
            pltpu.VMEM((2, LATE * slots, width), BF16),
            pltpu.VMEM((LATE * slots, width), BF16),
            pltpu.VMEM((2 * slots, ft), BF16),
            pltpu.VMEM((2 * slots, width), F32),
            pltpu.VMEM((LATE_RING, width, ft), BF16),
            pltpu.VMEM((LATE_RING, width, ft), BF16),
            pltpu.VMEM((LATE_RING, ft, width), BF16),
            pltpu.SemaphoreType.DMA((len(REMOTE),)),
            pltpu.SemaphoreType.DMA((len(REMOTE),)),
            pltpu.SemaphoreType.DMA((owners // 2 + 1,)),
            pltpu.SemaphoreType.DMA((owners // 2 + 1,)),
            pltpu.SemaphoreType.DMA((LATE_RING, 3)),
        ],
        compiler_params=pltpu.CompilerParams(collective_id=1 + n, has_side_effects=True, vmem_limit_bytes=34 * 1024 * 1024),
    )(ret, near, tok, goal, hidden, scale, w1, w3, w2)


def capacities(local, slots):
    full = [slots * n + 16 * (local - n) for n in range(1, local + 1)]
    chip = [2 * slots + 8 + (slots - 8) * n for n in range(local - 1)]
    return (*zip(full, chip), (local * slots, 2 * local * slots))


def solution(mesh):
    owners = mesh.shape['ep']

    def local_step(hidden, router_w, expert_ids, w_gate, w_up, w_down, post_scale):
        tokens = hidden.shape[0]
        local = w_gate.shape[0]
        slots = tokens // max(1, local * owners // 8)
        caps = capacities(local, slots)
        near, far, y_own, tok, goal, sizes, w1p, w3p, w2p = gather_call(hidden, expert_ids.T, router_w.T, w_gate, w_up, w_down, owners, caps)
        ret = expert_call(sizes, far, y_own, w1p, w3p, w2p, w_gate, w_up, w_down, caps)
        branches = [functools.partial(return_call, n, cap) for n, cap in enumerate(caps)]
        return lax.switch(sizes[0], branches, ret, near, tok, goal, hidden, post_scale, w_gate, w_up, w_down)

    tok_spec = P(('dp', 'ep'))
    return jax.shard_map(local_step, mesh=mesh, in_specs=(tok_spec, P(), tok_spec, P('ep'), P('ep'), P('ep'), P()), out_specs=tok_spec, check_vma=False)
```

```python
import functools

import jax
import jax.numpy as jnp
from jax import lax
from jax.experimental import pallas as pl
from jax.experimental.pallas import tpu as pltpu
from jax.sharding import PartitionSpec as P

MESH = pl.DeviceIdType.MESH
F32, BF16, I32 = jnp.float32, jnp.bfloat16, jnp.int32
NT = (((1,), (1,)), ((), ()))


def flip(idx, mask):
    out = idx
    for bit in (1, 2, 4):
        if mask & bit:
            out = out + bit - 2 * bit * ((idx // bit) % 2)
    return out


def dev(idx):
    return (lax.axis_index('dp'), idx)


def iota(shape, dim):
    return lax.broadcasted_iota(I32, shape, dim)


def weight_copies(w1, w3, w2, w1b, w3b, w2b, sem, e, f, n):
    ft = w1b.shape[2]
    cols = pl.ds(pl.multiple_of(f * ft, ft), ft)
    return (
        pltpu.make_async_copy(w1.at[e, :, cols], w1b.at[n], sem.at[n, 0]),
        pltpu.make_async_copy(w3.at[e, :, cols], w3b.at[n], sem.at[n, 1]),
        pltpu.make_async_copy(w2.at[e, cols, :], w2b.at[n], sem.at[n, 2]),
    )


def ffn_part(x, w1b, w3b, w2b, n, mid, yacc, fresh, m):
    for c in range(0, w1b.shape[2], 256):
        gate = jnp.dot(x, w1b[n, :, c:c + 256], preferred_element_type=F32)
        up = jnp.dot(x, w3b[n, :, c:c + 256], preferred_element_type=F32)
        mid[0:m, c:c + 256] = (gate * jax.nn.sigmoid(gate) * up).astype(BF16)
    for c in range(0, w2b.shape[2], 512):
        part = jnp.dot(mid[0:m, :], w2b[n, :, c:c + 512], preferred_element_type=F32)
        yacc[0:m, c:c + 512] = jnp.where(fresh, 0.0, yacc[0:m, c:c + 512]) + part


CHUNKS = 4
NF = 3
RING = 4
LATE_RING = 2
LATE = 2


def gather_kernel(caps, hid_in, ids_in, wrt_in, w1, w3, w2, near, far, y_own, tok, goal, plan, w1p, w3p, w2p, hid, ids, wrt, pos, mid, yacc, land, ids_all, send, recv, id_send, id_recv, wsem, in_sem):
    me = lax.axis_index('ep')
    own = [pltpu.make_async_copy(src, dst, in_sem.at[n]) for n, (src, dst) in enumerate(((hid_in, hid), (ids_in, ids), (wrt_in, wrt)))]
    for c in own:
        c.start()
    local, _, slots, _ = near.shape
    owners = 2 + far.shape[1]
    steps = (local - LATE) * NF

    def weights(t):
        return weight_copies(w1, w3, w2, w1p, w3p, w2p, wsem, local - 1 - t // NF, t % NF, t % RING)

    tokens, width = hid.shape
    experts = wrt.shape[0]
    rows = tokens // CHUNKS
    barrier = pltpu.get_barrier_semaphore()
    for q in range(1, owners):
        pl.semaphore_signal(barrier, inc=1, device_id=dev(flip(me, q)), device_id_type=MESH)
    pl.semaphore_wait(barrier, owners - 1)
    own[0].wait()
    own[1].wait()

    def piece(q, c):
        return (hid if q == 0 else land.at[q]).at[pl.ds(c * rows, rows)]

    def remote(q, c, n, to):
        return pltpu.make_async_remote_copy(src_ref=piece(q, c), dst_ref=land.at[q ^ to, pl.ds(c * rows, rows)], send_sem=send.at[n], recv_sem=recv.at[n], device_id=dev(flip(me, to)), device_id_type=MESH)

    id_copies = []
    for q in range(1, owners):
        id_copies.append(pltpu.make_async_remote_copy(src_ref=ids, dst_ref=ids_all.at[q], send_sem=id_send.at[q], recv_sem=id_recv.at[q], device_id=dev(flip(me, q)), device_id_type=MESH))
    for c in id_copies:
        c.start()
    x_order, y_order = (0, 1, 2, 3), (2, 3, 0, 1)
    to_x = {c: remote(0, c, c, 2) for c in x_order}
    to_y = {c: remote(0, c, 4 + c, 4) for c in y_order}
    for cx, cy in zip(x_order, y_order):
        to_x[cx].start()
        to_y[cy].start()
    to_mate = pltpu.make_async_remote_copy(src_ref=hid, dst_ref=land.at[1], send_sem=send.at[24], recv_sem=recv.at[24], device_id=dev(flip(me, 1)), device_id_type=MESH)
    to_mate.start()
    for t in range(RING):
        for c in weights(t):
            c.start()

    own[2].wait()
    h = hid[...]
    w = wrt[...]
    w_hi = w.astype(BF16)
    rest = w - w_hi.astype(F32)
    w_mid = rest.astype(BF16)
    w_lo = (rest - w_mid.astype(F32)).astype(BF16)
    dot = functools.partial(lax.dot_general, dimension_numbers=NT, preferred_element_type=F32)
    logits = dot(h, w_hi) + (dot(h, w_mid) + dot(h, w_lo))
    ex = jnp.exp(logits - jnp.max(logits, axis=1, keepdims=True))
    prob = ex / jnp.sum(ex, axis=1, keepdims=True)
    ta, tb = iota((tokens, tokens), 0), iota((tokens, tokens), 1)
    eye = (ta == tb).astype(F32).astype(BF16)
    own_ids = ids[...].astype(F32)
    lane = iota((tokens, experts), 1).astype(F32)
    id_col = [dot(eye, jnp.broadcast_to(own_ids[k:k + 1], (8, tokens)).astype(BF16))[:, 0:1] for k in (0, 1)]
    pick = [(id_col[k] == lane).astype(F32) for k in (0, 1)]
    g = [jnp.sum(pick[k] * prob, axis=1, keepdims=True) for k in (0, 1)]
    total = g[0] + g[1]

    for c in id_copies:
        c.wait_recv()
    ids_all[0] = ids[...]
    counts = []
    for q in range(owners):
        both = ids_all[q]
        e_col = iota((experts, tokens), 0)
        hot = ((both[0:1] == e_col) | (both[1:2] == e_col)).astype(F32).astype(BF16)
        counts.append(dot(jnp.ones((8, tokens), BF16), hot))
    most = functools.reduce(jnp.maximum, counts)
    count = jnp.concatenate([c[0:1] for c in counts], axis=0)
    stride = jnp.where(most > 32.0, float(slots), jnp.where(most > 16.0, 32.0, 16.0))
    mark = lambda mask: mask.astype(F32).astype(BF16)
    plain = functools.partial(jnp.dot, preferred_element_type=F32)
    ea, eb = iota((experts, experts), 0), iota((experts, experts), 1)
    same, same_chip = ea // local == eb // local, ea // (2 * local) == eb // (2 * local)
    offset = plain(stride.astype(BF16), mark(same & (ea < eb)))
    need = jnp.max(plain(stride.astype(BF16), mark(same))).astype(I32)
    need_chip = jnp.max(plain(count.astype(BF16), mark(same_chip))).astype(I32)
    branch = jnp.int32(0)
    for limit, limit_chip in caps[:-1]:
        branch = branch + ((need > limit) | (need_chip > limit_chip)).astype(I32)
    plan[0] = branch
    rank = plain(mark(tb < ta), (pick[0] + pick[1]).astype(BF16))
    chip_first = plain(count.astype(BF16), mark(same_chip & (ea < eb)))[0:1]
    local_of = lane - jnp.floor(lane * (1.0 / local)) * local
    late_place = jnp.where(local_of < LATE, local_of * slots + rank, -1.0)
    late = [jnp.sum(pick[k] * late_place, axis=1, keepdims=True) for k in (0, 1)]
    slot = [jnp.sum(pick[k] * (rank + offset[0:1]), axis=1, keepdims=True) for k in (0, 1)]
    packed = [jnp.sum(pick[k] * (rank + chip_first), axis=1, keepdims=True) for k in (0, 1)]
    owner = [jnp.floor(id_col[k] * (1.0 / local)) for k in (0, 1)]
    wide = iota((tokens, 128), 1)
    table = jnp.zeros((tokens, 128), F32)
    for n, col in enumerate((g[0] / total, g[1] / total, *owner, *slot, *packed, *late)):
        table = jnp.where(wide == n, col, table)
    tok[...] = table

    e_row, n_col = iota((experts, 128), 0), iota((experts, 128), 1)
    e_of = jnp.where(n_col < local, me * local + n_col, flip(me, 1) * local + n_col - local)
    used = n_col < 2 * local
    held = plain(count.astype(BF16), mark(used & (e_row == e_of)))
    start = plain(count.astype(BF16), mark(used & (e_row // (2 * local) == me // 2) & (e_row < e_of)))
    base = plain(stride.astype(BF16), mark(used & (e_row // local == e_of // local) & (e_row < e_of)))
    base_size = plain(stride.astype(BF16), mark(used & (e_row == e_of)))
    lane_of = iota((owners, goal.shape[1]), 1)
    where_to = jnp.full((owners, goal.shape[1]), -1.0, F32)
    for n in range(2 * local):
        at = (lane_of - (n // local) * (goal.shape[1] // 2)).astype(F32) - base[0:1, n:n + 1]
        where_to = jnp.where((at >= 0.0) & (at < held[:, n:n + 1]), at + start[:, n:n + 1], where_to)
    goal[...] = where_to

    first, second = (jnp.concatenate([ids_all[q, k:k + 1] for q in range(owners)], axis=0) for k in (0, 1))
    marks = jnp.concatenate([((first == me * local + j) | (second == me * local + j)).astype(F32) for j in range(local)], axis=0)
    earlier = plain(marks.astype(BF16), (ta < tb).astype(F32).astype(BF16))
    pos[...] = jnp.where(marks > 0.5, earlier, -1.0)
    for j in range(local):
        plan[1 + j] = jnp.max(base_size[:, j:j + 1]).astype(I32)

    def pick_rows(q):
        at = iota((slots, tokens), 0).astype(F32)
        match = jnp.concatenate([(at == pos[j * owners + q:j * owners + q + 1, :]).astype(F32) for j in range(local)], axis=0).astype(BF16)

        def columns(cols):
            block = hid[:, cols] if q == 0 else land[q, :, cols]
            part = jnp.dot(match, block, preferred_element_type=F32).astype(BF16)
            for j in range(local):
                to = near.at[j, q] if q < 2 else far.at[j, q - 2]
                to[:, cols] = part[j * slots:(j + 1) * slots]

        if q < 6:
            @pl.loop(0, width // 512)
            def _(n):
                columns(pl.ds(pl.multiple_of(n * 512, 512), 512))
        else:
            for c in range(0, width, 512):
                columns(pl.ds(c, 512))

    def own_steps(first, last):
        @pl.loop(first, last)
        def _(t):
            e, f, n = local - 1 - t // NF, t % NF, t % RING
            for c in weights(t):
                c.wait()
            x = near[e, :, :, :].reshape(2 * slots, width)
            ffn_part(x, w1p, w3p, w2p, n, mid, yacc, f == 0, 2 * slots)

            @pl.when(f == NF - 1)
            def _():
                for q in (0, 1):
                    y_own[e - LATE, q, :, :] = yacc[q * slots:(q + 1) * slots, :].astype(BF16)

            @pl.when(t + RING < steps)
            def _():
                for c in weights(t + RING):
                    c.start()

    sent = [*to_x.values(), *to_y.values(), to_mate]

    def pass_on(q, c, n, to):
        copy = remote(q, c, n, to)
        copy.start()
        sent.append(copy)
        return copy

    pick_rows(0)
    to_mate.wait_recv()
    pick_rows(1)
    across, mates = {}, {2: [], 4: [], 6: []}
    for n, (cx, cy) in enumerate(zip(x_order, y_order)):
        if n < 2:
            own_steps(n * steps // 2, (n + 1) * steps // 2)
        to_x[cx].wait_recv()
        if cx in (0, 1):
            across[cx] = pass_on(2, cx, 8 + cx, 4)
        mates[2].append(pass_on(2, cx, 12 + cx, 1))
        to_y[cy].wait_recv()
        if cy in (2, 3):
            across[cy] = pass_on(4, cy, 8 + cy, 2)
        mates[4].append(pass_on(4, cy, 16 + cy, 1))
    for q in (2, 4):
        pick_rows(q)
    for q in (2, 4):
        for m in mates[q]:
            m.wait_recv()
        pick_rows(q + 1)
    for c in (0, 2, 1, 3):
        across[c].wait_recv()
        mates[6].append(pass_on(6, c, 20 + c, 1))
    pick_rows(6)
    for m in mates[6]:
        m.wait_recv()
    pick_rows(7)
    for m in sent:
        m.wait_send()
    for c in id_copies:
        c.wait_send()


def gather_call(hidden, ids_t, wr_t, w1, w3, w2, owners, caps):
    tokens, width = hidden.shape
    experts = wr_t.shape[0]
    local, _, ffn = w1.shape
    slots = caps[-1][0] // local
    ft = ffn // NF
    vmem = pl.BlockSpec(memory_space=pltpu.VMEM)
    hbm = pl.BlockSpec(memory_space=pl.ANY)
    return pl.pallas_call(
        functools.partial(gather_kernel, caps),
        name='gather_tokens',
        out_shape=(
            pltpu.VMEM((local, 2, slots, width), BF16),
            pltpu.VMEM((local, owners - 2, slots, width), BF16),
            pltpu.VMEM((local - LATE, 2, slots, width), BF16),
            jax.ShapeDtypeStruct((tokens, 128), F32),
            jax.ShapeDtypeStruct((owners, 2 * local * slots), F32),
            jax.ShapeDtypeStruct((1 + local,), I32),
            pltpu.VMEM((RING, width, ft), BF16),
            pltpu.VMEM((RING, width, ft), BF16),
            pltpu.VMEM((RING, ft, width), BF16),
        ),
        in_specs=[hbm, *[pl.BlockSpec(memory_space=pltpu.HBM)] * 2, hbm, hbm, hbm],
        out_specs=(vmem, vmem, vmem, vmem, vmem, pl.BlockSpec(memory_space=pltpu.SMEM), vmem, vmem, vmem),
        scratch_shapes=[
            pltpu.VMEM((tokens, width), BF16),
            pltpu.VMEM((2, tokens), I32),
            pltpu.VMEM((experts, width), F32),
            pltpu.VMEM((local * owners, tokens), F32),
            pltpu.VMEM((2 * slots, ft), BF16),
            pltpu.VMEM((2 * slots, width), F32),
            pltpu.VMEM((owners, tokens, width), BF16),
            pltpu.VMEM((owners, 2, tokens), I32),
            pltpu.SemaphoreType.DMA((25,)),
            pltpu.SemaphoreType.DMA((25,)),
            pltpu.SemaphoreType.DMA((owners,)),
            pltpu.SemaphoreType.DMA((owners,)),
            pltpu.SemaphoreType.DMA((RING, 3)),
            pltpu.SemaphoreType.DMA((3,)),
        ],
        compiler_params=pltpu.CompilerParams(collective_id=0, has_side_effects=True, vmem_limit_bytes=13 * 1024 * 1024),
    )(hidden, *(pltpu.with_memory_space_constraint(x, pltpu.HBM) for x in (ids_t, wr_t)), w1, w3, w2)


def expert_kernel(caps, sizes, rows, y_own, _w1b, _w3b, _w2b, w1, w3, w2, ret, w1b, w3b, w2b, mid, yacc, plan, wsem):
    local, distant, slots, width = rows.shape
    owners = distant + 2
    steps = local * NF
    done = (local - LATE) * NF

    size = [sizes[1 + j] for j in range(local)]
    for j in range(local):
        rank = jnp.int32(j - LATE if j >= LATE else local - LATE)
        offset = jnp.int32(0)
        for i in range(local):
            if i < LATE and j < LATE and i != j:
                ahead = (size[i] >= size[j]) if i < j else (size[i] > size[j])
                rank = rank + ahead.astype(I32)
            if i < j:
                offset = offset + size[i]
        plan[0, rank] = jnp.int32(j)
        plan[1, rank] = size[j]
        plan[2, rank] = offset
    used = size[0]
    for j in range(1, local):
        used = used + size[j]

    def part_of(t):
        turn = jnp.where(t < NF, 0, 2 * NF - RING)
        return (t % NF + turn) % NF

    def weights(t):
        return weight_copies(w1, w3, w2, w1b, w3b, w2b, wsem, plan[0, t // NF], part_of(t), (t + done - NF) % RING)

    limit = jnp.int32(caps[0][0])
    for n in range(1, len(caps)):
        limit = jnp.where(sizes[0] >= n, caps[n][0], limit)

    @pl.loop(used // 16, limit // 16)
    def _(n):
        blank = pl.ds(pl.multiple_of(n * 16, 16), 16)
        for q in range(owners):
            ret[q, blank, :] = jnp.zeros((16, width), BF16)

    @pl.loop(0, steps)
    def _(t):
        r, f, n = t // NF, t % NF, (t + done - NF) % RING
        e = plan[0, r]

        @pl.when(t >= RING)
        def _():
            for c in weights(t):
                c.wait()

        for size in (16, 32, slots):
            m = size * distant

            @pl.when(plan[1, r] == size)
            def _():
                x = rows[e, :, 0:size, :].reshape(m, width)
                ffn_part(x, w1b, w3b, w2b, n, mid, yacc, f == 0, m)

                @pl.when(f == NF - 1)
                def _():
                    first = pl.multiple_of(plan[2, r], 16)
                    for q in (0, 1):
                        mine = y_own[jnp.maximum(e - LATE, 0), q, 0:size, :]
                        ret[q, pl.ds(first, size), :] = jnp.where(e >= LATE, mine, jnp.zeros_like(mine))
                    for q in range(2, owners):
                        ret[q, pl.ds(first, size), :] = yacc[(q - 2) * size:(q - 1) * size, :].astype(BF16)

        @pl.when(t + RING < steps)
        def _():
            for c in weights(t + RING):
                c.start()


def expert_call(sizes, rows, y_own, w1p, w3p, w2p, w1, w3, w2, caps):
    local, distant, slots, width = rows.shape
    owners = distant + 2
    ft = w1p.shape[2]
    hbm = pl.BlockSpec(memory_space=pl.ANY)
    vmem = pl.BlockSpec(memory_space=pltpu.VMEM)
    flops = 3 * 2 * local * slots * owners * width * ft * NF // 2
    return pl.pallas_call(
        functools.partial(expert_kernel, caps),
        name='experts',
        out_shape=(
            pltpu.VMEM((owners, caps[-1][0], width), BF16),
            pltpu.VMEM(w1p.shape, BF16),
            pltpu.VMEM(w3p.shape, BF16),
            pltpu.VMEM(w2p.shape, BF16),
        ),
        in_specs=[pl.BlockSpec(memory_space=pltpu.SMEM), vmem, vmem, vmem, vmem, vmem, hbm, hbm, hbm],
        out_specs=(vmem, vmem, vmem, vmem),
        input_output_aliases={3: 1, 4: 2, 5: 3},
        scratch_shapes=[
            pltpu.VMEM((distant * slots, ft), BF16),
            pltpu.VMEM((distant * slots, width), F32),
            pltpu.SMEM((3, local), I32),
            pltpu.SemaphoreType.DMA((RING, 3)),
        ],
        compiler_params=pltpu.CompilerParams(vmem_limit_bytes=12 * 1024 * 1024),
        cost_estimate=pl.CostEstimate(flops=flops, bytes_accessed=3 * 2 * local * width * ft * NF, transcendentals=0),
    )(sizes, rows, y_own, w1p, w3p, w2p, w1, w3, w2)[0]


REMOTE = (2, 4, 6)


def return_kernel(cap, chip_cap, ret, near, tok, goal, hid, scale, w1, w3, w2, out, half, pack, got, acc, late, late_half, mid, yacc, w1b, w3b, w2b, send, recv, half_send, half_recv, wsem):
    me = lax.axis_index('ep')
    slots = near.shape[2]
    steps = LATE * NF

    def weights(t):
        return weight_copies(w1, w3, w2, w1b, w3b, w2b, wsem, t // NF, t % NF, t % LATE_RING)

    tokens, width = hid.shape
    lanes = goal.shape[1] // 2
    barrier = pltpu.get_barrier_semaphore()
    for q in (1, *REMOTE):
        pl.semaphore_signal(barrier, inc=1, device_id=dev(flip(me, q)), device_id_type=MESH)
    pl.semaphore_wait(barrier, 1 + len(REMOTE))
    halves, copies = {}, {}
    for q in (*REMOTE, 0):
        halves[q] = pltpu.make_async_remote_copy(src_ref=ret.at[q + 1, pl.ds(0, cap)], dst_ref=half.at[q // 2], send_sem=half_send.at[q // 2], recv_sem=half_recv.at[q // 2], device_id=dev(flip(me, 1)), device_id_type=MESH)
        halves[q].start()

    for q in REMOTE:
        row = iota((chip_cap, cap), 0).astype(F32)
        mine = (row == goal[q:q + 1, 0:cap]).astype(F32).astype(BF16)
        theirs = (row == goal[q:q + 1, lanes:lanes + cap]).astype(F32).astype(BF16)
        halves[q].wait_recv()
        for c in range(0, width, 512):
            part = jnp.dot(mine, ret[q, 0:cap, c:c + 512], preferred_element_type=F32)
            part = part + jnp.dot(theirs, half[q // 2, :, c:c + 512], preferred_element_type=F32)
            pack[q // 2 - 1, :, c:c + 512] = part.astype(BF16)
        copies[q] = pltpu.make_async_remote_copy(src_ref=pack.at[q // 2 - 1], dst_ref=got.at[q // 2 - 1], send_sem=send.at[q // 2 - 1], recv_sem=recv.at[q // 2 - 1], device_id=dev(flip(me, q)), device_id_type=MESH)
        copies[q].start()

    for t in range(LATE_RING):
        for c in weights(t):
            c.start()
    table = tok[...]

    def chosen(column, peer, at, count):
        lane = iota((tokens, count), 1).astype(F32)
        return jnp.concatenate([((column[k] == peer) & (table[:, at + k:at + k + 1] == lane)).astype(F32) for k in (0, 1)], axis=0).astype(BF16)

    owner = [table[:, 2 + k:3 + k] for k in (0, 1)]
    chip = [jnp.floor(o * 0.5) for o in owner]

    gate = [table[:, k:k + 1] for k in (0, 1)]

    def add(pick, block, fresh=False, last=False):
        for c in range(0, width, 512):
            part = jnp.dot(pick, block(c), preferred_element_type=F32)
            mixed = gate[0] * part[0:tokens] + gate[1] * part[tokens:2 * tokens]
            if not fresh:
                mixed = acc[:, c:c + 512] + mixed
            if last:
                out[:, c:c + 512] = (scale[0] * hid[:, c:c + 512].astype(F32) + scale[1] * mixed).astype(BF16)
            else:
                acc[:, c:c + 512] = mixed

    add(chosen(owner, me.astype(F32), 4, cap), lambda c: ret[0, 0:cap, c:c + 512], fresh=True)
    pick = chosen(owner, flip(me, 1).astype(F32), 4, cap)
    halves[0].wait_recv()
    add(pick, lambda c: half[0, :, c:c + 512])

    @pl.loop(0, steps)
    def _(t):
        e, f, n = t // NF, t % NF, t % LATE_RING
        for c in weights(t):
            c.wait()
        ffn_part(near[e, :, :, :].reshape(2 * slots, width), w1b, w3b, w2b, n, mid, yacc, f == 0, 2 * slots)

        @pl.when(f == NF - 1)
        def _():
            for q in (0, 1):
                late[q, pl.ds(pl.multiple_of(e * slots, slots), slots), :] = yacc[q * slots:(q + 1) * slots, :].astype(BF16)

        @pl.when(t + LATE_RING < steps)
        def _():
            for c in weights(t + LATE_RING):
                c.start()

    swap = pltpu.make_async_remote_copy(src_ref=late.at[1], dst_ref=late_half, send_sem=half_send.at[4], recv_sem=half_recv.at[4], device_id=dev(flip(me, 1)), device_id_type=MESH)
    swap.start()
    add(chosen(owner, me.astype(F32), 8, LATE * slots), lambda c: late[0, :, c:c + 512])
    pick = chosen(owner, flip(me, 1).astype(F32), 8, LATE * slots)
    swap.wait_recv()
    add(pick, lambda c: late_half[:, c:c + 512])
    for q in REMOTE:
        pick = chosen(chip, (flip(me, q) // 2).astype(F32), 6, chip_cap)
        copies[q].wait_recv()
        add(pick, lambda c: got[q // 2 - 1, :, c:c + 512], last=q == REMOTE[-1])

    for copy in (*halves.values(), *copies.values(), swap):
        copy.wait_send()


def return_call(n, caps, ret, near, tok, goal, hidden, scale, w1, w3, w2):
    owners, _, width = ret.shape
    slots, ft = near.shape[2], w1.shape[2] // NF
    tokens = hidden.shape[0]
    cap, chip_cap = caps
    vmem = pl.BlockSpec(memory_space=pltpu.VMEM)
    return pl.pallas_call(
        functools.partial(return_kernel, cap, chip_cap),
        name=f'return_{cap}_{chip_cap}',
        out_shape=jax.ShapeDtypeStruct((tokens, width), BF16),
        in_specs=[vmem, vmem, vmem, vmem, vmem, pl.BlockSpec(memory_space=pltpu.SMEM), *[pl.BlockSpec(memory_space=pl.ANY)] * 3],
        out_specs=vmem,
        scratch_shapes=[
            pltpu.VMEM((owners // 2, cap, width), BF16),
            pltpu.VMEM((len(REMOTE), chip_cap, width), BF16),
            pltpu.VMEM((len(REMOTE), chip_cap, width), BF16),
            pltpu.VMEM((tokens, width), F32),
            pltpu.VMEM((2, LATE * slots, width), BF16),
            pltpu.VMEM((LATE * slots, width), BF16),
            pltpu.VMEM((2 * slots, ft), BF16),
            pltpu.VMEM((2 * slots, width), F32),
            pltpu.VMEM((LATE_RING, width, ft), BF16),
            pltpu.VMEM((LATE_RING, width, ft), BF16),
            pltpu.VMEM((LATE_RING, ft, width), BF16),
            pltpu.SemaphoreType.DMA((len(REMOTE),)),
            pltpu.SemaphoreType.DMA((len(REMOTE),)),
            pltpu.SemaphoreType.DMA((owners // 2 + 1,)),
            pltpu.SemaphoreType.DMA((owners // 2 + 1,)),
            pltpu.SemaphoreType.DMA((LATE_RING, 3)),
        ],
        compiler_params=pltpu.CompilerParams(collective_id=1 + n, has_side_effects=True, vmem_limit_bytes=34 * 1024 * 1024),
    )(ret, near, tok, goal, hidden, scale, w1, w3, w2)


def capacities(local, slots):
    full = [slots * n + 16 * (local - n) for n in range(1, local + 1)]
    chip = [2 * slots + 8 + (slots - 8) * n for n in range(local - 1)]
    return (*zip(full, chip), (local * slots, 2 * local * slots))


def solution(mesh):
    owners = mesh.shape['ep']

    def local_step(hidden, router_w, expert_ids, w_gate, w_up, w_down, post_scale):
        tokens = hidden.shape[0]
        local = w_gate.shape[0]
        slots = tokens // max(1, local * owners // 8)
        caps = capacities(local, slots)
        near, far, y_own, tok, goal, sizes, w1p, w3p, w2p = gather_call(hidden, expert_ids.T, router_w.T, w_gate, w_up, w_down, owners, caps)
        ret = expert_call(sizes, far, y_own, w1p, w3p, w2p, w_gate, w_up, w_down, caps)
        branches = [functools.partial(return_call, n, cap) for n, cap in enumerate(caps)]
        return lax.switch(sizes[0], branches, ret, near, tok, goal, hidden, post_scale, w_gate, w_up, w_down)

    tok_spec = P(('dp', 'ep'))
    return jax.shard_map(local_step, mesh=mesh, in_specs=(tok_spec, P(), tok_spec, P('ep'), P('ep'), P('ep'), P()), out_specs=tok_spec, check_vma=False)
```

```python
import functools

import jax
import jax.numpy as jnp
from jax import lax
from jax.experimental import pallas as pl
from jax.experimental.pallas import tpu as pltpu
from jax.sharding import PartitionSpec as P

MESH = pl.DeviceIdType.MESH
F32, BF16, I32 = jnp.float32, jnp.bfloat16, jnp.int32
NT = (((1,), (1,)), ((), ()))


def flip(idx, mask):
    out = idx
    for bit in (1, 2, 4):
        if mask & bit:
            out = out + bit - 2 * bit * ((idx // bit) % 2)
    return out


def dev(idx):
    return (lax.axis_index('dp'), idx)


def iota(shape, dim):
    return lax.broadcasted_iota(I32, shape, dim)


def weight_copies(w1, w3, w2, w1b, w3b, w2b, sem, e, f, n):
    ft = w1b.shape[2]
    cols = pl.ds(pl.multiple_of(f * ft, ft), ft)
    return (
        pltpu.make_async_copy(w1.at[e, :, cols], w1b.at[n], sem.at[n, 0]),
        pltpu.make_async_copy(w3.at[e, :, cols], w3b.at[n], sem.at[n, 1]),
        pltpu.make_async_copy(w2.at[e, cols, :], w2b.at[n], sem.at[n, 2]),
    )


def ffn_part(x, w1b, w3b, w2b, n, mid, yacc, fresh, m):
    for c in range(0, w1b.shape[2], 256):
        gate = jnp.dot(x, w1b[n, :, c:c + 256], preferred_element_type=F32)
        up = jnp.dot(x, w3b[n, :, c:c + 256], preferred_element_type=F32)
        mid[0:m, c:c + 256] = (gate * jax.nn.sigmoid(gate) * up).astype(BF16)
    for c in range(0, w2b.shape[2], 512):
        part = jnp.dot(mid[0:m, :], w2b[n, :, c:c + 512], preferred_element_type=F32)
        yacc[0:m, c:c + 512] = jnp.where(fresh, 0.0, yacc[0:m, c:c + 512]) + part


CHUNKS = 4
NF = 3
RING = 4
LATE_RING = 2
LATE = 2


def gather_kernel(caps, hid_in, ids_in, wrt_in, w1, w3, w2, near, far, y_own, tok, goal, plan, w1p, w3p, w2p, hid, ids, wrt, pos, mid, yacc, land, ids_all, send, recv, id_send, id_recv, wsem, in_sem):
    me = lax.axis_index('ep')
    own = [pltpu.make_async_copy(src, dst, in_sem.at[n]) for n, (src, dst) in enumerate(((hid_in, hid), (ids_in, ids), (wrt_in, wrt)))]
    for c in own:
        c.start()
    local, _, slots, _ = near.shape
    owners = 2 + far.shape[1]
    steps = (local - LATE) * NF

    def weights(t):
        return weight_copies(w1, w3, w2, w1p, w3p, w2p, wsem, local - 1 - t // NF, t % NF, t % RING)

    tokens, width = hid.shape
    experts = wrt.shape[0]
    rows = tokens // CHUNKS
    barrier = pltpu.get_barrier_semaphore()
    for q in range(1, owners):
        pl.semaphore_signal(barrier, inc=1, device_id=dev(flip(me, q)), device_id_type=MESH)
    pl.semaphore_wait(barrier, owners - 1)
    own[0].wait()
    own[1].wait()

    def piece(q, c):
        return (hid if q == 0 else land.at[q]).at[pl.ds(c * rows, rows)]

    def remote(q, c, n, to):
        return pltpu.make_async_remote_copy(src_ref=piece(q, c), dst_ref=land.at[q ^ to, pl.ds(c * rows, rows)], send_sem=send.at[n], recv_sem=recv.at[n], device_id=dev(flip(me, to)), device_id_type=MESH)

    id_copies = []
    for q in range(1, owners):
        id_copies.append(pltpu.make_async_remote_copy(src_ref=ids, dst_ref=ids_all.at[q], send_sem=id_send.at[q], recv_sem=id_recv.at[q], device_id=dev(flip(me, q)), device_id_type=MESH))
    for c in id_copies:
        c.start()
    x_order, y_order = (0, 1, 2, 3), (2, 3, 0, 1)
    to_x = {c: remote(0, c, c, 2) for c in x_order}
    to_y = {c: remote(0, c, 4 + c, 4) for c in y_order}
    for cx, cy in zip(x_order, y_order):
        to_x[cx].start()
        to_y[cy].start()
    to_mate = pltpu.make_async_remote_copy(src_ref=hid, dst_ref=land.at[1], send_sem=send.at[24], recv_sem=recv.at[24], device_id=dev(flip(me, 1)), device_id_type=MESH)
    to_mate.start()
    for t in range(RING):
        for c in weights(t):
            c.start()

    own[2].wait()
    h = hid[...]
    w = wrt[...]
    w_hi = w.astype(BF16)
    rest = w - w_hi.astype(F32)
    w_mid = rest.astype(BF16)
    w_lo = (rest - w_mid.astype(F32)).astype(BF16)
    dot = functools.partial(lax.dot_general, dimension_numbers=NT, preferred_element_type=F32)
    logits = dot(h, w_hi) + (dot(h, w_mid) + dot(h, w_lo))
    ex = jnp.exp(logits - jnp.max(logits, axis=1, keepdims=True))
    prob = ex / jnp.sum(ex, axis=1, keepdims=True)
    ta, tb = iota((tokens, tokens), 0), iota((tokens, tokens), 1)
    eye = (ta == tb).astype(F32).astype(BF16)
    own_ids = ids[...].astype(F32)
    lane = iota((tokens, experts), 1).astype(F32)
    id_col = [dot(eye, jnp.broadcast_to(own_ids[k:k + 1], (8, tokens)).astype(BF16))[:, 0:1] for k in (0, 1)]
    pick = [(id_col[k] == lane).astype(F32) for k in (0, 1)]
    g = [jnp.sum(pick[k] * prob, axis=1, keepdims=True) for k in (0, 1)]
    total = g[0] + g[1]

    for c in id_copies:
        c.wait_recv()
    ids_all[0] = ids[...]
    counts = []
    for q in range(owners):
        both = ids_all[q]
        e_col = iota((experts, tokens), 0)
        hot = ((both[0:1] == e_col) | (both[1:2] == e_col)).astype(F32).astype(BF16)
        counts.append(dot(jnp.ones((8, tokens), BF16), hot))
    most = functools.reduce(jnp.maximum, counts)
    count = jnp.concatenate([c[0:1] for c in counts], axis=0)
    stride = jnp.where(most > 32.0, float(slots), jnp.where(most > 16.0, 32.0, 16.0))
    mark = lambda mask: mask.astype(F32).astype(BF16)
    plain = functools.partial(jnp.dot, preferred_element_type=F32)
    ea, eb = iota((experts, experts), 0), iota((experts, experts), 1)
    same, same_chip = ea // local == eb // local, ea // (2 * local) == eb // (2 * local)
    offset = plain(stride.astype(BF16), mark(same & (ea < eb)))
    need = jnp.max(plain(stride.astype(BF16), mark(same))).astype(I32)
    need_chip = jnp.max(plain(count.astype(BF16), mark(same_chip))).astype(I32)
    branch = jnp.int32(0)
    for limit, limit_chip in caps[:-1]:
        branch = branch + ((need > limit) | (need_chip > limit_chip)).astype(I32)
    plan[0] = branch
    rank = plain(mark(tb < ta), (pick[0] + pick[1]).astype(BF16))
    chip_first = plain(count.astype(BF16), mark(same_chip & (ea < eb)))[0:1]
    local_of = lane - jnp.floor(lane * (1.0 / local)) * local
    late_place = jnp.where(local_of < LATE, local_of * slots + rank, -1.0)
    late = [jnp.sum(pick[k] * late_place, axis=1, keepdims=True) for k in (0, 1)]
    slot = [jnp.sum(pick[k] * (rank + offset[0:1]), axis=1, keepdims=True) for k in (0, 1)]
    packed = [jnp.sum(pick[k] * (rank + chip_first), axis=1, keepdims=True) for k in (0, 1)]
    owner = [jnp.floor(id_col[k] * (1.0 / local)) for k in (0, 1)]
    wide = iota((tokens, 128), 1)
    table = jnp.zeros((tokens, 128), F32)
    for n, col in enumerate((g[0] / total, g[1] / total, *owner, *slot, *packed, *late)):
        table = jnp.where(wide == n, col, table)
    tok[...] = table

    e_row, n_col = iota((experts, 128), 0), iota((experts, 128), 1)
    e_of = jnp.where(n_col < local, me * local + n_col, flip(me, 1) * local + n_col - local)
    used = n_col < 2 * local
    held = plain(count.astype(BF16), mark(used & (e_row == e_of)))
    start = plain(count.astype(BF16), mark(used & (e_row // (2 * local) == me // 2) & (e_row < e_of)))
    base = plain(stride.astype(BF16), mark(used & (e_row // local == e_of // local) & (e_row < e_of)))
    base_size = plain(stride.astype(BF16), mark(used & (e_row == e_of)))
    lane_of = iota((owners, goal.shape[1]), 1)
    where_to = jnp.full((owners, goal.shape[1]), -1.0, F32)
    for n in range(2 * local):
        at = (lane_of - (n // local) * (goal.shape[1] // 2)).astype(F32) - base[0:1, n:n + 1]
        where_to = jnp.where((at >= 0.0) & (at < held[:, n:n + 1]), at + start[:, n:n + 1], where_to)
    goal[...] = where_to

    first, second = (jnp.concatenate([ids_all[q, k:k + 1] for q in range(owners)], axis=0) for k in (0, 1))
    marks = jnp.concatenate([((first == me * local + j) | (second == me * local + j)).astype(F32) for j in range(local)], axis=0)
    earlier = plain(marks.astype(BF16), (ta < tb).astype(F32).astype(BF16))
    pos[...] = jnp.where(marks > 0.5, earlier, -1.0)
    for j in range(local):
        plan[1 + j] = jnp.max(base_size[:, j:j + 1]).astype(I32)

    def pick_rows(q):
        at = iota((slots, tokens), 0).astype(F32)
        match = jnp.concatenate([(at == pos[j * owners + q:j * owners + q + 1, :]).astype(F32) for j in range(local)], axis=0).astype(BF16)

        def columns(cols):
            block = hid[:, cols] if q == 0 else land[q, :, cols]
            part = jnp.dot(match, block, preferred_element_type=F32).astype(BF16)
            for j in range(local):
                to = near.at[j, q] if q < 2 else far.at[j, q - 2]
                to[:, cols] = part[j * slots:(j + 1) * slots]

        if q < 6:
            @pl.loop(0, width // 512)
            def _(n):
                columns(pl.ds(pl.multiple_of(n * 512, 512), 512))
        else:
            for c in range(0, width, 512):
                columns(pl.ds(c, 512))

    def own_steps(first, last):
        @pl.loop(first, last)
        def _(t):
            e, f, n = local - 1 - t // NF, t % NF, t % RING
            for c in weights(t):
                c.wait()
            x = near[e, :, :, :].reshape(2 * slots, width)
            ffn_part(x, w1p, w3p, w2p, n, mid, yacc, f == 0, 2 * slots)

            @pl.when(f == NF - 1)
            def _():
                for q in (0, 1):
                    y_own[e - LATE, q, :, :] = yacc[q * slots:(q + 1) * slots, :].astype(BF16)

            @pl.when(t + RING < steps)
            def _():
                for c in weights(t + RING):
                    c.start()

    sent = [*to_x.values(), *to_y.values(), to_mate]

    def pass_on(q, c, n, to):
        copy = remote(q, c, n, to)
        copy.start()
        sent.append(copy)
        return copy

    pick_rows(0)
    to_mate.wait_recv()
    pick_rows(1)
    across, mates = {}, {2: [], 4: [], 6: []}
    for n, (cx, cy) in enumerate(zip(x_order, y_order)):
        if n < 2:
            own_steps(n * steps // 2, (n + 1) * steps // 2)
        to_x[cx].wait_recv()
        if cx in (0, 1):
            across[cx] = pass_on(2, cx, 8 + cx, 4)
        mates[2].append(pass_on(2, cx, 12 + cx, 1))
        to_y[cy].wait_recv()
        if cy in (2, 3):
            across[cy] = pass_on(4, cy, 8 + cy, 2)
        mates[4].append(pass_on(4, cy, 16 + cy, 1))
    for q in (2, 4):
        pick_rows(q)
    for q in (2, 4):
        for m in mates[q]:
            m.wait_recv()
        pick_rows(q + 1)
    for c in (0, 2, 1, 3):
        across[c].wait_recv()
        mates[6].append(pass_on(6, c, 20 + c, 1))
    pick_rows(6)
    for m in mates[6]:
        m.wait_recv()
    pick_rows(7)
    for m in sent:
        m.wait_send()
    for c in id_copies:
        c.wait_send()


def gather_call(hidden, ids_t, wr_t, w1, w3, w2, owners, caps):
    tokens, width = hidden.shape
    experts = wr_t.shape[0]
    local, _, ffn = w1.shape
    slots = caps[-1][0] // local
    ft = ffn // NF
    vmem = pl.BlockSpec(memory_space=pltpu.VMEM)
    hbm = pl.BlockSpec(memory_space=pl.ANY)
    return pl.pallas_call(
        functools.partial(gather_kernel, caps),
        name='gather_tokens',
        out_shape=(
            pltpu.VMEM((local, 2, slots, width), BF16),
            pltpu.VMEM((local, owners - 2, slots, width), BF16),
            pltpu.VMEM((local - LATE, 2, slots, width), BF16),
            jax.ShapeDtypeStruct((tokens, 128), F32),
            jax.ShapeDtypeStruct((owners, 2 * local * slots), F32),
            jax.ShapeDtypeStruct((1 + local,), I32),
            pltpu.VMEM((RING, width, ft), BF16),
            pltpu.VMEM((RING, width, ft), BF16),
            pltpu.VMEM((RING, ft, width), BF16),
        ),
        in_specs=[hbm, *[pl.BlockSpec(memory_space=pltpu.HBM)] * 2, hbm, hbm, hbm],
        out_specs=(vmem, vmem, vmem, vmem, vmem, pl.BlockSpec(memory_space=pltpu.SMEM), vmem, vmem, vmem),
        scratch_shapes=[
            pltpu.VMEM((tokens, width), BF16),
            pltpu.VMEM((2, tokens), I32),
            pltpu.VMEM((experts, width), F32),
            pltpu.VMEM((local * owners, tokens), F32),
            pltpu.VMEM((2 * slots, ft), BF16),
            pltpu.VMEM((2 * slots, width), F32),
            pltpu.VMEM((owners, tokens, width), BF16),
            pltpu.VMEM((owners, 2, tokens), I32),
            pltpu.SemaphoreType.DMA((25,)),
            pltpu.SemaphoreType.DMA((25,)),
            pltpu.SemaphoreType.DMA((owners,)),
            pltpu.SemaphoreType.DMA((owners,)),
            pltpu.SemaphoreType.DMA((RING, 3)),
            pltpu.SemaphoreType.DMA((3,)),
        ],
        compiler_params=pltpu.CompilerParams(collective_id=0, has_side_effects=True, vmem_limit_bytes=13 * 1024 * 1024),
    )(hidden, *(pltpu.with_memory_space_constraint(x, pltpu.HBM) for x in (ids_t, wr_t)), w1, w3, w2)


def expert_kernel(caps, sizes, rows, y_own, _w1b, _w3b, _w2b, w1, w3, w2, ret, w1b, w3b, w2b, mid, yacc, plan, wsem):
    local, distant, slots, width = rows.shape
    owners = distant + 2
    steps = local * NF
    done = (local - LATE) * NF

    size = [sizes[1 + j] for j in range(local)]
    for j in range(local):
        rank = jnp.int32(j - LATE if j >= LATE else local - LATE)
        offset = jnp.int32(0)
        for i in range(local):
            if i < LATE and j < LATE and i != j:
                ahead = (size[i] >= size[j]) if i < j else (size[i] > size[j])
                rank = rank + ahead.astype(I32)
            if i < j:
                offset = offset + size[i]
        plan[0, rank] = jnp.int32(j)
        plan[1, rank] = size[j]
        plan[2, rank] = offset
    used = size[0]
    for j in range(1, local):
        used = used + size[j]

    def part_of(t):
        turn = jnp.where(t < NF, 0, 2 * NF - RING)
        return (t % NF + turn) % NF

    def weights(t):
        return weight_copies(w1, w3, w2, w1b, w3b, w2b, wsem, plan[0, t // NF], part_of(t), (t + done - NF) % RING)

    limit = jnp.int32(caps[0][0])
    for n in range(1, len(caps)):
        limit = jnp.where(sizes[0] >= n, caps[n][0], limit)

    @pl.loop(used // 16, limit // 16)
    def _(n):
        blank = pl.ds(pl.multiple_of(n * 16, 16), 16)
        for q in range(owners):
            ret[q, blank, :] = jnp.zeros((16, width), BF16)

    @pl.loop(0, steps)
    def _(t):
        r, f, n = t // NF, t % NF, (t + done - NF) % RING
        e = plan[0, r]

        @pl.when(t >= RING)
        def _():
            for c in weights(t):
                c.wait()

        for size in (16, 32, slots):
            m = size * distant

            @pl.when(plan[1, r] == size)
            def _():
                x = rows[e, :, 0:size, :].reshape(m, width)
                ffn_part(x, w1b, w3b, w2b, n, mid, yacc, f == 0, m)

                @pl.when(f == NF - 1)
                def _():
                    first = pl.multiple_of(plan[2, r], 16)
                    for q in (0, 1):
                        mine = y_own[jnp.maximum(e - LATE, 0), q, 0:size, :]
                        ret[q, pl.ds(first, size), :] = jnp.where(e >= LATE, mine, jnp.zeros_like(mine))
                    for q in range(2, owners):
                        ret[q, pl.ds(first, size), :] = yacc[(q - 2) * size:(q - 1) * size, :].astype(BF16)

        @pl.when(t + RING < steps)
        def _():
            for c in weights(t + RING):
                c.start()


def expert_call(sizes, rows, y_own, w1p, w3p, w2p, w1, w3, w2, caps):
    local, distant, slots, width = rows.shape
    owners = distant + 2
    ft = w1p.shape[2]
    hbm = pl.BlockSpec(memory_space=pl.ANY)
    vmem = pl.BlockSpec(memory_space=pltpu.VMEM)
    flops = 3 * 2 * local * slots * owners * width * ft * NF // 2
    return pl.pallas_call(
        functools.partial(expert_kernel, caps),
        name='experts',
        out_shape=(
            pltpu.VMEM((owners, caps[-1][0], width), BF16),
            pltpu.VMEM(w1p.shape, BF16),
            pltpu.VMEM(w3p.shape, BF16),
            pltpu.VMEM(w2p.shape, BF16),
        ),
        in_specs=[pl.BlockSpec(memory_space=pltpu.SMEM), vmem, vmem, vmem, vmem, vmem, hbm, hbm, hbm],
        out_specs=(vmem, vmem, vmem, vmem),
        input_output_aliases={3: 1, 4: 2, 5: 3},
        scratch_shapes=[
            pltpu.VMEM((distant * slots, ft), BF16),
            pltpu.VMEM((distant * slots, width), F32),
            pltpu.SMEM((3, local), I32),
            pltpu.SemaphoreType.DMA((RING, 3)),
        ],
        compiler_params=pltpu.CompilerParams(vmem_limit_bytes=12 * 1024 * 1024),
        cost_estimate=pl.CostEstimate(flops=flops, bytes_accessed=3 * 2 * local * width * ft * NF, transcendentals=0),
    )(sizes, rows, y_own, w1p, w3p, w2p, w1, w3, w2)[0]


REMOTE = (2, 4, 6)


def return_kernel(cap, chip_cap, ret, near, tok, goal, hid, scale, w1, w3, w2, out, half, pack, got, acc, late, late_half, mid, yacc, w1b, w3b, w2b, send, recv, half_send, half_recv, wsem):
    me = lax.axis_index('ep')
    slots = near.shape[2]
    steps = LATE * NF

    def weights(t):
        return weight_copies(w1, w3, w2, w1b, w3b, w2b, wsem, t // NF, t % NF, t % LATE_RING)

    tokens, width = hid.shape
    lanes = goal.shape[1] // 2
    barrier = pltpu.get_barrier_semaphore()
    for q in (1, *REMOTE):
        pl.semaphore_signal(barrier, inc=1, device_id=dev(flip(me, q)), device_id_type=MESH)
    pl.semaphore_wait(barrier, 1 + len(REMOTE))
    halves, copies = {}, {}
    for q in (*REMOTE, 0):
        halves[q] = pltpu.make_async_remote_copy(src_ref=ret.at[q + 1, pl.ds(0, cap)], dst_ref=half.at[q // 2], send_sem=half_send.at[q // 2], recv_sem=half_recv.at[q // 2], device_id=dev(flip(me, 1)), device_id_type=MESH)
        halves[q].start()

    for q in REMOTE:
        row = iota((chip_cap, cap), 0).astype(F32)
        mine = (row == goal[q:q + 1, 0:cap]).astype(F32).astype(BF16)
        theirs = (row == goal[q:q + 1, lanes:lanes + cap]).astype(F32).astype(BF16)
        halves[q].wait_recv()
        for c in range(0, width, 512):
            part = jnp.dot(mine, ret[q, 0:cap, c:c + 512], preferred_element_type=F32)
            part = part + jnp.dot(theirs, half[q // 2, :, c:c + 512], preferred_element_type=F32)
            pack[q // 2 - 1, :, c:c + 512] = part.astype(BF16)
        copies[q] = pltpu.make_async_remote_copy(src_ref=pack.at[q // 2 - 1], dst_ref=got.at[q // 2 - 1], send_sem=send.at[q // 2 - 1], recv_sem=recv.at[q // 2 - 1], device_id=dev(flip(me, q)), device_id_type=MESH)
        copies[q].start()

    for t in range(LATE_RING):
        for c in weights(t):
            c.start()
    table = tok[...]

    def chosen(column, peer, at, count):
        lane = iota((tokens, count), 1).astype(F32)
        return jnp.concatenate([((column[k] == peer) & (table[:, at + k:at + k + 1] == lane)).astype(F32) for k in (0, 1)], axis=0).astype(BF16)

    owner = [table[:, 2 + k:3 + k] for k in (0, 1)]
    chip = [jnp.floor(o * 0.5) for o in owner]

    gate = [table[:, k:k + 1] for k in (0, 1)]

    def add(pick, block, fresh=False, last=False):
        @pl.loop(0, width // 512)
        def _(n):
            cols = pl.ds(pl.multiple_of(n * 512, 512), 512)
            part = jnp.dot(pick, block(cols), preferred_element_type=F32)
            mixed = gate[0] * part[0:tokens] + gate[1] * part[tokens:2 * tokens]
            if not fresh:
                mixed = acc[:, cols] + mixed
            if last:
                out[:, cols] = (scale[0] * hid[:, cols].astype(F32) + scale[1] * mixed).astype(BF16)
            else:
                acc[:, cols] = mixed

    add(chosen(owner, me.astype(F32), 4, cap), lambda c: ret[0, 0:cap, c], fresh=True)
    pick = chosen(owner, flip(me, 1).astype(F32), 4, cap)
    halves[0].wait_recv()
    add(pick, lambda c: half[0, :, c])

    @pl.loop(0, steps)
    def _(t):
        e, f, n = t // NF, t % NF, t % LATE_RING
        for c in weights(t):
            c.wait()
        ffn_part(near[e, :, :, :].reshape(2 * slots, width), w1b, w3b, w2b, n, mid, yacc, f == 0, 2 * slots)

        @pl.when(f == NF - 1)
        def _():
            for q in (0, 1):
                late[q, pl.ds(pl.multiple_of(e * slots, slots), slots), :] = yacc[q * slots:(q + 1) * slots, :].astype(BF16)

        @pl.when(t + LATE_RING < steps)
        def _():
            for c in weights(t + LATE_RING):
                c.start()

    swap = pltpu.make_async_remote_copy(src_ref=late.at[1], dst_ref=late_half, send_sem=half_send.at[4], recv_sem=half_recv.at[4], device_id=dev(flip(me, 1)), device_id_type=MESH)
    swap.start()
    add(chosen(owner, me.astype(F32), 8, LATE * slots), lambda c: late[0, :, c])
    pick = chosen(owner, flip(me, 1).astype(F32), 8, LATE * slots)
    swap.wait_recv()
    add(pick, lambda c: late_half[:, c])
    for q in REMOTE:
        pick = chosen(chip, (flip(me, q) // 2).astype(F32), 6, chip_cap)
        copies[q].wait_recv()
        add(pick, lambda c: got[q // 2 - 1, :, c], last=q == REMOTE[-1])

    for copy in (*halves.values(), *copies.values(), swap):
        copy.wait_send()


def return_call(n, caps, ret, near, tok, goal, hidden, scale, w1, w3, w2):
    owners, _, width = ret.shape
    slots, ft = near.shape[2], w1.shape[2] // NF
    tokens = hidden.shape[0]
    cap, chip_cap = caps
    vmem = pl.BlockSpec(memory_space=pltpu.VMEM)
    return pl.pallas_call(
        functools.partial(return_kernel, cap, chip_cap),
        name=f'return_{cap}_{chip_cap}',
        out_shape=jax.ShapeDtypeStruct((tokens, width), BF16),
        in_specs=[vmem, vmem, vmem, vmem, vmem, pl.BlockSpec(memory_space=pltpu.SMEM), *[pl.BlockSpec(memory_space=pl.ANY)] * 3],
        out_specs=vmem,
        scratch_shapes=[
            pltpu.VMEM((owners // 2, cap, width), BF16),
            pltpu.VMEM((len(REMOTE), chip_cap, width), BF16),
            pltpu.VMEM((len(REMOTE), chip_cap, width), BF16),
            pltpu.VMEM((tokens, width), F32),
            pltpu.VMEM((2, LATE * slots, width), BF16),
            pltpu.VMEM((LATE * slots, width), BF16),
            pltpu.VMEM((2 * slots, ft), BF16),
            pltpu.VMEM((2 * slots, width), F32),
            pltpu.VMEM((LATE_RING, width, ft), BF16),
            pltpu.VMEM((LATE_RING, width, ft), BF16),
            pltpu.VMEM((LATE_RING, ft, width), BF16),
            pltpu.SemaphoreType.DMA((len(REMOTE),)),
            pltpu.SemaphoreType.DMA((len(REMOTE),)),
            pltpu.SemaphoreType.DMA((owners // 2 + 1,)),
            pltpu.SemaphoreType.DMA((owners // 2 + 1,)),
            pltpu.SemaphoreType.DMA((LATE_RING, 3)),
        ],
        compiler_params=pltpu.CompilerParams(collective_id=1 + n, has_side_effects=True, vmem_limit_bytes=34 * 1024 * 1024),
    )(ret, near, tok, goal, hidden, scale, w1, w3, w2)


def capacities(local, slots):
    full = [slots * n + 16 * (local - n) for n in range(1, local + 1)]
    chip = [2 * slots + 8 + (slots - 8) * n for n in range(local - 1)]
    return (*zip(full, chip), (local * slots, 2 * local * slots))


def solution(mesh):
    owners = mesh.shape['ep']

    def local_step(hidden, router_w, expert_ids, w_gate, w_up, w_down, post_scale):
        tokens = hidden.shape[0]
        local = w_gate.shape[0]
        slots = tokens // max(1, local * owners // 8)
        caps = capacities(local, slots)
        near, far, y_own, tok, goal, sizes, w1p, w3p, w2p = gather_call(hidden, expert_ids.T, router_w.T, w_gate, w_up, w_down, owners, caps)
        ret = expert_call(sizes, far, y_own, w1p, w3p, w2p, w_gate, w_up, w_down, caps)
        branches = [functools.partial(return_call, n, cap) for n, cap in enumerate(caps)]
        return lax.switch(sizes[0], branches, ret, near, tok, goal, hidden, post_scale, w_gate, w_up, w_down)

    tok_spec = P(('dp', 'ep'))
    return jax.shard_map(local_step, mesh=mesh, in_specs=(tok_spec, P(), tok_spec, P('ep'), P('ep'), P('ep'), P()), out_specs=tok_spec, check_vma=False)
```

```python
import functools

import jax
import jax.numpy as jnp
from jax import lax
from jax.experimental import pallas as pl
from jax.experimental.pallas import tpu as pltpu
from jax.sharding import PartitionSpec as P

MESH = pl.DeviceIdType.MESH
F32, BF16, I32 = jnp.float32, jnp.bfloat16, jnp.int32
NT = (((1,), (1,)), ((), ()))


def flip(idx, mask):
    out = idx
    for bit in (1, 2, 4):
        if mask & bit:
            out = out + bit - 2 * bit * ((idx // bit) % 2)
    return out


def dev(idx):
    return (lax.axis_index('dp'), idx)


def iota(shape, dim):
    return lax.broadcasted_iota(I32, shape, dim)


def weight_copies(w1, w3, w2, w1b, w3b, w2b, sem, e, f, n):
    ft = w1b.shape[2]
    cols = pl.ds(pl.multiple_of(f * ft, ft), ft)
    return (
        pltpu.make_async_copy(w1.at[e, :, cols], w1b.at[n], sem.at[n, 0]),
        pltpu.make_async_copy(w3.at[e, :, cols], w3b.at[n], sem.at[n, 1]),
        pltpu.make_async_copy(w2.at[e, cols, :], w2b.at[n], sem.at[n, 2]),
    )


def ffn_part(x, w1b, w3b, w2b, n, mid, yacc, fresh, m):
    for c in range(0, w1b.shape[2], 256):
        gate = jnp.dot(x, w1b[n, :, c:c + 256], preferred_element_type=F32)
        up = jnp.dot(x, w3b[n, :, c:c + 256], preferred_element_type=F32)
        mid[0:m, c:c + 256] = (gate * jax.nn.sigmoid(gate) * up).astype(BF16)
    for c in range(0, w2b.shape[2], 512):
        part = jnp.dot(mid[0:m, :], w2b[n, :, c:c + 512], preferred_element_type=F32)
        yacc[0:m, c:c + 512] = jnp.where(fresh, 0.0, yacc[0:m, c:c + 512]) + part


CHUNKS = 4
NF = 3
RING = 4
LATE_RING = 2
BRANCH_LANE = 127
LATE = 2


def gather_kernel(caps, hid_in, ids_in, wrt_in, scale_in, w1, w3, w2, near, far, y_own, tok, goal, plan, w1p, w3p, w2p, hid, ids, wrt, scale, pos, mid, yacc, land, ids_all, send, recv, id_send, id_recv, wsem, in_sem):
    me = lax.axis_index('ep')
    own = [pltpu.make_async_copy(src, dst, in_sem.at[n]) for n, (src, dst) in enumerate(((hid_in, hid), (ids_in, ids), (wrt_in, wrt), (scale_in, scale)))]
    for c in own:
        c.start()
    local, _, slots, _ = near.shape
    owners = 2 + far.shape[1]
    steps = (local - LATE) * NF

    def weights(t):
        return weight_copies(w1, w3, w2, w1p, w3p, w2p, wsem, local - 1 - t // NF, t % NF, t % RING)

    tokens, width = hid.shape
    experts = wrt.shape[0]
    rows = tokens // CHUNKS
    barrier = pltpu.get_barrier_semaphore()
    for q in range(1, owners):
        pl.semaphore_signal(barrier, inc=1, device_id=dev(flip(me, q)), device_id_type=MESH)
    pl.semaphore_wait(barrier, owners - 1)
    own[0].wait()
    own[1].wait()

    def piece(q, c):
        return (hid if q == 0 else land.at[q]).at[pl.ds(c * rows, rows)]

    def remote(q, c, n, to):
        return pltpu.make_async_remote_copy(src_ref=piece(q, c), dst_ref=land.at[q ^ to, pl.ds(c * rows, rows)], send_sem=send.at[n], recv_sem=recv.at[n], device_id=dev(flip(me, to)), device_id_type=MESH)

    id_copies = []
    for q in range(1, owners):
        id_copies.append(pltpu.make_async_remote_copy(src_ref=ids, dst_ref=ids_all.at[q], send_sem=id_send.at[q], recv_sem=id_recv.at[q], device_id=dev(flip(me, q)), device_id_type=MESH))
    for c in id_copies:
        c.start()
    x_order, y_order = (0, 1, 2, 3), (2, 3, 0, 1)
    to_x = {c: remote(0, c, c, 2) for c in x_order}
    to_y = {c: remote(0, c, 4 + c, 4) for c in y_order}
    for cx, cy in zip(x_order, y_order):
        to_x[cx].start()
        to_y[cy].start()
    to_mate = pltpu.make_async_remote_copy(src_ref=hid, dst_ref=land.at[1], send_sem=send.at[24], recv_sem=recv.at[24], device_id=dev(flip(me, 1)), device_id_type=MESH)
    to_mate.start()
    for t in range(RING):
        for c in weights(t):
            c.start()

    own[2].wait()
    own[3].wait()
    h = hid[...]
    w = wrt[...]
    w_hi = w.astype(BF16)
    rest = w - w_hi.astype(F32)
    w_mid = rest.astype(BF16)
    w_lo = (rest - w_mid.astype(F32)).astype(BF16)
    dot = functools.partial(lax.dot_general, dimension_numbers=NT, preferred_element_type=F32)
    logits = dot(h, w_hi) + (dot(h, w_mid) + dot(h, w_lo))
    ex = jnp.exp(logits - jnp.max(logits, axis=1, keepdims=True))
    prob = ex / jnp.sum(ex, axis=1, keepdims=True)
    ta, tb = iota((tokens, tokens), 0), iota((tokens, tokens), 1)
    eye = (ta == tb).astype(F32).astype(BF16)
    own_ids = ids[...].astype(F32)
    lane = iota((tokens, experts), 1).astype(F32)
    id_col = [dot(eye, jnp.broadcast_to(own_ids[k:k + 1], (8, tokens)).astype(BF16))[:, 0:1] for k in (0, 1)]
    pick = [(id_col[k] == lane).astype(F32) for k in (0, 1)]
    g = [jnp.sum(pick[k] * prob, axis=1, keepdims=True) for k in (0, 1)]
    total = g[0] + g[1]

    for c in id_copies:
        c.wait_recv()
    ids_all[0] = ids[...]
    counts = []
    for q in range(owners):
        both = ids_all[q]
        e_col = iota((experts, tokens), 0)
        hot = ((both[0:1] == e_col) | (both[1:2] == e_col)).astype(F32).astype(BF16)
        counts.append(dot(jnp.ones((8, tokens), BF16), hot))
    most = functools.reduce(jnp.maximum, counts)
    count = jnp.concatenate([c[0:1] for c in counts], axis=0)
    stride = jnp.where(most > 32.0, float(slots), jnp.where(most > 16.0, 32.0, 16.0))
    mark = lambda mask: mask.astype(F32).astype(BF16)
    plain = functools.partial(jnp.dot, preferred_element_type=F32)
    ea, eb = iota((experts, experts), 0), iota((experts, experts), 1)
    same, same_chip = ea // local == eb // local, ea // (2 * local) == eb // (2 * local)
    offset = plain(stride.astype(BF16), mark(same & (ea < eb)))
    need = jnp.max(plain(stride.astype(BF16), mark(same)), axis=1, keepdims=True)[0:1]
    need_chip = jnp.max(jnp.max(plain(count.astype(BF16), mark(same_chip)), axis=1, keepdims=True), axis=0, keepdims=True)
    branch = jnp.zeros((1, 1), F32)
    for limit, limit_chip in caps[:-1]:
        branch = branch + ((need > limit) | (need_chip > limit_chip)).astype(F32)
    rank = plain(mark(tb < ta), (pick[0] + pick[1]).astype(BF16))
    chip_first = plain(count.astype(BF16), mark(same_chip & (ea < eb)))[0:1]
    local_of = lane - jnp.floor(lane * (1.0 / local)) * local
    late_place = jnp.where(local_of < LATE, local_of * slots + rank, -1.0)
    late = [jnp.sum(pick[k] * late_place, axis=1, keepdims=True) for k in (0, 1)]
    slot = [jnp.sum(pick[k] * (rank + offset[0:1]), axis=1, keepdims=True) for k in (0, 1)]
    packed = [jnp.sum(pick[k] * (rank + chip_first), axis=1, keepdims=True) for k in (0, 1)]
    owner = [jnp.floor(id_col[k] * (1.0 / local)) for k in (0, 1)]
    wide = iota((tokens, 128), 1)
    table = jnp.zeros((tokens, 128), F32)
    for n, col in enumerate((g[0] / total, g[1] / total, *owner, *slot, *packed, *late, scale[0], scale[1])):
        table = jnp.where(wide == n, col, table)
    tok[...] = table

    e_row, n_col = iota((experts, 128), 0), iota((experts, 128), 1)
    e_of = jnp.where(n_col < local, me * local + n_col, flip(me, 1) * local + n_col - local)
    used = n_col < 2 * local
    held = plain(count.astype(BF16), mark(used & (e_row == e_of)))
    start = plain(count.astype(BF16), mark(used & (e_row // (2 * local) == me // 2) & (e_row < e_of)))
    base = plain(stride.astype(BF16), mark(used & (e_row // local == e_of // local) & (e_row < e_of)))
    base_size = plain(stride.astype(BF16), mark(used & (e_row == e_of)))
    lane_of = iota((owners, goal.shape[1]), 1)
    where_to = jnp.full((owners, goal.shape[1]), -1.0, F32)
    for n in range(2 * local):
        at = (lane_of - (n // local) * (goal.shape[1] // 2)).astype(F32) - base[0:1, n:n + 1]
        where_to = jnp.where((at >= 0.0) & (at < held[:, n:n + 1]), at + start[:, n:n + 1], where_to)
    goal[...] = where_to

    first, second = (jnp.concatenate([ids_all[q, k:k + 1] for q in range(owners)], axis=0) for k in (0, 1))
    marks = jnp.concatenate([((first == me * local + j) | (second == me * local + j)).astype(F32) for j in range(local)], axis=0)
    earlier = plain(marks.astype(BF16), (ta < tb).astype(F32).astype(BF16))
    pos[...] = jnp.where(marks > 0.5, earlier, -1.0)
    plan[...] = jnp.where(n_col[0:8] == BRANCH_LANE, branch, base_size).astype(I32)

    def pick_rows(q):
        at = iota((slots, tokens), 0).astype(F32)
        match = jnp.concatenate([(at == pos[j * owners + q:j * owners + q + 1, :]).astype(F32) for j in range(local)], axis=0).astype(BF16)

        def columns(cols):
            block = hid[:, cols] if q == 0 else land[q, :, cols]
            part = jnp.dot(match, block, preferred_element_type=F32).astype(BF16)
            for j in range(local):
                to = near.at[j, q] if q < 2 else far.at[j, q - 2]
                to[:, cols] = part[j * slots:(j + 1) * slots]

        if q < 6:
            @pl.loop(0, width // 512)
            def _(n):
                columns(pl.ds(pl.multiple_of(n * 512, 512), 512))
        else:
            for c in range(0, width, 512):
                columns(pl.ds(c, 512))

    def own_steps(first, last):
        @pl.loop(first, last)
        def _(t):
            e, f, n = local - 1 - t // NF, t % NF, t % RING
            for c in weights(t):
                c.wait()
            x = near[e, :, :, :].reshape(2 * slots, width)
            ffn_part(x, w1p, w3p, w2p, n, mid, yacc, f == 0, 2 * slots)

            @pl.when(f == NF - 1)
            def _():
                for q in (0, 1):
                    y_own[e - LATE, q, :, :] = yacc[q * slots:(q + 1) * slots, :].astype(BF16)

            @pl.when(t + RING < steps)
            def _():
                for c in weights(t + RING):
                    c.start()

    sent = [*to_x.values(), *to_y.values(), to_mate]

    def pass_on(q, c, n, to):
        copy = remote(q, c, n, to)
        copy.start()
        sent.append(copy)
        return copy

    pick_rows(0)
    to_mate.wait_recv()
    pick_rows(1)
    across, mates = {}, {2: [], 4: [], 6: []}
    for n, (cx, cy) in enumerate(zip(x_order, y_order)):
        if n < 2:
            own_steps(n * steps // 2, (n + 1) * steps // 2)
        to_x[cx].wait_recv()
        if cx in (0, 1):
            across[cx] = pass_on(2, cx, 8 + cx, 4)
        mates[2].append(pass_on(2, cx, 12 + cx, 1))
        to_y[cy].wait_recv()
        if cy in (2, 3):
            across[cy] = pass_on(4, cy, 8 + cy, 2)
        mates[4].append(pass_on(4, cy, 16 + cy, 1))
    for q in (2, 4):
        pick_rows(q)
    for q in (2, 4):
        for m in mates[q]:
            m.wait_recv()
        pick_rows(q + 1)
    for c in (0, 2, 1, 3):
        across[c].wait_recv()
        mates[6].append(pass_on(6, c, 20 + c, 1))
    pick_rows(6)
    for m in mates[6]:
        m.wait_recv()
    pick_rows(7)
    for m in sent:
        m.wait_send()
    for c in id_copies:
        c.wait_send()


def gather_call(hidden, ids_t, wr_t, scale, w1, w3, w2, owners, caps):
    tokens, width = hidden.shape
    experts = wr_t.shape[0]
    local, _, ffn = w1.shape
    slots = caps[-1][0] // local
    ft = ffn // NF
    vmem = pl.BlockSpec(memory_space=pltpu.VMEM)
    hbm = pl.BlockSpec(memory_space=pl.ANY)
    return pl.pallas_call(
        functools.partial(gather_kernel, caps),
        name='gather_tokens',
        out_shape=(
            pltpu.VMEM((local, 2, slots, width), BF16),
            pltpu.VMEM((local, owners - 2, slots, width), BF16),
            pltpu.VMEM((local - LATE, 2, slots, width), BF16),
            jax.ShapeDtypeStruct((tokens, 128), F32),
            jax.ShapeDtypeStruct((owners, 2 * local * slots), F32),
            jax.ShapeDtypeStruct((8, 128), I32),
            pltpu.VMEM((RING, width, ft), BF16),
            pltpu.VMEM((RING, width, ft), BF16),
            pltpu.VMEM((RING, ft, width), BF16),
        ),
        in_specs=[hbm, *[pl.BlockSpec(memory_space=pltpu.HBM)] * 3, hbm, hbm, hbm],
        out_specs=(vmem,) * 9,
        scratch_shapes=[
            pltpu.VMEM((tokens, width), BF16),
            pltpu.VMEM((2, tokens), I32),
            pltpu.VMEM((experts, width), F32),
            pltpu.SMEM((2,), F32),
            pltpu.VMEM((local * owners, tokens), F32),
            pltpu.VMEM((2 * slots, ft), BF16),
            pltpu.VMEM((2 * slots, width), F32),
            pltpu.VMEM((owners, tokens, width), BF16),
            pltpu.VMEM((owners, 2, tokens), I32),
            pltpu.SemaphoreType.DMA((25,)),
            pltpu.SemaphoreType.DMA((25,)),
            pltpu.SemaphoreType.DMA((owners,)),
            pltpu.SemaphoreType.DMA((owners,)),
            pltpu.SemaphoreType.DMA((RING, 3)),
            pltpu.SemaphoreType.DMA((4,)),
        ],
        compiler_params=pltpu.CompilerParams(collective_id=0, has_side_effects=True, vmem_limit_bytes=13 * 1024 * 1024),
    )(hidden, *(pltpu.with_memory_space_constraint(x, pltpu.HBM) for x in (ids_t, wr_t, scale)), w1, w3, w2)


def expert_kernel(caps, info, rows, y_own, _w1b, _w3b, _w2b, w1, w3, w2, ret, w1b, w3b, w2b, mid, yacc, plan, wsem):
    local, distant, slots, width = rows.shape
    owners = distant + 2
    steps = local * NF
    done = (local - LATE) * NF

    size = [info[0, j] for j in range(local)]
    branch = info[0, BRANCH_LANE]
    for j in range(local):
        rank = jnp.int32(j - LATE if j >= LATE else local - LATE)
        offset = jnp.int32(0)
        for i in range(local):
            if i < LATE and j < LATE and i != j:
                ahead = (size[i] >= size[j]) if i < j else (size[i] > size[j])
                rank = rank + ahead.astype(I32)
            if i < j:
                offset = offset + size[i]
        plan[0, rank] = jnp.int32(j)
        plan[1, rank] = size[j]
        plan[2, rank] = offset
    used = size[0]
    for j in range(1, local):
        used = used + size[j]

    def part_of(t):
        turn = jnp.where(t < NF, 0, 2 * NF - RING)
        return (t % NF + turn) % NF

    def weights(t):
        return weight_copies(w1, w3, w2, w1b, w3b, w2b, wsem, plan[0, t // NF], part_of(t), (t + done - NF) % RING)

    limit = jnp.int32(caps[0][0])
    for n in range(1, len(caps)):
        limit = jnp.where(branch >= n, caps[n][0], limit)

    @pl.loop(used // 16, limit // 16)
    def _(n):
        blank = pl.ds(pl.multiple_of(n * 16, 16), 16)
        for q in range(owners):
            ret[q, blank, :] = jnp.zeros((16, width), BF16)

    @pl.loop(0, steps)
    def _(t):
        r, f, n = t // NF, t % NF, (t + done - NF) % RING
        e = plan[0, r]

        @pl.when(t >= RING)
        def _():
            for c in weights(t):
                c.wait()

        for size in (16, 32, slots):
            m = size * distant

            @pl.when(plan[1, r] == size)
            def _():
                x = rows[e, :, 0:size, :].reshape(m, width)
                ffn_part(x, w1b, w3b, w2b, n, mid, yacc, f == 0, m)

                @pl.when(f == NF - 1)
                def _():
                    first = pl.multiple_of(plan[2, r], 16)
                    for q in (0, 1):
                        mine = y_own[jnp.maximum(e - LATE, 0), q, 0:size, :]
                        ret[q, pl.ds(first, size), :] = jnp.where(e >= LATE, mine, jnp.zeros_like(mine))
                    for q in range(2, owners):
                        ret[q, pl.ds(first, size), :] = yacc[(q - 2) * size:(q - 1) * size, :].astype(BF16)

        @pl.when(t + RING < steps)
        def _():
            for c in weights(t + RING):
                c.start()


def expert_call(sizes, rows, y_own, w1p, w3p, w2p, w1, w3, w2, caps):
    local, distant, slots, width = rows.shape
    owners = distant + 2
    ft = w1p.shape[2]
    hbm = pl.BlockSpec(memory_space=pl.ANY)
    vmem = pl.BlockSpec(memory_space=pltpu.VMEM)
    flops = 3 * 2 * local * slots * owners * width * ft * NF // 2
    return pl.pallas_call(
        functools.partial(expert_kernel, caps),
        name='experts',
        out_shape=(
            pltpu.VMEM((owners, caps[-1][0], width), BF16),
            pltpu.VMEM(w1p.shape, BF16),
            pltpu.VMEM(w3p.shape, BF16),
            pltpu.VMEM(w2p.shape, BF16),
        ),
        in_specs=[vmem] * 6 + [hbm] * 3,
        out_specs=(vmem, vmem, vmem, vmem),
        input_output_aliases={3: 1, 4: 2, 5: 3},
        scratch_shapes=[
            pltpu.VMEM((distant * slots, ft), BF16),
            pltpu.VMEM((distant * slots, width), F32),
            pltpu.SMEM((3, local), I32),
            pltpu.SemaphoreType.DMA((RING, 3)),
        ],
        compiler_params=pltpu.CompilerParams(vmem_limit_bytes=12 * 1024 * 1024),
        cost_estimate=pl.CostEstimate(flops=flops, bytes_accessed=3 * 2 * local * width * ft * NF, transcendentals=0),
    )(sizes, rows, y_own, w1p, w3p, w2p, w1, w3, w2)[0]


REMOTE = (2, 4, 6)


def return_kernel(cap, chip_cap, ret, near, tok, goal, hid, w1, w3, w2, out, half, pack, got, acc, late, late_half, mid, yacc, w1b, w3b, w2b, send, recv, half_send, half_recv, wsem):
    me = lax.axis_index('ep')
    slots = near.shape[2]
    steps = LATE * NF

    def weights(t):
        return weight_copies(w1, w3, w2, w1b, w3b, w2b, wsem, t // NF, t % NF, t % LATE_RING)

    tokens, width = hid.shape
    lanes = goal.shape[1] // 2
    barrier = pltpu.get_barrier_semaphore()
    for q in (1, *REMOTE):
        pl.semaphore_signal(barrier, inc=1, device_id=dev(flip(me, q)), device_id_type=MESH)
    pl.semaphore_wait(barrier, 1 + len(REMOTE))
    halves, copies = {}, {}
    for q in (*REMOTE, 0):
        halves[q] = pltpu.make_async_remote_copy(src_ref=ret.at[q + 1, pl.ds(0, cap)], dst_ref=half.at[q // 2], send_sem=half_send.at[q // 2], recv_sem=half_recv.at[q // 2], device_id=dev(flip(me, 1)), device_id_type=MESH)
        halves[q].start()

    for q in REMOTE:
        row = iota((chip_cap, cap), 0).astype(F32)
        mine = (row == goal[q:q + 1, 0:cap]).astype(F32).astype(BF16)
        theirs = (row == goal[q:q + 1, lanes:lanes + cap]).astype(F32).astype(BF16)
        halves[q].wait_recv()
        for c in range(0, width, 512):
            part = jnp.dot(mine, ret[q, 0:cap, c:c + 512], preferred_element_type=F32)
            part = part + jnp.dot(theirs, half[q // 2, :, c:c + 512], preferred_element_type=F32)
            pack[q // 2 - 1, :, c:c + 512] = part.astype(BF16)
        copies[q] = pltpu.make_async_remote_copy(src_ref=pack.at[q // 2 - 1], dst_ref=got.at[q // 2 - 1], send_sem=send.at[q // 2 - 1], recv_sem=recv.at[q // 2 - 1], device_id=dev(flip(me, q)), device_id_type=MESH)
        copies[q].start()

    for t in range(LATE_RING):
        for c in weights(t):
            c.start()
    table = tok[...]

    def chosen(column, peer, at, count):
        lane = iota((tokens, count), 1).astype(F32)
        return jnp.concatenate([((column[k] == peer) & (table[:, at + k:at + k + 1] == lane)).astype(F32) for k in (0, 1)], axis=0).astype(BF16)

    owner = [table[:, 2 + k:3 + k] for k in (0, 1)]
    chip = [jnp.floor(o * 0.5) for o in owner]

    gate = [table[:, k:k + 1] for k in (0, 1)]
    scale = [table[:, 10 + k:11 + k] for k in (0, 1)]

    def add(pick, block, fresh=False, last=False):
        @pl.loop(0, width // 512)
        def _(n):
            cols = pl.ds(pl.multiple_of(n * 512, 512), 512)
            part = jnp.dot(pick, block(cols), preferred_element_type=F32)
            mixed = gate[0] * part[0:tokens] + gate[1] * part[tokens:2 * tokens]
            if not fresh:
                mixed = acc[:, cols] + mixed
            if last:
                out[:, cols] = (scale[0] * hid[:, cols].astype(F32) + scale[1] * mixed).astype(BF16)
            else:
                acc[:, cols] = mixed

    add(chosen(owner, me.astype(F32), 4, cap), lambda c: ret[0, 0:cap, c], fresh=True)
    pick = chosen(owner, flip(me, 1).astype(F32), 4, cap)
    halves[0].wait_recv()
    add(pick, lambda c: half[0, :, c])

    @pl.loop(0, steps)
    def _(t):
        e, f, n = t // NF, t % NF, t % LATE_RING
        for c in weights(t):
            c.wait()
        ffn_part(near[e, :, :, :].reshape(2 * slots, width), w1b, w3b, w2b, n, mid, yacc, f == 0, 2 * slots)

        @pl.when(f == NF - 1)
        def _():
            for q in (0, 1):
                late[q, pl.ds(pl.multiple_of(e * slots, slots), slots), :] = yacc[q * slots:(q + 1) * slots, :].astype(BF16)

        @pl.when(t + LATE_RING < steps)
        def _():
            for c in weights(t + LATE_RING):
                c.start()

    swap = pltpu.make_async_remote_copy(src_ref=late.at[1], dst_ref=late_half, send_sem=half_send.at[4], recv_sem=half_recv.at[4], device_id=dev(flip(me, 1)), device_id_type=MESH)
    swap.start()
    add(chosen(owner, me.astype(F32), 8, LATE * slots), lambda c: late[0, :, c])
    pick = chosen(owner, flip(me, 1).astype(F32), 8, LATE * slots)
    swap.wait_recv()
    add(pick, lambda c: late_half[:, c])
    for q in REMOTE:
        pick = chosen(chip, (flip(me, q) // 2).astype(F32), 6, chip_cap)
        copies[q].wait_recv()
        add(pick, lambda c: got[q // 2 - 1, :, c], last=q == REMOTE[-1])

    for copy in (*halves.values(), *copies.values(), swap):
        copy.wait_send()


def return_call(n, caps, ret, near, tok, goal, hidden, w1, w3, w2):
    owners, _, width = ret.shape
    slots, ft = near.shape[2], w1.shape[2] // NF
    tokens = hidden.shape[0]
    cap, chip_cap = caps
    vmem = pl.BlockSpec(memory_space=pltpu.VMEM)
    return pl.pallas_call(
        functools.partial(return_kernel, cap, chip_cap),
        name=f'return_{cap}_{chip_cap}',
        out_shape=jax.ShapeDtypeStruct((tokens, width), BF16),
        in_specs=[vmem] * 5 + [pl.BlockSpec(memory_space=pl.ANY)] * 3,
        out_specs=vmem,
        scratch_shapes=[
            pltpu.VMEM((owners // 2, cap, width), BF16),
            pltpu.VMEM((len(REMOTE), chip_cap, width), BF16),
            pltpu.VMEM((len(REMOTE), chip_cap, width), BF16),
            pltpu.VMEM((tokens, width), F32),
            pltpu.VMEM((2, LATE * slots, width), BF16),
            pltpu.VMEM((LATE * slots, width), BF16),
            pltpu.VMEM((2 * slots, ft), BF16),
            pltpu.VMEM((2 * slots, width), F32),
            pltpu.VMEM((LATE_RING, width, ft), BF16),
            pltpu.VMEM((LATE_RING, width, ft), BF16),
            pltpu.VMEM((LATE_RING, ft, width), BF16),
            pltpu.SemaphoreType.DMA((len(REMOTE),)),
            pltpu.SemaphoreType.DMA((len(REMOTE),)),
            pltpu.SemaphoreType.DMA((owners // 2 + 1,)),
            pltpu.SemaphoreType.DMA((owners // 2 + 1,)),
            pltpu.SemaphoreType.DMA((LATE_RING, 3)),
        ],
        compiler_params=pltpu.CompilerParams(collective_id=1 + n, has_side_effects=True, vmem_limit_bytes=34 * 1024 * 1024),
    )(ret, near, tok, goal, hidden, w1, w3, w2)


def capacities(local, slots):
    full = [slots * n + 16 * (local - n) for n in range(1, local + 1)]
    chip = [2 * slots + 8 + (slots - 8) * n for n in range(local - 1)]
    return (*zip(full, chip), (local * slots, 2 * local * slots))


def solution(mesh):
    owners = mesh.shape['ep']

    def local_step(hidden, router_w, expert_ids, w_gate, w_up, w_down, post_scale):
        tokens = hidden.shape[0]
        local = w_gate.shape[0]
        slots = tokens // max(1, local * owners // 8)
        caps = capacities(local, slots)
        near, far, y_own, tok, goal, plan, w1p, w3p, w2p = gather_call(hidden, expert_ids.T, router_w.T, post_scale, w_gate, w_up, w_down, owners, caps)
        ret = expert_call(plan, far, y_own, w1p, w3p, w2p, w_gate, w_up, w_down, caps)
        branches = [functools.partial(return_call, n, cap) for n, cap in enumerate(caps)]
        return lax.switch(plan[0, BRANCH_LANE], branches, ret, near, tok, goal, hidden, w_gate, w_up, w_down)

    tok_spec = P(('dp', 'ep'))
    return jax.shard_map(local_step, mesh=mesh, in_specs=(tok_spec, P(), tok_spec, P('ep'), P('ep'), P('ep'), P()), out_specs=tok_spec, check_vma=False)
```

```python
import functools

import jax
import jax.numpy as jnp
from jax import lax
from jax.experimental import pallas as pl
from jax.experimental.pallas import tpu as pltpu
from jax.sharding import PartitionSpec as P

MESH = pl.DeviceIdType.MESH
F32, BF16, I32 = jnp.float32, jnp.bfloat16, jnp.int32
NT = (((1,), (1,)), ((), ()))


def flip(idx, mask):
    out = idx
    for bit in (1, 2, 4):
        if mask & bit:
            out = out + bit - 2 * bit * ((idx // bit) % 2)
    return out


def dev(idx):
    return (lax.axis_index('dp'), idx)


def iota(shape, dim):
    return lax.broadcasted_iota(I32, shape, dim)


def weight_copies(w1, w3, w2, w1b, w3b, w2b, sem, e, f, n):
    ft = w1b.shape[2]
    cols = pl.ds(pl.multiple_of(f * ft, ft), ft)
    return (
        pltpu.make_async_copy(w1.at[e, :, cols], w1b.at[n], sem.at[n, 0]),
        pltpu.make_async_copy(w3.at[e, :, cols], w3b.at[n], sem.at[n, 1]),
        pltpu.make_async_copy(w2.at[e, cols, :], w2b.at[n], sem.at[n, 2]),
    )


def ffn_part(x, w1b, w3b, w2b, n, mid, yacc, fresh, m):
    for c in range(0, w1b.shape[2], 256):
        gate = jnp.dot(x, w1b[n, :, c:c + 256], preferred_element_type=F32)
        up = jnp.dot(x, w3b[n, :, c:c + 256], preferred_element_type=F32)
        mid[0:m, c:c + 256] = (gate * jax.nn.sigmoid(gate) * up).astype(BF16)
    for c in range(0, w2b.shape[2], 512):
        part = jnp.dot(mid[0:m, :], w2b[n, :, c:c + 512], preferred_element_type=F32)
        yacc[0:m, c:c + 512] = jnp.where(fresh, 0.0, yacc[0:m, c:c + 512]) + part


CHUNKS = 4
NF = 3
RING = 4
LATE_RING = 2
BRANCH_LANE = 127
LATE = 2


def gather_kernel(caps, hid_in, ids_in, wrt_in, scale_in, w1, w3, w2, near, far, y_own, tok, goal, plan, which, w1p, w3p, w2p, hid, ids, wrt, scale, pos, mid, yacc, land, ids_all, send, recv, id_send, id_recv, wsem, in_sem):
    me = lax.axis_index('ep')
    own = [pltpu.make_async_copy(src, dst, in_sem.at[n]) for n, (src, dst) in enumerate(((hid_in, hid), (ids_in, ids), (wrt_in, wrt), (scale_in, scale)))]
    for c in own:
        c.start()
    local, _, slots, _ = near.shape
    owners = 2 + far.shape[1]
    steps = (local - LATE) * NF

    def weights(t):
        return weight_copies(w1, w3, w2, w1p, w3p, w2p, wsem, local - 1 - t // NF, t % NF, t % RING)

    tokens, width = hid.shape
    experts = wrt.shape[0]
    rows = tokens // CHUNKS
    barrier = pltpu.get_barrier_semaphore()
    for q in range(1, owners):
        pl.semaphore_signal(barrier, inc=1, device_id=dev(flip(me, q)), device_id_type=MESH)
    pl.semaphore_wait(barrier, owners - 1)
    own[0].wait()
    own[1].wait()

    def piece(q, c):
        return (hid if q == 0 else land.at[q]).at[pl.ds(c * rows, rows)]

    def remote(q, c, n, to):
        return pltpu.make_async_remote_copy(src_ref=piece(q, c), dst_ref=land.at[q ^ to, pl.ds(c * rows, rows)], send_sem=send.at[n], recv_sem=recv.at[n], device_id=dev(flip(me, to)), device_id_type=MESH)

    id_copies = []
    for q in range(1, owners):
        id_copies.append(pltpu.make_async_remote_copy(src_ref=ids, dst_ref=ids_all.at[q], send_sem=id_send.at[q], recv_sem=id_recv.at[q], device_id=dev(flip(me, q)), device_id_type=MESH))
    x_order, y_order = (0, 1, 2, 3), (2, 3, 0, 1)
    to_x = {c: remote(0, c, c, 2) for c in x_order}
    to_y = {c: remote(0, c, 4 + c, 4) for c in y_order}
    for cx, cy in zip(x_order, y_order):
        to_x[cx].start()
        to_y[cy].start()
        if cx == 0:
            for c in id_copies:
                c.start()
    to_mate = pltpu.make_async_remote_copy(src_ref=hid, dst_ref=land.at[1], send_sem=send.at[24], recv_sem=recv.at[24], device_id=dev(flip(me, 1)), device_id_type=MESH)
    to_mate.start()
    for t in range(RING):
        for c in weights(t):
            c.start()

    own[2].wait()
    own[3].wait()
    h = hid[...]
    w = wrt[...]
    w_hi = w.astype(BF16)
    rest = w - w_hi.astype(F32)
    w_mid = rest.astype(BF16)
    w_lo = (rest - w_mid.astype(F32)).astype(BF16)
    dot = functools.partial(lax.dot_general, dimension_numbers=NT, preferred_element_type=F32)
    logits = dot(h, w_hi) + (dot(h, w_mid) + dot(h, w_lo))
    ex = jnp.exp(logits - jnp.max(logits, axis=1, keepdims=True))
    prob = ex / jnp.sum(ex, axis=1, keepdims=True)
    ta, tb = iota((tokens, tokens), 0), iota((tokens, tokens), 1)
    eye = (ta == tb).astype(F32).astype(BF16)
    own_ids = ids[...].astype(F32)
    lane = iota((tokens, experts), 1).astype(F32)
    id_col = [dot(eye, jnp.broadcast_to(own_ids[k:k + 1], (8, tokens)).astype(BF16))[:, 0:1] for k in (0, 1)]
    pick = [(id_col[k] == lane).astype(F32) for k in (0, 1)]
    g = [jnp.sum(pick[k] * prob, axis=1, keepdims=True) for k in (0, 1)]
    total = g[0] + g[1]

    for c in id_copies:
        c.wait_recv()
    ids_all[0] = ids[...]
    counts = []
    for q in range(owners):
        both = ids_all[q]
        e_col = iota((experts, tokens), 0)
        hot = ((both[0:1] == e_col) | (both[1:2] == e_col)).astype(F32).astype(BF16)
        counts.append(dot(jnp.ones((8, tokens), BF16), hot))
    most = functools.reduce(jnp.maximum, counts)
    count = jnp.concatenate([c[0:1] for c in counts], axis=0)
    stride = jnp.where(most > 32.0, float(slots), jnp.where(most > 16.0, 32.0, 16.0))
    mark = lambda mask: mask.astype(F32).astype(BF16)
    plain = functools.partial(jnp.dot, preferred_element_type=F32)
    ea, eb = iota((experts, experts), 0), iota((experts, experts), 1)
    same, same_chip = ea // local == eb // local, ea // (2 * local) == eb // (2 * local)
    offset = plain(stride.astype(BF16), mark(same & (ea < eb)))
    need = jnp.max(plain(stride.astype(BF16), mark(same)), axis=1, keepdims=True)[0:1]
    need_chip = jnp.max(jnp.max(plain(count.astype(BF16), mark(same_chip)), axis=1, keepdims=True), axis=0, keepdims=True)
    branch = jnp.zeros((1, 1), F32)
    for limit, limit_chip in caps[:-1]:
        branch = branch + ((need > limit) | (need_chip > limit_chip)).astype(F32)
    which[0] = jnp.max(branch).astype(I32)
    rank = plain(mark(tb < ta), (pick[0] + pick[1]).astype(BF16))
    chip_first = plain(count.astype(BF16), mark(same_chip & (ea < eb)))[0:1]
    local_of = lane - jnp.floor(lane * (1.0 / local)) * local
    late_place = jnp.where(local_of < LATE, local_of * slots + rank, -1.0)
    late = [jnp.sum(pick[k] * late_place, axis=1, keepdims=True) for k in (0, 1)]
    slot = [jnp.sum(pick[k] * (rank + offset[0:1]), axis=1, keepdims=True) for k in (0, 1)]
    packed = [jnp.sum(pick[k] * (rank + chip_first), axis=1, keepdims=True) for k in (0, 1)]
    owner = [jnp.floor(id_col[k] * (1.0 / local)) for k in (0, 1)]
    wide = iota((tokens, 128), 1)
    table = jnp.zeros((tokens, 128), F32)
    for n, col in enumerate((g[0] / total, g[1] / total, *owner, *slot, *packed, *late, scale[0], scale[1])):
        table = jnp.where(wide == n, col, table)
    tok[...] = table

    e_row, n_col = iota((experts, 128), 0), iota((experts, 128), 1)
    e_of = jnp.where(n_col < local, me * local + n_col, flip(me, 1) * local + n_col - local)
    used = n_col < 2 * local
    held = plain(count.astype(BF16), mark(used & (e_row == e_of)))
    start = plain(count.astype(BF16), mark(used & (e_row // (2 * local) == me // 2) & (e_row < e_of)))
    base = plain(stride.astype(BF16), mark(used & (e_row // local == e_of // local) & (e_row < e_of)))
    base_size = plain(stride.astype(BF16), mark(used & (e_row == e_of)))
    lane_of = iota((owners, goal.shape[1]), 1)
    where_to = jnp.full((owners, goal.shape[1]), -1.0, F32)
    for n in range(2 * local):
        at = (lane_of - (n // local) * (goal.shape[1] // 2)).astype(F32) - base[0:1, n:n + 1]
        where_to = jnp.where((at >= 0.0) & (at < held[:, n:n + 1]), at + start[:, n:n + 1], where_to)
    goal[...] = where_to

    first, second = (jnp.concatenate([ids_all[q, k:k + 1] for q in range(owners)], axis=0) for k in (0, 1))
    marks = jnp.concatenate([((first == me * local + j) | (second == me * local + j)).astype(F32) for j in range(local)], axis=0)
    earlier = plain(marks.astype(BF16), (ta < tb).astype(F32).astype(BF16))
    pos[...] = jnp.where(marks > 0.5, earlier, -1.0)
    plan[...] = jnp.where(n_col[0:8] == BRANCH_LANE, branch, base_size).astype(I32)

    def pick_rows(q):
        at = iota((slots, tokens), 0).astype(F32)
        match = jnp.concatenate([(at == pos[j * owners + q:j * owners + q + 1, :]).astype(F32) for j in range(local)], axis=0).astype(BF16)

        def columns(cols):
            block = hid[:, cols] if q == 0 else land[q, :, cols]
            part = jnp.dot(match, block, preferred_element_type=F32).astype(BF16)
            for j in range(local):
                to = near.at[j, q] if q < 2 else far.at[j, q - 2]
                to[:, cols] = part[j * slots:(j + 1) * slots]

        if q < 6:
            @pl.loop(0, width // 512)
            def _(n):
                columns(pl.ds(pl.multiple_of(n * 512, 512), 512))
        else:
            for c in range(0, width, 512):
                columns(pl.ds(c, 512))

    def own_steps(first, last):
        @pl.loop(first, last)
        def _(t):
            e, f, n = local - 1 - t // NF, t % NF, t % RING
            for c in weights(t):
                c.wait()
            x = near[e, :, :, :].reshape(2 * slots, width)
            ffn_part(x, w1p, w3p, w2p, n, mid, yacc, f == 0, 2 * slots)

            @pl.when(f == NF - 1)
            def _():
                for q in (0, 1):
                    y_own[e - LATE, q, :, :] = yacc[q * slots:(q + 1) * slots, :].astype(BF16)

            @pl.when(t + RING < steps)
            def _():
                for c in weights(t + RING):
                    c.start()

    sent = [*to_x.values(), *to_y.values(), to_mate]

    def pass_on(q, c, n, to):
        copy = remote(q, c, n, to)
        copy.start()
        sent.append(copy)
        return copy

    pick_rows(0)
    to_mate.wait_recv()
    pick_rows(1)
    across, mates = {}, {2: [], 4: [], 6: []}
    for n, (cx, cy) in enumerate(zip(x_order, y_order)):
        if n < 2:
            own_steps(n * steps // 2, (n + 1) * steps // 2)
        to_x[cx].wait_recv()
        if cx in (0, 1):
            across[cx] = pass_on(2, cx, 8 + cx, 4)
        mates[2].append(pass_on(2, cx, 12 + cx, 1))
        to_y[cy].wait_recv()
        if cy in (2, 3):
            across[cy] = pass_on(4, cy, 8 + cy, 2)
        mates[4].append(pass_on(4, cy, 16 + cy, 1))
    for q in (2, 4):
        pick_rows(q)
    for q in (2, 4):
        for m in mates[q]:
            m.wait_recv()
        pick_rows(q + 1)
    for c in (0, 2, 1, 3):
        across[c].wait_recv()
        mates[6].append(pass_on(6, c, 20 + c, 1))
    pick_rows(6)
    for m in mates[6]:
        m.wait_recv()
    pick_rows(7)
    for m in sent:
        m.wait_send()
    for c in id_copies:
        c.wait_send()


def gather_call(hidden, ids_t, wr_t, scale, w1, w3, w2, owners, caps):
    tokens, width = hidden.shape
    experts = wr_t.shape[0]
    local, _, ffn = w1.shape
    slots = caps[-1][0] // local
    ft = ffn // NF
    vmem = pl.BlockSpec(memory_space=pltpu.VMEM)
    hbm = pl.BlockSpec(memory_space=pl.ANY)
    return pl.pallas_call(
        functools.partial(gather_kernel, caps),
        name='gather_tokens',
        out_shape=(
            pltpu.VMEM((local, 2, slots, width), BF16),
            pltpu.VMEM((local, owners - 2, slots, width), BF16),
            pltpu.VMEM((local - LATE, 2, slots, width), BF16),
            jax.ShapeDtypeStruct((tokens, 128), F32),
            jax.ShapeDtypeStruct((owners, 2 * local * slots), F32),
            jax.ShapeDtypeStruct((8, 128), I32),
            jax.ShapeDtypeStruct((1,), I32),
            pltpu.VMEM((RING, width, ft), BF16),
            pltpu.VMEM((RING, width, ft), BF16),
            pltpu.VMEM((RING, ft, width), BF16),
        ),
        in_specs=[hbm, *[pl.BlockSpec(memory_space=pltpu.HBM)] * 3, hbm, hbm, hbm],
        out_specs=(*[vmem] * 6, pl.BlockSpec(memory_space=pltpu.SMEM), *[vmem] * 3),
        scratch_shapes=[
            pltpu.VMEM((tokens, width), BF16),
            pltpu.VMEM((2, tokens), I32),
            pltpu.VMEM((experts, width), F32),
            pltpu.SMEM((2,), F32),
            pltpu.VMEM((local * owners, tokens), F32),
            pltpu.VMEM((2 * slots, ft), BF16),
            pltpu.VMEM((2 * slots, width), F32),
            pltpu.VMEM((owners, tokens, width), BF16),
            pltpu.VMEM((owners, 2, tokens), I32),
            pltpu.SemaphoreType.DMA((25,)),
            pltpu.SemaphoreType.DMA((25,)),
            pltpu.SemaphoreType.DMA((owners,)),
            pltpu.SemaphoreType.DMA((owners,)),
            pltpu.SemaphoreType.DMA((RING, 3)),
            pltpu.SemaphoreType.DMA((4,)),
        ],
        compiler_params=pltpu.CompilerParams(collective_id=0, has_side_effects=True, vmem_limit_bytes=13 * 1024 * 1024),
    )(hidden, *(pltpu.with_memory_space_constraint(x, pltpu.HBM) for x in (ids_t, wr_t, scale)), w1, w3, w2)


def expert_kernel(caps, info, rows, y_own, _w1b, _w3b, _w2b, w1, w3, w2, ret, w1b, w3b, w2b, mid, yacc, plan, wsem):
    local, distant, slots, width = rows.shape
    owners = distant + 2
    steps = local * NF
    done = (local - LATE) * NF

    size = [info[0, j] for j in range(local)]
    branch = info[0, BRANCH_LANE]
    for j in range(local):
        rank = jnp.int32(j - LATE if j >= LATE else local - LATE)
        offset = jnp.int32(0)
        for i in range(local):
            if i < LATE and j < LATE and i != j:
                ahead = (size[i] >= size[j]) if i < j else (size[i] > size[j])
                rank = rank + ahead.astype(I32)
            if i < j:
                offset = offset + size[i]
        plan[0, rank] = jnp.int32(j)
        plan[1, rank] = size[j]
        plan[2, rank] = offset
    used = size[0]
    for j in range(1, local):
        used = used + size[j]

    def part_of(t):
        turn = jnp.where(t < NF, 0, 2 * NF - RING)
        return (t % NF + turn) % NF

    def weights(t):
        return weight_copies(w1, w3, w2, w1b, w3b, w2b, wsem, plan[0, t // NF], part_of(t), (t + done - NF) % RING)

    limit = jnp.int32(caps[0][0])
    for n in range(1, len(caps)):
        limit = jnp.where(branch >= n, caps[n][0], limit)

    @pl.loop(used // 16, limit // 16)
    def _(n):
        blank = pl.ds(pl.multiple_of(n * 16, 16), 16)
        for q in range(owners):
            ret[q, blank, :] = jnp.zeros((16, width), BF16)

    @pl.loop(0, steps)
    def _(t):
        r, f, n = t // NF, t % NF, (t + done - NF) % RING
        e = plan[0, r]

        @pl.when(t >= RING)
        def _():
            for c in weights(t):
                c.wait()

        for size in (16, 32, slots):
            m = size * distant

            @pl.when(plan[1, r] == size)
            def _():
                x = rows[e, :, 0:size, :].reshape(m, width)
                ffn_part(x, w1b, w3b, w2b, n, mid, yacc, f == 0, m)

                @pl.when(f == NF - 1)
                def _():
                    first = pl.multiple_of(plan[2, r], 16)
                    for q in (0, 1):
                        mine = y_own[jnp.maximum(e - LATE, 0), q, 0:size, :]
                        ret[q, pl.ds(first, size), :] = jnp.where(e >= LATE, mine, jnp.zeros_like(mine))
                    for q in range(2, owners):
                        ret[q, pl.ds(first, size), :] = yacc[(q - 2) * size:(q - 1) * size, :].astype(BF16)

        @pl.when(t + RING < steps)
        def _():
            for c in weights(t + RING):
                c.start()


def expert_call(sizes, rows, y_own, w1p, w3p, w2p, w1, w3, w2, caps):
    local, distant, slots, width = rows.shape
    owners = distant + 2
    ft = w1p.shape[2]
    hbm = pl.BlockSpec(memory_space=pl.ANY)
    vmem = pl.BlockSpec(memory_space=pltpu.VMEM)
    flops = 3 * 2 * local * slots * owners * width * ft * NF // 2
    return pl.pallas_call(
        functools.partial(expert_kernel, caps),
        name='experts',
        out_shape=(
            pltpu.VMEM((owners, caps[-1][0], width), BF16),
            pltpu.VMEM(w1p.shape, BF16),
            pltpu.VMEM(w3p.shape, BF16),
            pltpu.VMEM(w2p.shape, BF16),
        ),
        in_specs=[vmem] * 6 + [hbm] * 3,
        out_specs=(vmem, vmem, vmem, vmem),
        input_output_aliases={3: 1, 4: 2, 5: 3},
        scratch_shapes=[
            pltpu.VMEM((distant * slots, ft), BF16),
            pltpu.VMEM((distant * slots, width), F32),
            pltpu.SMEM((3, local), I32),
            pltpu.SemaphoreType.DMA((RING, 3)),
        ],
        compiler_params=pltpu.CompilerParams(vmem_limit_bytes=12 * 1024 * 1024),
        cost_estimate=pl.CostEstimate(flops=flops, bytes_accessed=3 * 2 * local * width * ft * NF, transcendentals=0),
    )(sizes, rows, y_own, w1p, w3p, w2p, w1, w3, w2)[0]


REMOTE = (2, 4, 6)


def return_kernel(cap, chip_cap, ret, near, tok, goal, hid, w1, w3, w2, out, half, pack, got, acc, late, late_half, mid, yacc, w1b, w3b, w2b, send, recv, half_send, half_recv, wsem):
    me = lax.axis_index('ep')
    slots = near.shape[2]
    steps = LATE * NF

    def weights(t):
        return weight_copies(w1, w3, w2, w1b, w3b, w2b, wsem, t // NF, t % NF, t % LATE_RING)

    tokens, width = hid.shape
    lanes = goal.shape[1] // 2
    barrier = pltpu.get_barrier_semaphore()
    for q in (1, *REMOTE):
        pl.semaphore_signal(barrier, inc=1, device_id=dev(flip(me, q)), device_id_type=MESH)
    pl.semaphore_wait(barrier, 1 + len(REMOTE))
    halves, copies = {}, {}
    for q in (*REMOTE, 0):
        halves[q] = pltpu.make_async_remote_copy(src_ref=ret.at[q + 1, pl.ds(0, cap)], dst_ref=half.at[q // 2], send_sem=half_send.at[q // 2], recv_sem=half_recv.at[q // 2], device_id=dev(flip(me, 1)), device_id_type=MESH)
        halves[q].start()

    for q in REMOTE:
        row = iota((chip_cap, cap), 0).astype(F32)
        mine = (row == goal[q:q + 1, 0:cap]).astype(F32).astype(BF16)
        theirs = (row == goal[q:q + 1, lanes:lanes + cap]).astype(F32).astype(BF16)
        halves[q].wait_recv()
        for c in range(0, width, 512):
            part = jnp.dot(mine, ret[q, 0:cap, c:c + 512], preferred_element_type=F32)
            part = part + jnp.dot(theirs, half[q // 2, :, c:c + 512], preferred_element_type=F32)
            pack[q // 2 - 1, :, c:c + 512] = part.astype(BF16)
        copies[q] = pltpu.make_async_remote_copy(src_ref=pack.at[q // 2 - 1], dst_ref=got.at[q // 2 - 1], send_sem=send.at[q // 2 - 1], recv_sem=recv.at[q // 2 - 1], device_id=dev(flip(me, q)), device_id_type=MESH)
        copies[q].start()

    for t in range(LATE_RING):
        for c in weights(t):
            c.start()
    table = tok[...]

    def chosen(column, peer, at, count):
        lane = iota((tokens, count), 1).astype(F32)
        return jnp.concatenate([((column[k] == peer) & (table[:, at + k:at + k + 1] == lane)).astype(F32) for k in (0, 1)], axis=0).astype(BF16)

    owner = [table[:, 2 + k:3 + k] for k in (0, 1)]
    chip = [jnp.floor(o * 0.5) for o in owner]

    gate = [table[:, k:k + 1] for k in (0, 1)]
    scale = [table[:, 10 + k:11 + k] for k in (0, 1)]

    def add(pick, block, fresh=False, last=False):
        @pl.loop(0, width // 512)
        def _(n):
            cols = pl.ds(pl.multiple_of(n * 512, 512), 512)
            part = jnp.dot(pick, block(cols), preferred_element_type=F32)
            mixed = gate[0] * part[0:tokens] + gate[1] * part[tokens:2 * tokens]
            if not fresh:
                mixed = acc[:, cols] + mixed
            if last:
                out[:, cols] = (scale[0] * hid[:, cols].astype(F32) + scale[1] * mixed).astype(BF16)
            else:
                acc[:, cols] = mixed

    add(chosen(owner, me.astype(F32), 4, cap), lambda c: ret[0, 0:cap, c], fresh=True)
    pick = chosen(owner, flip(me, 1).astype(F32), 4, cap)
    halves[0].wait_recv()
    add(pick, lambda c: half[0, :, c])

    @pl.loop(0, steps)
    def _(t):
        e, f, n = t // NF, t % NF, t % LATE_RING
        for c in weights(t):
            c.wait()
        ffn_part(near[e, :, :, :].reshape(2 * slots, width), w1b, w3b, w2b, n, mid, yacc, f == 0, 2 * slots)

        @pl.when(f == NF - 1)
        def _():
            for q in (0, 1):
                late[q, pl.ds(pl.multiple_of(e * slots, slots), slots), :] = yacc[q * slots:(q + 1) * slots, :].astype(BF16)

        @pl.when(t + LATE_RING < steps)
        def _():
            for c in weights(t + LATE_RING):
                c.start()

    swap = pltpu.make_async_remote_copy(src_ref=late.at[1], dst_ref=late_half, send_sem=half_send.at[4], recv_sem=half_recv.at[4], device_id=dev(flip(me, 1)), device_id_type=MESH)
    swap.start()
    add(chosen(owner, me.astype(F32), 8, LATE * slots), lambda c: late[0, :, c])
    pick = chosen(owner, flip(me, 1).astype(F32), 8, LATE * slots)
    swap.wait_recv()
    add(pick, lambda c: late_half[:, c])
    for q in REMOTE:
        pick = chosen(chip, (flip(me, q) // 2).astype(F32), 6, chip_cap)
        copies[q].wait_recv()
        add(pick, lambda c: got[q // 2 - 1, :, c], last=q == REMOTE[-1])

    for copy in (*halves.values(), *copies.values(), swap):
        copy.wait_send()


def return_call(n, caps, ret, near, tok, goal, hidden, w1, w3, w2):
    owners, _, width = ret.shape
    slots, ft = near.shape[2], w1.shape[2] // NF
    tokens = hidden.shape[0]
    cap, chip_cap = caps
    vmem = pl.BlockSpec(memory_space=pltpu.VMEM)
    return pl.pallas_call(
        functools.partial(return_kernel, cap, chip_cap),
        name=f'return_{cap}_{chip_cap}',
        out_shape=jax.ShapeDtypeStruct((tokens, width), BF16),
        in_specs=[vmem] * 5 + [pl.BlockSpec(memory_space=pl.ANY)] * 3,
        out_specs=vmem,
        scratch_shapes=[
            pltpu.VMEM((owners // 2, cap, width), BF16),
            pltpu.VMEM((len(REMOTE), chip_cap, width), BF16),
            pltpu.VMEM((len(REMOTE), chip_cap, width), BF16),
            pltpu.VMEM((tokens, width), F32),
            pltpu.VMEM((2, LATE * slots, width), BF16),
            pltpu.VMEM((LATE * slots, width), BF16),
            pltpu.VMEM((2 * slots, ft), BF16),
            pltpu.VMEM((2 * slots, width), F32),
            pltpu.VMEM((LATE_RING, width, ft), BF16),
            pltpu.VMEM((LATE_RING, width, ft), BF16),
            pltpu.VMEM((LATE_RING, ft, width), BF16),
            pltpu.SemaphoreType.DMA((len(REMOTE),)),
            pltpu.SemaphoreType.DMA((len(REMOTE),)),
            pltpu.SemaphoreType.DMA((owners // 2 + 1,)),
            pltpu.SemaphoreType.DMA((owners // 2 + 1,)),
            pltpu.SemaphoreType.DMA((LATE_RING, 3)),
        ],
        compiler_params=pltpu.CompilerParams(collective_id=1 + n, has_side_effects=True, vmem_limit_bytes=34 * 1024 * 1024),
    )(ret, near, tok, goal, hidden, w1, w3, w2)


def capacities(local, slots):
    full = [slots * n + 16 * (local - n) for n in range(1, local + 1)]
    chip = [2 * slots + 8 + (slots - 8) * n for n in range(local - 1)]
    return (*zip(full, chip), (local * slots, 2 * local * slots))


def solution(mesh):
    owners = mesh.shape['ep']

    def local_step(hidden, router_w, expert_ids, w_gate, w_up, w_down, post_scale):
        tokens = hidden.shape[0]
        local = w_gate.shape[0]
        slots = tokens // max(1, local * owners // 8)
        caps = capacities(local, slots)
        near, far, y_own, tok, goal, plan, which, w1p, w3p, w2p = gather_call(hidden, expert_ids.T, router_w.T, post_scale, w_gate, w_up, w_down, owners, caps)
        ret = expert_call(plan, far, y_own, w1p, w3p, w2p, w_gate, w_up, w_down, caps)
        branches = [functools.partial(return_call, n, cap) for n, cap in enumerate(caps)]
        return lax.switch(which[0], branches, ret, near, tok, goal, hidden, w_gate, w_up, w_down)

    tok_spec = P(('dp', 'ep'))
    return jax.shard_map(local_step, mesh=mesh, in_specs=(tok_spec, P(), tok_spec, P('ep'), P('ep'), P('ep'), P()), out_specs=tok_spec, check_vma=False)
```

```python
import functools

import jax
import jax.numpy as jnp
from jax import lax
from jax.experimental import pallas as pl
from jax.experimental.pallas import tpu as pltpu
from jax.sharding import PartitionSpec as P

MESH = pl.DeviceIdType.MESH
F32, BF16, I32 = jnp.float32, jnp.bfloat16, jnp.int32
NT = (((1,), (1,)), ((), ()))


def flip(idx, mask):
    out = idx
    for bit in (1, 2, 4):
        if mask & bit:
            out = out + bit - 2 * bit * ((idx // bit) % 2)
    return out


def dev(idx):
    return (lax.axis_index('dp'), idx)


def iota(shape, dim):
    return lax.broadcasted_iota(I32, shape, dim)


def weight_copies(w1, w3, w2, w1b, w3b, w2b, sem, e, f, n):
    ft = w1b.shape[2]
    cols = pl.ds(pl.multiple_of(f * ft, ft), ft)
    return (
        pltpu.make_async_copy(w1.at[e, :, cols], w1b.at[n], sem.at[n, 0]),
        pltpu.make_async_copy(w3.at[e, :, cols], w3b.at[n], sem.at[n, 1]),
        pltpu.make_async_copy(w2.at[e, cols, :], w2b.at[n], sem.at[n, 2]),
    )


def ffn_part(x, w1b, w3b, w2b, n, mid, yacc, fresh, m):
    for c in range(0, w1b.shape[2], 256):
        gate = jnp.dot(x, w1b[n, :, c:c + 256], preferred_element_type=F32)
        up = jnp.dot(x, w3b[n, :, c:c + 256], preferred_element_type=F32)
        mid[0:m, c:c + 256] = (gate * jax.nn.sigmoid(gate) * up).astype(BF16)
    for c in range(0, w2b.shape[2], 512):
        part = jnp.dot(mid[0:m, :], w2b[n, :, c:c + 512], preferred_element_type=F32)
        yacc[0:m, c:c + 512] = jnp.where(fresh, 0.0, yacc[0:m, c:c + 512]) + part


CHUNKS = 4
NF = 3
RING = 4
LATE_RING = 2
BRANCH_LANE = 127
LATE = 2


def gather_kernel(caps, hid_in, ids_in, wrt_in, scale_in, w1, w3, w2, near, far, y_own, tok, goal, plan, which, w1p, w3p, w2p, hid, ids, wrt, scale, pos, mid, yacc, land, ids_all, send, recv, id_send, id_recv, wsem, in_sem):
    me = lax.axis_index('ep')
    own = [pltpu.make_async_copy(src, dst, in_sem.at[n]) for n, (src, dst) in enumerate(((hid_in, hid), (ids_in, ids), (wrt_in, wrt), (scale_in, scale)))]
    for c in own:
        c.start()
    local, _, slots, _ = near.shape
    owners = 2 + far.shape[1]
    steps = (local - LATE) * NF

    def weights(t):
        return weight_copies(w1, w3, w2, w1p, w3p, w2p, wsem, local - 1 - t // NF, t % NF, t % RING)

    tokens, width = hid.shape
    experts = wrt.shape[0]
    rows = tokens // CHUNKS
    barrier = pltpu.get_barrier_semaphore()
    for q in range(1, owners):
        pl.semaphore_signal(barrier, inc=1, device_id=dev(flip(me, q)), device_id_type=MESH)
    pl.semaphore_wait(barrier, owners - 1)
    own[0].wait()
    own[1].wait()

    def piece(q, c):
        return (hid if q == 0 else land.at[q]).at[pl.ds(c * rows, rows)]

    def remote(q, c, n, to):
        return pltpu.make_async_remote_copy(src_ref=piece(q, c), dst_ref=land.at[q ^ to, pl.ds(c * rows, rows)], send_sem=send.at[n], recv_sem=recv.at[n], device_id=dev(flip(me, to)), device_id_type=MESH)

    id_copies = []
    for q in range(1, owners):
        id_copies.append(pltpu.make_async_remote_copy(src_ref=ids, dst_ref=ids_all.at[q], send_sem=id_send.at[q], recv_sem=id_recv.at[q], device_id=dev(flip(me, q)), device_id_type=MESH))
    x_order, y_order = (0, 1, 2, 3), (2, 3, 0, 1)
    to_x = {c: remote(0, c, c, 2) for c in x_order}
    to_y = {c: remote(0, c, 4 + c, 4) for c in y_order}
    for cx, cy in zip(x_order, y_order):
        to_x[cx].start()
        to_y[cy].start()
        if cx == 0:
            for c in id_copies:
                c.start()
    to_mate = pltpu.make_async_remote_copy(src_ref=hid, dst_ref=land.at[1], send_sem=send.at[24], recv_sem=recv.at[24], device_id=dev(flip(me, 1)), device_id_type=MESH)
    to_mate.start()
    for t in range(RING):
        for c in weights(t):
            c.start()

    own[2].wait()
    own[3].wait()
    h = hid[...]
    w = wrt[...]
    w_hi = w.astype(BF16)
    rest = w - w_hi.astype(F32)
    w_mid = rest.astype(BF16)
    w_lo = (rest - w_mid.astype(F32)).astype(BF16)
    dot = functools.partial(lax.dot_general, dimension_numbers=NT, preferred_element_type=F32)
    logits = dot(h, w_hi) + (dot(h, w_mid) + dot(h, w_lo))
    ex = jnp.exp(logits - jnp.max(logits, axis=1, keepdims=True))
    prob = ex / jnp.sum(ex, axis=1, keepdims=True)
    ta, tb = iota((tokens, tokens), 0), iota((tokens, tokens), 1)
    eye = (ta == tb).astype(F32).astype(BF16)
    own_ids = ids[...].astype(F32)
    lane = iota((tokens, experts), 1).astype(F32)
    id_col = [dot(eye, jnp.broadcast_to(own_ids[k:k + 1], (8, tokens)).astype(BF16))[:, 0:1] for k in (0, 1)]
    pick = [(id_col[k] == lane).astype(F32) for k in (0, 1)]
    g = [jnp.sum(pick[k] * prob, axis=1, keepdims=True) for k in (0, 1)]
    total = g[0] + g[1]

    for c in id_copies:
        c.wait_recv()
    ids_all[0] = ids[...]
    counts = []
    for q in range(owners):
        both = ids_all[q]
        e_col = iota((experts, tokens), 0)
        hot = ((both[0:1] == e_col) | (both[1:2] == e_col)).astype(F32).astype(BF16)
        counts.append(dot(jnp.ones((8, tokens), BF16), hot))
    most = functools.reduce(jnp.maximum, counts)
    count = jnp.concatenate([c[0:1] for c in counts], axis=0)
    stride = jnp.where(most > 32.0, float(slots), jnp.where(most > 16.0, 32.0, 16.0))
    mark = lambda mask: mask.astype(F32).astype(BF16)
    plain = functools.partial(jnp.dot, preferred_element_type=F32)
    ea, eb = iota((experts, experts), 0), iota((experts, experts), 1)
    same, same_chip = ea // local == eb // local, ea // (2 * local) == eb // (2 * local)
    offset = plain(stride.astype(BF16), mark(same & (ea < eb)))
    need = jnp.max(plain(stride.astype(BF16), mark(same)), axis=1, keepdims=True)[0:1]
    need_chip = jnp.max(jnp.max(plain(count.astype(BF16), mark(same_chip)), axis=1, keepdims=True), axis=0, keepdims=True)
    branch = jnp.zeros((1, 1), F32)
    for limit, limit_chip in caps[:-1]:
        branch = branch + ((need > limit) | (need_chip > limit_chip)).astype(F32)
    which[...] = branch.astype(I32)
    rank = plain(mark(tb < ta), (pick[0] + pick[1]).astype(BF16))
    chip_first = plain(count.astype(BF16), mark(same_chip & (ea < eb)))[0:1]
    local_of = lane - jnp.floor(lane * (1.0 / local)) * local
    late_place = jnp.where(local_of < LATE, local_of * slots + rank, -1.0)
    late = [jnp.sum(pick[k] * late_place, axis=1, keepdims=True) for k in (0, 1)]
    slot = [jnp.sum(pick[k] * (rank + offset[0:1]), axis=1, keepdims=True) for k in (0, 1)]
    packed = [jnp.sum(pick[k] * (rank + chip_first), axis=1, keepdims=True) for k in (0, 1)]
    owner = [jnp.floor(id_col[k] * (1.0 / local)) for k in (0, 1)]
    wide = iota((tokens, 128), 1)
    table = jnp.zeros((tokens, 128), F32)
    for n, col in enumerate((g[0] / total, g[1] / total, *owner, *slot, *packed, *late, scale[0], scale[1])):
        table = jnp.where(wide == n, col, table)
    tok[...] = table

    e_row, n_col = iota((experts, 128), 0), iota((experts, 128), 1)
    e_of = jnp.where(n_col < local, me * local + n_col, flip(me, 1) * local + n_col - local)
    used = n_col < 2 * local
    held = plain(count.astype(BF16), mark(used & (e_row == e_of)))
    start = plain(count.astype(BF16), mark(used & (e_row // (2 * local) == me // 2) & (e_row < e_of)))
    base = plain(stride.astype(BF16), mark(used & (e_row // local == e_of // local) & (e_row < e_of)))
    base_size = plain(stride.astype(BF16), mark(used & (e_row == e_of)))
    lane_of = iota((owners, goal.shape[1]), 1)
    where_to = jnp.full((owners, goal.shape[1]), -1.0, F32)
    for n in range(2 * local):
        at = (lane_of - (n // local) * (goal.shape[1] // 2)).astype(F32) - base[0:1, n:n + 1]
        where_to = jnp.where((at >= 0.0) & (at < held[:, n:n + 1]), at + start[:, n:n + 1], where_to)
    goal[...] = where_to

    first, second = (jnp.concatenate([ids_all[q, k:k + 1] for q in range(owners)], axis=0) for k in (0, 1))
    marks = jnp.concatenate([((first == me * local + j) | (second == me * local + j)).astype(F32) for j in range(local)], axis=0)
    earlier = plain(marks.astype(BF16), (ta < tb).astype(F32).astype(BF16))
    pos[...] = jnp.where(marks > 0.5, earlier, -1.0)
    plan[...] = jnp.where(n_col[0:8] == BRANCH_LANE, branch, base_size).astype(I32)

    def pick_rows(q):
        at = iota((slots, tokens), 0).astype(F32)
        match = jnp.concatenate([(at == pos[j * owners + q:j * owners + q + 1, :]).astype(F32) for j in range(local)], axis=0).astype(BF16)

        def columns(cols):
            block = hid[:, cols] if q == 0 else land[q, :, cols]
            part = jnp.dot(match, block, preferred_element_type=F32).astype(BF16)
            for j in range(local):
                to = near.at[j, q] if q < 2 else far.at[j, q - 2]
                to[:, cols] = part[j * slots:(j + 1) * slots]

        if q < 6:
            @pl.loop(0, width // 512)
            def _(n):
                columns(pl.ds(pl.multiple_of(n * 512, 512), 512))
        else:
            for c in range(0, width, 512):
                columns(pl.ds(c, 512))

    def own_steps(first, last):
        @pl.loop(first, last)
        def _(t):
            e, f, n = local - 1 - t // NF, t % NF, t % RING
            for c in weights(t):
                c.wait()
            x = near[e, :, :, :].reshape(2 * slots, width)
            ffn_part(x, w1p, w3p, w2p, n, mid, yacc, f == 0, 2 * slots)

            @pl.when(f == NF - 1)
            def _():
                for q in (0, 1):
                    y_own[e - LATE, q, :, :] = yacc[q * slots:(q + 1) * slots, :].astype(BF16)

            @pl.when(t + RING < steps)
            def _():
                for c in weights(t + RING):
                    c.start()

    sent = [*to_x.values(), *to_y.values(), to_mate]

    def pass_on(q, c, n, to):
        copy = remote(q, c, n, to)
        copy.start()
        sent.append(copy)
        return copy

    pick_rows(0)
    to_mate.wait_recv()
    pick_rows(1)
    across, mates = {}, {2: [], 4: [], 6: []}
    for n, (cx, cy) in enumerate(zip(x_order, y_order)):
        if n < 2:
            own_steps(n * steps // 2, (n + 1) * steps // 2)
        to_x[cx].wait_recv()
        if cx in (0, 1):
            across[cx] = pass_on(2, cx, 8 + cx, 4)
        mates[2].append(pass_on(2, cx, 12 + cx, 1))
        to_y[cy].wait_recv()
        if cy in (2, 3):
            across[cy] = pass_on(4, cy, 8 + cy, 2)
        mates[4].append(pass_on(4, cy, 16 + cy, 1))
    for q in (2, 4):
        pick_rows(q)
    for q in (2, 4):
        for m in mates[q]:
            m.wait_recv()
        pick_rows(q + 1)
    for c in (0, 2, 1, 3):
        across[c].wait_recv()
        mates[6].append(pass_on(6, c, 20 + c, 1))
    pick_rows(6)
    for m in mates[6]:
        m.wait_recv()
    pick_rows(7)
    for m in sent:
        m.wait_send()
    for c in id_copies:
        c.wait_send()


def gather_call(hidden, ids_t, wr_t, scale, w1, w3, w2, owners, caps):
    tokens, width = hidden.shape
    experts = wr_t.shape[0]
    local, _, ffn = w1.shape
    slots = caps[-1][0] // local
    ft = ffn // NF
    vmem = pl.BlockSpec(memory_space=pltpu.VMEM)
    hbm = pl.BlockSpec(memory_space=pl.ANY)
    return pl.pallas_call(
        functools.partial(gather_kernel, caps),
        name='gather_tokens',
        out_shape=(
            pltpu.VMEM((local, 2, slots, width), BF16),
            pltpu.VMEM((local, owners - 2, slots, width), BF16),
            pltpu.VMEM((local - LATE, 2, slots, width), BF16),
            jax.ShapeDtypeStruct((tokens, 128), F32),
            jax.ShapeDtypeStruct((owners, 2 * local * slots), F32),
            jax.ShapeDtypeStruct((8, 128), I32),
            jax.ShapeDtypeStruct((1, 1), I32),
            pltpu.VMEM((RING, width, ft), BF16),
            pltpu.VMEM((RING, width, ft), BF16),
            pltpu.VMEM((RING, ft, width), BF16),
        ),
        in_specs=[hbm, *[pl.BlockSpec(memory_space=pltpu.HBM)] * 3, hbm, hbm, hbm],
        out_specs=(vmem,) * 10,
        scratch_shapes=[
            pltpu.VMEM((tokens, width), BF16),
            pltpu.VMEM((2, tokens), I32),
            pltpu.VMEM((experts, width), F32),
            pltpu.SMEM((2,), F32),
            pltpu.VMEM((local * owners, tokens), F32),
            pltpu.VMEM((2 * slots, ft), BF16),
            pltpu.VMEM((2 * slots, width), F32),
            pltpu.VMEM((owners, tokens, width), BF16),
            pltpu.VMEM((owners, 2, tokens), I32),
            pltpu.SemaphoreType.DMA((25,)),
            pltpu.SemaphoreType.DMA((25,)),
            pltpu.SemaphoreType.DMA((owners,)),
            pltpu.SemaphoreType.DMA((owners,)),
            pltpu.SemaphoreType.DMA((RING, 3)),
            pltpu.SemaphoreType.DMA((4,)),
        ],
        compiler_params=pltpu.CompilerParams(collective_id=0, has_side_effects=True, vmem_limit_bytes=13 * 1024 * 1024),
    )(hidden, *(pltpu.with_memory_space_constraint(x, pltpu.HBM) for x in (ids_t, wr_t, scale)), w1, w3, w2)


def expert_kernel(caps, info, rows, y_own, _w1b, _w3b, _w2b, w1, w3, w2, ret, w1b, w3b, w2b, mid, yacc, plan, wsem):
    local, distant, slots, width = rows.shape
    owners = distant + 2
    steps = local * NF
    done = (local - LATE) * NF

    size = [info[0, j] for j in range(local)]
    branch = info[0, BRANCH_LANE]
    for j in range(local):
        rank = jnp.int32(j - LATE if j >= LATE else local - LATE)
        offset = jnp.int32(0)
        for i in range(local):
            if i < LATE and j < LATE and i != j:
                ahead = (size[i] >= size[j]) if i < j else (size[i] > size[j])
                rank = rank + ahead.astype(I32)
            if i < j:
                offset = offset + size[i]
        plan[0, rank] = jnp.int32(j)
        plan[1, rank] = size[j]
        plan[2, rank] = offset
    used = size[0]
    for j in range(1, local):
        used = used + size[j]

    def part_of(t):
        turn = jnp.where(t < NF, 0, 2 * NF - RING)
        return (t % NF + turn) % NF

    def weights(t):
        return weight_copies(w1, w3, w2, w1b, w3b, w2b, wsem, plan[0, t // NF], part_of(t), (t + done - NF) % RING)

    limit = jnp.int32(caps[0][0])
    for n in range(1, len(caps)):
        limit = jnp.where(branch >= n, caps[n][0], limit)

    @pl.loop(used // 16, limit // 16)
    def _(n):
        blank = pl.ds(pl.multiple_of(n * 16, 16), 16)
        for q in range(owners):
            ret[q, blank, :] = jnp.zeros((16, width), BF16)

    @pl.loop(0, steps)
    def _(t):
        r, f, n = t // NF, t % NF, (t + done - NF) % RING
        e = plan[0, r]

        @pl.when(t >= RING)
        def _():
            for c in weights(t):
                c.wait()

        for size in (16, 32, slots):
            m = size * distant

            @pl.when(plan[1, r] == size)
            def _():
                x = rows[e, :, 0:size, :].reshape(m, width)
                ffn_part(x, w1b, w3b, w2b, n, mid, yacc, f == 0, m)

                @pl.when(f == NF - 1)
                def _():
                    first = pl.multiple_of(plan[2, r], 16)
                    for q in (0, 1):
                        mine = y_own[jnp.maximum(e - LATE, 0), q, 0:size, :]
                        ret[q, pl.ds(first, size), :] = jnp.where(e >= LATE, mine, jnp.zeros_like(mine))
                    for q in range(2, owners):
                        ret[q, pl.ds(first, size), :] = yacc[(q - 2) * size:(q - 1) * size, :].astype(BF16)

        @pl.when(t + RING < steps)
        def _():
            for c in weights(t + RING):
                c.start()


def expert_call(sizes, rows, y_own, w1p, w3p, w2p, w1, w3, w2, caps):
    local, distant, slots, width = rows.shape
    owners = distant + 2
    ft = w1p.shape[2]
    hbm = pl.BlockSpec(memory_space=pl.ANY)
    vmem = pl.BlockSpec(memory_space=pltpu.VMEM)
    flops = 3 * 2 * local * slots * owners * width * ft * NF // 2
    return pl.pallas_call(
        functools.partial(expert_kernel, caps),
        name='experts',
        out_shape=(
            pltpu.VMEM((owners, caps[-1][0], width), BF16),
            pltpu.VMEM(w1p.shape, BF16),
            pltpu.VMEM(w3p.shape, BF16),
            pltpu.VMEM(w2p.shape, BF16),
        ),
        in_specs=[vmem] * 6 + [hbm] * 3,
        out_specs=(vmem, vmem, vmem, vmem),
        input_output_aliases={3: 1, 4: 2, 5: 3},
        scratch_shapes=[
            pltpu.VMEM((distant * slots, ft), BF16),
            pltpu.VMEM((distant * slots, width), F32),
            pltpu.SMEM((3, local), I32),
            pltpu.SemaphoreType.DMA((RING, 3)),
        ],
        compiler_params=pltpu.CompilerParams(vmem_limit_bytes=12 * 1024 * 1024),
        cost_estimate=pl.CostEstimate(flops=flops, bytes_accessed=3 * 2 * local * width * ft * NF, transcendentals=0),
    )(sizes, rows, y_own, w1p, w3p, w2p, w1, w3, w2)[0]


REMOTE = (2, 4, 6)


def return_kernel(cap, chip_cap, ret, near, tok, goal, hid, w1, w3, w2, out, half, pack, got, acc, late, late_half, mid, yacc, w1b, w3b, w2b, send, recv, half_send, half_recv, wsem):
    me = lax.axis_index('ep')
    slots = near.shape[2]
    steps = LATE * NF

    def weights(t):
        return weight_copies(w1, w3, w2, w1b, w3b, w2b, wsem, t // NF, t % NF, t % LATE_RING)

    tokens, width = hid.shape
    lanes = goal.shape[1] // 2
    barrier = pltpu.get_barrier_semaphore()
    for q in (1, *REMOTE):
        pl.semaphore_signal(barrier, inc=1, device_id=dev(flip(me, q)), device_id_type=MESH)
    pl.semaphore_wait(barrier, 1 + len(REMOTE))
    halves, copies = {}, {}
    for q in (*REMOTE, 0):
        halves[q] = pltpu.make_async_remote_copy(src_ref=ret.at[q + 1, pl.ds(0, cap)], dst_ref=half.at[q // 2], send_sem=half_send.at[q // 2], recv_sem=half_recv.at[q // 2], device_id=dev(flip(me, 1)), device_id_type=MESH)
        halves[q].start()

    for q in REMOTE:
        row = iota((chip_cap, cap), 0).astype(F32)
        mine = (row == goal[q:q + 1, 0:cap]).astype(F32).astype(BF16)
        theirs = (row == goal[q:q + 1, lanes:lanes + cap]).astype(F32).astype(BF16)
        halves[q].wait_recv()
        for c in range(0, width, 512):
            part = jnp.dot(mine, ret[q, 0:cap, c:c + 512], preferred_element_type=F32)
            part = part + jnp.dot(theirs, half[q // 2, :, c:c + 512], preferred_element_type=F32)
            pack[q // 2 - 1, :, c:c + 512] = part.astype(BF16)
        copies[q] = pltpu.make_async_remote_copy(src_ref=pack.at[q // 2 - 1], dst_ref=got.at[q // 2 - 1], send_sem=send.at[q // 2 - 1], recv_sem=recv.at[q // 2 - 1], device_id=dev(flip(me, q)), device_id_type=MESH)
        copies[q].start()

    for t in range(LATE_RING):
        for c in weights(t):
            c.start()
    table = tok[...]

    def chosen(column, peer, at, count):
        lane = iota((tokens, count), 1).astype(F32)
        return jnp.concatenate([((column[k] == peer) & (table[:, at + k:at + k + 1] == lane)).astype(F32) for k in (0, 1)], axis=0).astype(BF16)

    owner = [table[:, 2 + k:3 + k] for k in (0, 1)]
    chip = [jnp.floor(o * 0.5) for o in owner]

    gate = [table[:, k:k + 1] for k in (0, 1)]
    scale = [table[:, 10 + k:11 + k] for k in (0, 1)]

    def add(pick, block, fresh=False, last=False):
        @pl.loop(0, width // 512)
        def _(n):
            cols = pl.ds(pl.multiple_of(n * 512, 512), 512)
            part = jnp.dot(pick, block(cols), preferred_element_type=F32)
            mixed = gate[0] * part[0:tokens] + gate[1] * part[tokens:2 * tokens]
            if not fresh:
                mixed = acc[:, cols] + mixed
            if last:
                out[:, cols] = (scale[0] * hid[:, cols].astype(F32) + scale[1] * mixed).astype(BF16)
            else:
                acc[:, cols] = mixed

    add(chosen(owner, me.astype(F32), 4, cap), lambda c: ret[0, 0:cap, c], fresh=True)
    pick = chosen(owner, flip(me, 1).astype(F32), 4, cap)
    halves[0].wait_recv()
    add(pick, lambda c: half[0, :, c])

    @pl.loop(0, steps)
    def _(t):
        e, f, n = t // NF, t % NF, t % LATE_RING
        for c in weights(t):
            c.wait()
        ffn_part(near[e, :, :, :].reshape(2 * slots, width), w1b, w3b, w2b, n, mid, yacc, f == 0, 2 * slots)

        @pl.when(f == NF - 1)
        def _():
            for q in (0, 1):
                late[q, pl.ds(pl.multiple_of(e * slots, slots), slots), :] = yacc[q * slots:(q + 1) * slots, :].astype(BF16)

        @pl.when(t + LATE_RING < steps)
        def _():
            for c in weights(t + LATE_RING):
                c.start()

    swap = pltpu.make_async_remote_copy(src_ref=late.at[1], dst_ref=late_half, send_sem=half_send.at[4], recv_sem=half_recv.at[4], device_id=dev(flip(me, 1)), device_id_type=MESH)
    swap.start()
    add(chosen(owner, me.astype(F32), 8, LATE * slots), lambda c: late[0, :, c])
    pick = chosen(owner, flip(me, 1).astype(F32), 8, LATE * slots)
    swap.wait_recv()
    add(pick, lambda c: late_half[:, c])
    for q in REMOTE:
        pick = chosen(chip, (flip(me, q) // 2).astype(F32), 6, chip_cap)
        copies[q].wait_recv()
        add(pick, lambda c: got[q // 2 - 1, :, c], last=q == REMOTE[-1])

    for copy in (*halves.values(), *copies.values(), swap):
        copy.wait_send()


def return_call(n, caps, ret, near, tok, goal, hidden, w1, w3, w2):
    owners, _, width = ret.shape
    slots, ft = near.shape[2], w1.shape[2] // NF
    tokens = hidden.shape[0]
    cap, chip_cap = caps
    vmem = pl.BlockSpec(memory_space=pltpu.VMEM)
    return pl.pallas_call(
        functools.partial(return_kernel, cap, chip_cap),
        name=f'return_{cap}_{chip_cap}',
        out_shape=jax.ShapeDtypeStruct((tokens, width), BF16),
        in_specs=[vmem] * 5 + [pl.BlockSpec(memory_space=pl.ANY)] * 3,
        out_specs=vmem,
        scratch_shapes=[
            pltpu.VMEM((owners // 2, cap, width), BF16),
            pltpu.VMEM((len(REMOTE), chip_cap, width), BF16),
            pltpu.VMEM((len(REMOTE), chip_cap, width), BF16),
            pltpu.VMEM((tokens, width), F32),
            pltpu.VMEM((2, LATE * slots, width), BF16),
            pltpu.VMEM((LATE * slots, width), BF16),
            pltpu.VMEM((2 * slots, ft), BF16),
            pltpu.VMEM((2 * slots, width), F32),
            pltpu.VMEM((LATE_RING, width, ft), BF16),
            pltpu.VMEM((LATE_RING, width, ft), BF16),
            pltpu.VMEM((LATE_RING, ft, width), BF16),
            pltpu.SemaphoreType.DMA((len(REMOTE),)),
            pltpu.SemaphoreType.DMA((len(REMOTE),)),
            pltpu.SemaphoreType.DMA((owners // 2 + 1,)),
            pltpu.SemaphoreType.DMA((owners // 2 + 1,)),
            pltpu.SemaphoreType.DMA((LATE_RING, 3)),
        ],
        compiler_params=pltpu.CompilerParams(collective_id=1 + n, has_side_effects=True, vmem_limit_bytes=34 * 1024 * 1024),
    )(ret, near, tok, goal, hidden, w1, w3, w2)


def capacities(local, slots):
    full = [slots * n + 16 * (local - n) for n in range(1, local + 1)]
    chip = [2 * slots + 8 + (slots - 8) * n for n in range(local - 1)]
    return (*zip(full, chip), (local * slots, 2 * local * slots))


def solution(mesh):
    owners = mesh.shape['ep']

    def local_step(hidden, router_w, expert_ids, w_gate, w_up, w_down, post_scale):
        tokens = hidden.shape[0]
        local = w_gate.shape[0]
        slots = tokens // max(1, local * owners // 8)
        caps = capacities(local, slots)
        near, far, y_own, tok, goal, plan, which, w1p, w3p, w2p = gather_call(hidden, expert_ids.T, router_w.T, post_scale, w_gate, w_up, w_down, owners, caps)
        ret = expert_call(plan, far, y_own, w1p, w3p, w2p, w_gate, w_up, w_down, caps)
        branches = [functools.partial(return_call, n, cap) for n, cap in enumerate(caps)]
        return lax.switch(which.reshape(()), branches, ret, near, tok, goal, hidden, w_gate, w_up, w_down)

    tok_spec = P(('dp', 'ep'))
    return jax.shard_map(local_step, mesh=mesh, in_specs=(tok_spec, P(), tok_spec, P('ep'), P('ep'), P('ep'), P()), out_specs=tok_spec, check_vma=False)
```

```python
import functools

import jax
import jax.numpy as jnp
from jax import lax
from jax.experimental import pallas as pl
from jax.experimental.pallas import tpu as pltpu
from jax.sharding import PartitionSpec as P

MESH = pl.DeviceIdType.MESH
F32, BF16, I32 = jnp.float32, jnp.bfloat16, jnp.int32
NT = (((1,), (1,)), ((), ()))


def flip(idx, mask):
    out = idx
    for bit in (1, 2, 4):
        if mask & bit:
            out = out + bit - 2 * bit * ((idx // bit) % 2)
    return out


def dev(idx):
    return (lax.axis_index('dp'), idx)


def iota(shape, dim):
    return lax.broadcasted_iota(I32, shape, dim)


def weight_copies(w1, w3, w2, w1b, w3b, w2b, sem, e, f, n):
    ft = w1b.shape[2]
    cols = pl.ds(pl.multiple_of(f * ft, ft), ft)
    return (
        pltpu.make_async_copy(w1.at[e, :, cols], w1b.at[n], sem.at[n, 0]),
        pltpu.make_async_copy(w3.at[e, :, cols], w3b.at[n], sem.at[n, 1]),
        pltpu.make_async_copy(w2.at[e, cols, :], w2b.at[n], sem.at[n, 2]),
    )


def ffn_part(x, w1b, w3b, w2b, n, mid, yacc, fresh, m):
    for c in range(0, w1b.shape[2], 256):
        gate = jnp.dot(x, w1b[n, :, c:c + 256], preferred_element_type=F32)
        up = jnp.dot(x, w3b[n, :, c:c + 256], preferred_element_type=F32)
        mid[0:m, c:c + 256] = (gate * jax.nn.sigmoid(gate) * up).astype(BF16)
    for c in range(0, w2b.shape[2], 512):
        part = jnp.dot(mid[0:m, :], w2b[n, :, c:c + 512], preferred_element_type=F32)
        yacc[0:m, c:c + 512] = jnp.where(fresh, 0.0, yacc[0:m, c:c + 512]) + part


CHUNKS = 4
NF = 3
RING = 4
LATE_RING = 2
BRANCH_LANE = 127
LATE = 2


def gather_kernel(caps, hid_in, ids_in, wrt_in, scale_in, w1, w3, w2, near, far, y_own, tok, goal, plan, which, w1p, w3p, w2p, hid, ids, wrt, scale, pos, mid, yacc, land, ids_all, send, recv, id_send, id_recv, wsem, in_sem):
    me = lax.axis_index('ep')
    own = [pltpu.make_async_copy(src, dst, in_sem.at[n]) for n, (src, dst) in enumerate(((hid_in, hid), (ids_in, ids), (wrt_in, wrt), (scale_in, scale)))]
    for c in own:
        c.start()
    local, _, slots, _ = near.shape
    owners = 2 + far.shape[1]
    steps = (local - LATE) * NF

    def weights(t):
        return weight_copies(w1, w3, w2, w1p, w3p, w2p, wsem, local - 1 - t // NF, t % NF, t % RING)

    tokens, width = hid.shape
    experts = wrt.shape[0]
    rows = tokens // CHUNKS
    barrier = pltpu.get_barrier_semaphore()
    for q in range(1, owners):
        pl.semaphore_signal(barrier, inc=1, device_id=dev(flip(me, q)), device_id_type=MESH)
    pl.semaphore_wait(barrier, owners - 1)
    own[0].wait()
    own[1].wait()

    def piece(q, c):
        return (hid if q == 0 else land.at[q]).at[pl.ds(c * rows, rows)]

    def remote(q, c, n, to):
        return pltpu.make_async_remote_copy(src_ref=piece(q, c), dst_ref=land.at[q ^ to, pl.ds(c * rows, rows)], send_sem=send.at[n], recv_sem=recv.at[n], device_id=dev(flip(me, to)), device_id_type=MESH)

    id_copies = []
    for q in range(1, owners):
        id_copies.append(pltpu.make_async_remote_copy(src_ref=ids, dst_ref=ids_all.at[q], send_sem=id_send.at[q], recv_sem=id_recv.at[q], device_id=dev(flip(me, q)), device_id_type=MESH))
    for c in id_copies:
        c.start()
    x_order, y_order = (0, 1, 2, 3), (2, 3, 0, 1)
    to_x = {c: remote(0, c, c, 2) for c in x_order}
    to_y = {c: remote(0, c, 4 + c, 4) for c in y_order}
    for cx, cy in zip(x_order, y_order):
        to_x[cx].start()
        to_y[cy].start()
    to_mate = pltpu.make_async_remote_copy(src_ref=hid, dst_ref=land.at[1], send_sem=send.at[24], recv_sem=recv.at[24], device_id=dev(flip(me, 1)), device_id_type=MESH)
    to_mate.start()
    for t in range(RING):
        for c in weights(t):
            c.start()

    own[2].wait()
    own[3].wait()
    h = hid[...]
    w = wrt[...]
    w_hi = w.astype(BF16)
    rest = w - w_hi.astype(F32)
    w_mid = rest.astype(BF16)
    w_lo = (rest - w_mid.astype(F32)).astype(BF16)
    dot = functools.partial(lax.dot_general, dimension_numbers=NT, preferred_element_type=F32)
    logits = dot(h, w_hi) + (dot(h, w_mid) + dot(h, w_lo))
    ex = jnp.exp(logits - jnp.max(logits, axis=1, keepdims=True))
    prob = ex / jnp.sum(ex, axis=1, keepdims=True)
    ta, tb = iota((tokens, tokens), 0), iota((tokens, tokens), 1)
    eye = (ta == tb).astype(F32).astype(BF16)
    own_ids = ids[...].astype(F32)
    lane = iota((tokens, experts), 1).astype(F32)
    id_col = [dot(eye, jnp.broadcast_to(own_ids[k:k + 1], (8, tokens)).astype(BF16))[:, 0:1] for k in (0, 1)]
    pick = [(id_col[k] == lane).astype(F32) for k in (0, 1)]
    g = [jnp.sum(pick[k] * prob, axis=1, keepdims=True) for k in (0, 1)]
    total = g[0] + g[1]

    for c in id_copies:
        c.wait_recv()
    ids_all[0] = ids[...]
    counts = []
    for q in range(owners):
        both = ids_all[q]
        e_col = iota((experts, tokens), 0)
        hot = ((both[0:1] == e_col) | (both[1:2] == e_col)).astype(F32).astype(BF16)
        counts.append(dot(jnp.ones((8, tokens), BF16), hot))
    most = functools.reduce(jnp.maximum, counts)
    count = jnp.concatenate([c[0:1] for c in counts], axis=0)
    stride = jnp.where(most > 32.0, float(slots), jnp.where(most > 16.0, 32.0, 16.0))
    mark = lambda mask: mask.astype(F32).astype(BF16)
    plain = functools.partial(jnp.dot, preferred_element_type=F32)
    ea, eb = iota((experts, experts), 0), iota((experts, experts), 1)
    same, same_chip = ea // local == eb // local, ea // (2 * local) == eb // (2 * local)
    offset = plain(stride.astype(BF16), mark(same & (ea < eb)))
    need = jnp.max(plain(stride.astype(BF16), mark(same)), axis=1, keepdims=True)[0:1]
    need_chip = jnp.max(jnp.max(plain(count.astype(BF16), mark(same_chip)), axis=1, keepdims=True), axis=0, keepdims=True)
    branch = jnp.zeros((1, 1), F32)
    for limit, limit_chip in caps[:-1]:
        branch = branch + ((need > limit) | (need_chip > limit_chip)).astype(F32)
    which[...] = branch.astype(I32)
    rank = plain(mark(tb < ta), (pick[0] + pick[1]).astype(BF16))
    chip_first = plain(count.astype(BF16), mark(same_chip & (ea < eb)))[0:1]
    local_of = lane - jnp.floor(lane * (1.0 / local)) * local
    late_place = jnp.where(local_of < LATE, local_of * slots + rank, -1.0)
    late = [jnp.sum(pick[k] * late_place, axis=1, keepdims=True) for k in (0, 1)]
    slot = [jnp.sum(pick[k] * (rank + offset[0:1]), axis=1, keepdims=True) for k in (0, 1)]
    packed = [jnp.sum(pick[k] * (rank + chip_first), axis=1, keepdims=True) for k in (0, 1)]
    owner = [jnp.floor(id_col[k] * (1.0 / local)) for k in (0, 1)]
    wide = iota((tokens, 128), 1)
    table = jnp.zeros((tokens, 128), F32)
    for n, col in enumerate((g[0] / total, g[1] / total, *owner, *slot, *packed, *late, scale[0], scale[1])):
        table = jnp.where(wide == n, col, table)
    tok[...] = table

    e_row, n_col = iota((experts, 128), 0), iota((experts, 128), 1)
    e_of = jnp.where(n_col < local, me * local + n_col, flip(me, 1) * local + n_col - local)
    used = n_col < 2 * local
    held = plain(count.astype(BF16), mark(used & (e_row == e_of)))
    start = plain(count.astype(BF16), mark(used & (e_row // (2 * local) == me // 2) & (e_row < e_of)))
    base = plain(stride.astype(BF16), mark(used & (e_row // local == e_of // local) & (e_row < e_of)))
    base_size = plain(stride.astype(BF16), mark(used & (e_row == e_of)))
    lane_of = iota((owners, goal.shape[1]), 1)
    where_to = jnp.full((owners, goal.shape[1]), -1.0, F32)
    for n in range(2 * local):
        at = (lane_of - (n // local) * (goal.shape[1] // 2)).astype(F32) - base[0:1, n:n + 1]
        where_to = jnp.where((at >= 0.0) & (at < held[:, n:n + 1]), at + start[:, n:n + 1], where_to)
    goal[...] = where_to

    first, second = (jnp.concatenate([ids_all[q, k:k + 1] for q in range(owners)], axis=0) for k in (0, 1))
    marks = jnp.concatenate([((first == me * local + j) | (second == me * local + j)).astype(F32) for j in range(local)], axis=0)
    earlier = plain(marks.astype(BF16), (ta < tb).astype(F32).astype(BF16))
    pos[...] = jnp.where(marks > 0.5, earlier, -1.0)
    plan[...] = jnp.where(n_col[0:8] == BRANCH_LANE, branch, base_size).astype(I32)

    def pick_rows(q):
        at = iota((slots, tokens), 0).astype(F32)
        match = jnp.concatenate([(at == pos[j * owners + q:j * owners + q + 1, :]).astype(F32) for j in range(local)], axis=0).astype(BF16)

        def columns(cols):
            block = hid[:, cols] if q == 0 else land[q, :, cols]
            part = jnp.dot(match, block, preferred_element_type=F32).astype(BF16)
            for j in range(local):
                to = near.at[j, q] if q < 2 else far.at[j, q - 2]
                to[:, cols] = part[j * slots:(j + 1) * slots]

        if q < 6:
            @pl.loop(0, width // 512)
            def _(n):
                columns(pl.ds(pl.multiple_of(n * 512, 512), 512))
        else:
            for c in range(0, width, 512):
                columns(pl.ds(c, 512))

    def own_steps(first, last):
        @pl.loop(first, last)
        def _(t):
            e, f, n = local - 1 - t // NF, t % NF, t % RING
            for c in weights(t):
                c.wait()
            x = near[e, :, :, :].reshape(2 * slots, width)
            ffn_part(x, w1p, w3p, w2p, n, mid, yacc, f == 0, 2 * slots)

            @pl.when(f == NF - 1)
            def _():
                for q in (0, 1):
                    y_own[e - LATE, q, :, :] = yacc[q * slots:(q + 1) * slots, :].astype(BF16)

            @pl.when(t + RING < steps)
            def _():
                for c in weights(t + RING):
                    c.start()

    sent = [*to_x.values(), *to_y.values(), to_mate]

    def pass_on(q, c, n, to):
        copy = remote(q, c, n, to)
        copy.start()
        sent.append(copy)
        return copy

    pick_rows(0)
    to_mate.wait_recv()
    pick_rows(1)
    across, mates = {}, {2: [], 4: [], 6: []}
    for n, (cx, cy) in enumerate(zip(x_order, y_order)):
        if n < 2:
            own_steps(n * steps // 2, (n + 1) * steps // 2)
        to_x[cx].wait_recv()
        if cx in (0, 1):
            across[cx] = pass_on(2, cx, 8 + cx, 4)
        mates[2].append(pass_on(2, cx, 12 + cx, 1))
        to_y[cy].wait_recv()
        if cy in (2, 3):
            across[cy] = pass_on(4, cy, 8 + cy, 2)
        mates[4].append(pass_on(4, cy, 16 + cy, 1))
    for q in (2, 4):
        pick_rows(q)
    for q in (2, 4):
        for m in mates[q]:
            m.wait_recv()
        pick_rows(q + 1)
    for c in (0, 2, 1, 3):
        across[c].wait_recv()
        mates[6].append(pass_on(6, c, 20 + c, 1))
    pick_rows(6)
    for m in mates[6]:
        m.wait_recv()
    pick_rows(7)
    for m in sent:
        m.wait_send()
    for c in id_copies:
        c.wait_send()


def gather_call(hidden, ids_t, wr_t, scale, w1, w3, w2, owners, caps):
    tokens, width = hidden.shape
    experts = wr_t.shape[0]
    local, _, ffn = w1.shape
    slots = caps[-1][0] // local
    ft = ffn // NF
    vmem = pl.BlockSpec(memory_space=pltpu.VMEM)
    hbm = pl.BlockSpec(memory_space=pl.ANY)
    return pl.pallas_call(
        functools.partial(gather_kernel, caps),
        name='gather_tokens',
        out_shape=(
            pltpu.VMEM((local, 2, slots, width), BF16),
            pltpu.VMEM((local, owners - 2, slots, width), BF16),
            pltpu.VMEM((local - LATE, 2, slots, width), BF16),
            jax.ShapeDtypeStruct((tokens, 128), F32),
            jax.ShapeDtypeStruct((owners, 2 * local * slots), F32),
            jax.ShapeDtypeStruct((8, 128), I32),
            jax.ShapeDtypeStruct((1, 1), I32),
            pltpu.VMEM((RING, width, ft), BF16),
            pltpu.VMEM((RING, width, ft), BF16),
            pltpu.VMEM((RING, ft, width), BF16),
        ),
        in_specs=[hbm, *[pl.BlockSpec(memory_space=pltpu.HBM)] * 3, hbm, hbm, hbm],
        out_specs=(vmem,) * 10,
        scratch_shapes=[
            pltpu.VMEM((tokens, width), BF16),
            pltpu.VMEM((2, tokens), I32),
            pltpu.VMEM((experts, width), F32),
            pltpu.SMEM((2,), F32),
            pltpu.VMEM((local * owners, tokens), F32),
            pltpu.VMEM((2 * slots, ft), BF16),
            pltpu.VMEM((2 * slots, width), F32),
            pltpu.VMEM((owners, tokens, width), BF16),
            pltpu.VMEM((owners, 2, tokens), I32),
            pltpu.SemaphoreType.DMA((25,)),
            pltpu.SemaphoreType.DMA((25,)),
            pltpu.SemaphoreType.DMA((owners,)),
            pltpu.SemaphoreType.DMA((owners,)),
            pltpu.SemaphoreType.DMA((RING, 3)),
            pltpu.SemaphoreType.DMA((4,)),
        ],
        compiler_params=pltpu.CompilerParams(collective_id=0, has_side_effects=True, vmem_limit_bytes=13 * 1024 * 1024),
    )(hidden, *(pltpu.with_memory_space_constraint(x, pltpu.HBM) for x in (ids_t, wr_t, scale)), w1, w3, w2)


def expert_kernel(caps, info, rows, y_own, _w1b, _w3b, _w2b, w1, w3, w2, ret, w1b, w3b, w2b, mid, yacc, plan, wsem):
    local, distant, slots, width = rows.shape
    owners = distant + 2
    steps = local * NF
    done = (local - LATE) * NF

    size = [info[0, j] for j in range(local)]
    branch = info[0, BRANCH_LANE]
    for j in range(local):
        rank = jnp.int32(j - LATE if j >= LATE else local - LATE)
        offset = jnp.int32(0)
        for i in range(local):
            if i < LATE and j < LATE and i != j:
                ahead = (size[i] >= size[j]) if i < j else (size[i] > size[j])
                rank = rank + ahead.astype(I32)
            if i < j:
                offset = offset + size[i]
        plan[0, rank] = jnp.int32(j)
        plan[1, rank] = size[j]
        plan[2, rank] = offset
    used = size[0]
    for j in range(1, local):
        used = used + size[j]

    def part_of(t):
        turn = jnp.where(t < NF, 0, 2 * NF - RING)
        return (t % NF + turn) % NF

    def weights(t):
        return weight_copies(w1, w3, w2, w1b, w3b, w2b, wsem, plan[0, t // NF], part_of(t), (t + done - NF) % RING)

    limit = jnp.int32(caps[0][0])
    for n in range(1, len(caps)):
        limit = jnp.where(branch >= n, caps[n][0], limit)

    @pl.loop(used // 16, limit // 16)
    def _(n):
        blank = pl.ds(pl.multiple_of(n * 16, 16), 16)
        for q in range(owners):
            ret[q, blank, :] = jnp.zeros((16, width), BF16)

    @pl.loop(0, steps)
    def _(t):
        r, f, n = t // NF, t % NF, (t + done - NF) % RING
        e = plan[0, r]

        @pl.when(t >= RING)
        def _():
            for c in weights(t):
                c.wait()

        for size in (16, 32, slots):
            m = size * distant

            @pl.when(plan[1, r] == size)
            def _():
                x = rows[e, :, 0:size, :].reshape(m, width)
                ffn_part(x, w1b, w3b, w2b, n, mid, yacc, f == 0, m)

                @pl.when(f == NF - 1)
                def _():
                    first = pl.multiple_of(plan[2, r], 16)
                    for q in (0, 1):
                        mine = y_own[jnp.maximum(e - LATE, 0), q, 0:size, :]
                        ret[q, pl.ds(first, size), :] = jnp.where(e >= LATE, mine, jnp.zeros_like(mine))
                    for q in range(2, owners):
                        ret[q, pl.ds(first, size), :] = yacc[(q - 2) * size:(q - 1) * size, :].astype(BF16)

        @pl.when(t + RING < steps)
        def _():
            for c in weights(t + RING):
                c.start()


def expert_call(sizes, rows, y_own, w1p, w3p, w2p, w1, w3, w2, caps):
    local, distant, slots, width = rows.shape
    owners = distant + 2
    ft = w1p.shape[2]
    hbm = pl.BlockSpec(memory_space=pl.ANY)
    vmem = pl.BlockSpec(memory_space=pltpu.VMEM)
    flops = 3 * 2 * local * slots * owners * width * ft * NF // 2
    return pl.pallas_call(
        functools.partial(expert_kernel, caps),
        name='experts',
        out_shape=(
            pltpu.VMEM((owners, caps[-1][0], width), BF16),
            pltpu.VMEM(w1p.shape, BF16),
            pltpu.VMEM(w3p.shape, BF16),
            pltpu.VMEM(w2p.shape, BF16),
        ),
        in_specs=[vmem] * 6 + [hbm] * 3,
        out_specs=(vmem, vmem, vmem, vmem),
        input_output_aliases={3: 1, 4: 2, 5: 3},
        scratch_shapes=[
            pltpu.VMEM((distant * slots, ft), BF16),
            pltpu.VMEM((distant * slots, width), F32),
            pltpu.SMEM((3, local), I32),
            pltpu.SemaphoreType.DMA((RING, 3)),
        ],
        compiler_params=pltpu.CompilerParams(vmem_limit_bytes=12 * 1024 * 1024),
        cost_estimate=pl.CostEstimate(flops=flops, bytes_accessed=3 * 2 * local * width * ft * NF, transcendentals=0),
    )(sizes, rows, y_own, w1p, w3p, w2p, w1, w3, w2)[0]


REMOTE = (2, 4, 6)


def return_kernel(cap, chip_cap, ret, near, tok, goal, hid, w1, w3, w2, out, half, pack, got, acc, late, late_half, mid, yacc, w1b, w3b, w2b, send, recv, half_send, half_recv, wsem):
    me = lax.axis_index('ep')
    slots = near.shape[2]
    steps = LATE * NF

    def weights(t):
        return weight_copies(w1, w3, w2, w1b, w3b, w2b, wsem, t // NF, t % NF, t % LATE_RING)

    tokens, width = hid.shape
    lanes = goal.shape[1] // 2
    barrier = pltpu.get_barrier_semaphore()
    for q in (1, *REMOTE):
        pl.semaphore_signal(barrier, inc=1, device_id=dev(flip(me, q)), device_id_type=MESH)
    pl.semaphore_wait(barrier, 1 + len(REMOTE))
    halves, copies = {}, {}
    for q in (*REMOTE, 0):
        halves[q] = pltpu.make_async_remote_copy(src_ref=ret.at[q + 1, pl.ds(0, cap)], dst_ref=half.at[q // 2], send_sem=half_send.at[q // 2], recv_sem=half_recv.at[q // 2], device_id=dev(flip(me, 1)), device_id_type=MESH)
        halves[q].start()

    for q in REMOTE:
        row = iota((chip_cap, cap), 0).astype(F32)
        mine = (row == goal[q:q + 1, 0:cap]).astype(F32).astype(BF16)
        theirs = (row == goal[q:q + 1, lanes:lanes + cap]).astype(F32).astype(BF16)
        halves[q].wait_recv()
        for c in range(0, width, 512):
            part = jnp.dot(mine, ret[q, 0:cap, c:c + 512], preferred_element_type=F32)
            part = part + jnp.dot(theirs, half[q // 2, :, c:c + 512], preferred_element_type=F32)
            pack[q // 2 - 1, :, c:c + 512] = part.astype(BF16)
        copies[q] = pltpu.make_async_remote_copy(src_ref=pack.at[q // 2 - 1], dst_ref=got.at[q // 2 - 1], send_sem=send.at[q // 2 - 1], recv_sem=recv.at[q // 2 - 1], device_id=dev(flip(me, q)), device_id_type=MESH)
        copies[q].start()

    for t in range(LATE_RING):
        for c in weights(t):
            c.start()
    table = tok[...]

    def chosen(column, peer, at, count):
        lane = iota((tokens, count), 1).astype(F32)
        return jnp.concatenate([((column[k] == peer) & (table[:, at + k:at + k + 1] == lane)).astype(F32) for k in (0, 1)], axis=0).astype(BF16)

    owner = [table[:, 2 + k:3 + k] for k in (0, 1)]
    chip = [jnp.floor(o * 0.5) for o in owner]

    gate = [table[:, k:k + 1] for k in (0, 1)]
    scale = [table[:, 10 + k:11 + k] for k in (0, 1)]

    def add(pick, block, fresh=False, last=False):
        @pl.loop(0, width // 512)
        def _(n):
            cols = pl.ds(pl.multiple_of(n * 512, 512), 512)
            part = jnp.dot(pick, block(cols), preferred_element_type=F32)
            mixed = gate[0] * part[0:tokens] + gate[1] * part[tokens:2 * tokens]
            if not fresh:
                mixed = acc[:, cols] + mixed
            if last:
                out[:, cols] = (scale[0] * hid[:, cols].astype(F32) + scale[1] * mixed).astype(BF16)
            else:
                acc[:, cols] = mixed

    add(chosen(owner, me.astype(F32), 4, cap), lambda c: ret[0, 0:cap, c], fresh=True)
    pick = chosen(owner, flip(me, 1).astype(F32), 4, cap)
    halves[0].wait_recv()
    add(pick, lambda c: half[0, :, c])

    @pl.loop(0, steps)
    def _(t):
        e, f, n = t // NF, t % NF, t % LATE_RING
        for c in weights(t):
            c.wait()
        ffn_part(near[e, :, :, :].reshape(2 * slots, width), w1b, w3b, w2b, n, mid, yacc, f == 0, 2 * slots)

        @pl.when(f == NF - 1)
        def _():
            for q in (0, 1):
                late[q, pl.ds(pl.multiple_of(e * slots, slots), slots), :] = yacc[q * slots:(q + 1) * slots, :].astype(BF16)

        @pl.when(t + LATE_RING < steps)
        def _():
            for c in weights(t + LATE_RING):
                c.start()

    swap = pltpu.make_async_remote_copy(src_ref=late.at[1], dst_ref=late_half, send_sem=half_send.at[4], recv_sem=half_recv.at[4], device_id=dev(flip(me, 1)), device_id_type=MESH)
    swap.start()
    add(chosen(owner, me.astype(F32), 8, LATE * slots), lambda c: late[0, :, c])
    pick = chosen(owner, flip(me, 1).astype(F32), 8, LATE * slots)
    swap.wait_recv()
    add(pick, lambda c: late_half[:, c])
    for q in REMOTE:
        pick = chosen(chip, (flip(me, q) // 2).astype(F32), 6, chip_cap)
        copies[q].wait_recv()
        add(pick, lambda c: got[q // 2 - 1, :, c], last=q == REMOTE[-1])

    for copy in (*halves.values(), *copies.values(), swap):
        copy.wait_send()


def return_call(n, caps, ret, near, tok, goal, hidden, w1, w3, w2):
    owners, _, width = ret.shape
    slots, ft = near.shape[2], w1.shape[2] // NF
    tokens = hidden.shape[0]
    cap, chip_cap = caps
    vmem = pl.BlockSpec(memory_space=pltpu.VMEM)
    return pl.pallas_call(
        functools.partial(return_kernel, cap, chip_cap),
        name=f'return_{cap}_{chip_cap}',
        out_shape=jax.ShapeDtypeStruct((tokens, width), BF16),
        in_specs=[vmem] * 5 + [pl.BlockSpec(memory_space=pl.ANY)] * 3,
        out_specs=vmem,
        scratch_shapes=[
            pltpu.VMEM((owners // 2, cap, width), BF16),
            pltpu.VMEM((len(REMOTE), chip_cap, width), BF16),
            pltpu.VMEM((len(REMOTE), chip_cap, width), BF16),
            pltpu.VMEM((tokens, width), F32),
            pltpu.VMEM((2, LATE * slots, width), BF16),
            pltpu.VMEM((LATE * slots, width), BF16),
            pltpu.VMEM((2 * slots, ft), BF16),
            pltpu.VMEM((2 * slots, width), F32),
            pltpu.VMEM((LATE_RING, width, ft), BF16),
            pltpu.VMEM((LATE_RING, width, ft), BF16),
            pltpu.VMEM((LATE_RING, ft, width), BF16),
            pltpu.SemaphoreType.DMA((len(REMOTE),)),
            pltpu.SemaphoreType.DMA((len(REMOTE),)),
            pltpu.SemaphoreType.DMA((owners // 2 + 1,)),
            pltpu.SemaphoreType.DMA((owners // 2 + 1,)),
            pltpu.SemaphoreType.DMA((LATE_RING, 3)),
        ],
        compiler_params=pltpu.CompilerParams(collective_id=1 + n, has_side_effects=True, vmem_limit_bytes=34 * 1024 * 1024),
    )(ret, near, tok, goal, hidden, w1, w3, w2)


def capacities(local, slots):
    full = [slots * n + 16 * (local - n) for n in range(1, local + 1)]
    chip = [2 * slots + 8 + (slots - 8) * n for n in range(local - 1)]
    return (*zip(full, chip), (local * slots, 2 * local * slots))


def solution(mesh):
    owners = mesh.shape['ep']

    def local_step(hidden, router_w, expert_ids, w_gate, w_up, w_down, post_scale):
        tokens = hidden.shape[0]
        local = w_gate.shape[0]
        slots = tokens // max(1, local * owners // 8)
        caps = capacities(local, slots)
        near, far, y_own, tok, goal, plan, which, w1p, w3p, w2p = gather_call(hidden, expert_ids.T, router_w.T, post_scale, w_gate, w_up, w_down, owners, caps)
        ret = expert_call(plan, far, y_own, w1p, w3p, w2p, w_gate, w_up, w_down, caps)
        branches = [functools.partial(return_call, n, cap) for n, cap in enumerate(caps)]
        return lax.switch(which.reshape(()), branches, ret, near, tok, goal, hidden, w_gate, w_up, w_down)

    tok_spec = P(('dp', 'ep'))
    return jax.shard_map(local_step, mesh=mesh, in_specs=(tok_spec, P(), tok_spec, P('ep'), P('ep'), P('ep'), P()), out_specs=tok_spec, check_vma=False)
```

```python
import functools

import jax
import jax.numpy as jnp
from jax import lax
from jax.experimental import pallas as pl
from jax.experimental.pallas import tpu as pltpu
from jax.sharding import PartitionSpec as P

MESH = pl.DeviceIdType.MESH
F32, BF16, I32 = jnp.float32, jnp.bfloat16, jnp.int32
NT = (((1,), (1,)), ((), ()))


def flip(idx, mask):
    out = idx
    for bit in (1, 2, 4):
        if mask & bit:
            out = out + bit - 2 * bit * ((idx // bit) % 2)
    return out


def dev(idx):
    return (lax.axis_index('dp'), idx)


def iota(shape, dim):
    return lax.broadcasted_iota(I32, shape, dim)


def weight_copies(w1, w3, w2, w1b, w3b, w2b, sem, e, f, n):
    ft = w1b.shape[2]
    cols = pl.ds(pl.multiple_of(f * ft, ft), ft)
    return (
        pltpu.make_async_copy(w1.at[e, :, cols], w1b.at[n], sem.at[n, 0]),
        pltpu.make_async_copy(w3.at[e, :, cols], w3b.at[n], sem.at[n, 1]),
        pltpu.make_async_copy(w2.at[e, cols, :], w2b.at[n], sem.at[n, 2]),
    )


def ffn_part(x, w1b, w3b, w2b, n, mid, yacc, fresh, m):
    for c in range(0, w1b.shape[2], 256):
        gate = jnp.dot(x, w1b[n, :, c:c + 256], preferred_element_type=F32)
        up = jnp.dot(x, w3b[n, :, c:c + 256], preferred_element_type=F32)
        mid[0:m, c:c + 256] = (gate * jax.nn.sigmoid(gate) * up).astype(BF16)
    for c in range(0, w2b.shape[2], 512):
        part = jnp.dot(mid[0:m, :], w2b[n, :, c:c + 512], preferred_element_type=F32)
        yacc[0:m, c:c + 512] = jnp.where(fresh, 0.0, yacc[0:m, c:c + 512]) + part


CHUNKS = 4
NF = 3
RING = 4
LATE_RING = 2
BRANCH_LANE = 127
LATE = 2


def gather_kernel(caps, hid_in, ids_in, wrt_in, scale_in, w1, w3, w2, near, far, y_own, tok, goal, plan, which, w1p, w3p, w2p, hid, ids, wrt, scale, pos, mid, yacc, land, ids_all, send, recv, id_send, id_recv, wsem, in_sem):
    me = lax.axis_index('ep')
    own = [pltpu.make_async_copy(src, dst, in_sem.at[n]) for n, (src, dst) in enumerate(((hid_in, hid), (ids_in, ids), (wrt_in, wrt), (scale_in, scale)))]
    for c in own:
        c.start()
    local, _, slots, _ = near.shape
    owners = 2 + far.shape[1]
    steps = (local - LATE) * NF

    def weights(t):
        return weight_copies(w1, w3, w2, w1p, w3p, w2p, wsem, local - 1 - t // NF, t % NF, t % RING)

    tokens, width = hid.shape
    experts = wrt.shape[0]
    rows = tokens // CHUNKS
    barrier = pltpu.get_barrier_semaphore()
    for q in range(1, owners):
        pl.semaphore_signal(barrier, inc=1, device_id=dev(flip(me, q)), device_id_type=MESH)
    pl.semaphore_wait(barrier, owners - 1)
    own[0].wait()
    own[1].wait()

    def piece(q, c):
        return (hid if q == 0 else land.at[q]).at[pl.ds(c * rows, rows)]

    def remote(q, c, n, to):
        return pltpu.make_async_remote_copy(src_ref=piece(q, c), dst_ref=land.at[q ^ to, pl.ds(c * rows, rows)], send_sem=send.at[n], recv_sem=recv.at[n], device_id=dev(flip(me, to)), device_id_type=MESH)

    id_copies = []
    for q in range(1, owners):
        id_copies.append(pltpu.make_async_remote_copy(src_ref=ids, dst_ref=ids_all.at[q], send_sem=id_send.at[q], recv_sem=id_recv.at[q], device_id=dev(flip(me, q)), device_id_type=MESH))
    x_order, y_order = (0, 1, 2, 3), (2, 3, 0, 1)
    to_x = {c: remote(0, c, c, 2) for c in x_order}
    to_y = {c: remote(0, c, 4 + c, 4) for c in y_order}
    for cx, cy in zip(x_order, y_order):
        to_x[cx].start()
        to_y[cy].start()
        if cx == 0:
            for c in id_copies:
                c.start()
    to_mate = pltpu.make_async_remote_copy(src_ref=hid, dst_ref=land.at[1], send_sem=send.at[24], recv_sem=recv.at[24], device_id=dev(flip(me, 1)), device_id_type=MESH)
    to_mate.start()
    for t in range(RING):
        for c in weights(t):
            c.start()

    own[2].wait()
    own[3].wait()
    h = hid[...]
    w = wrt[...]
    w_hi = w.astype(BF16)
    rest = w - w_hi.astype(F32)
    w_mid = rest.astype(BF16)
    w_lo = (rest - w_mid.astype(F32)).astype(BF16)
    dot = functools.partial(lax.dot_general, dimension_numbers=NT, preferred_element_type=F32)
    logits = dot(h, w_hi) + (dot(h, w_mid) + dot(h, w_lo))
    ex = jnp.exp(logits - jnp.max(logits, axis=1, keepdims=True))
    prob = ex / jnp.sum(ex, axis=1, keepdims=True)
    ta, tb = iota((tokens, tokens), 0), iota((tokens, tokens), 1)
    eye = (ta == tb).astype(F32).astype(BF16)
    own_ids = ids[...].astype(F32)
    lane = iota((tokens, experts), 1).astype(F32)
    id_col = [dot(eye, jnp.broadcast_to(own_ids[k:k + 1], (8, tokens)).astype(BF16))[:, 0:1] for k in (0, 1)]
    pick = [(id_col[k] == lane).astype(F32) for k in (0, 1)]
    g = [jnp.sum(pick[k] * prob, axis=1, keepdims=True) for k in (0, 1)]
    total = g[0] + g[1]

    for c in id_copies:
        c.wait_recv()
    ids_all[0] = ids[...]
    counts = []
    for q in range(owners):
        both = ids_all[q]
        e_col = iota((experts, tokens), 0)
        hot = ((both[0:1] == e_col) | (both[1:2] == e_col)).astype(F32).astype(BF16)
        counts.append(dot(jnp.ones((8, tokens), BF16), hot))
    most = functools.reduce(jnp.maximum, counts)
    count = jnp.concatenate([c[0:1] for c in counts], axis=0)
    stride = jnp.where(most > 32.0, float(slots), jnp.where(most > 16.0, 32.0, 16.0))
    mark = lambda mask: mask.astype(F32).astype(BF16)
    plain = functools.partial(jnp.dot, preferred_element_type=F32)
    ea, eb = iota((experts, experts), 0), iota((experts, experts), 1)
    same, same_chip = ea // local == eb // local, ea // (2 * local) == eb // (2 * local)
    offset = plain(stride.astype(BF16), mark(same & (ea < eb)))
    need = jnp.max(plain(stride.astype(BF16), mark(same)), axis=1, keepdims=True)[0:1]
    need_chip = jnp.max(jnp.max(plain(count.astype(BF16), mark(same_chip)), axis=1, keepdims=True), axis=0, keepdims=True)
    branch = jnp.zeros((1, 1), F32)
    for limit, limit_chip in caps[:-1]:
        branch = branch + ((need > limit) | (need_chip > limit_chip)).astype(F32)
    which[0] = jnp.max(branch).astype(I32)
    rank = plain(mark(tb < ta), (pick[0] + pick[1]).astype(BF16))
    chip_first = plain(count.astype(BF16), mark(same_chip & (ea < eb)))[0:1]
    local_of = lane - jnp.floor(lane * (1.0 / local)) * local
    late_place = jnp.where(local_of < LATE, local_of * slots + rank, -1.0)
    late = [jnp.sum(pick[k] * late_place, axis=1, keepdims=True) for k in (0, 1)]
    slot = [jnp.sum(pick[k] * (rank + offset[0:1]), axis=1, keepdims=True) for k in (0, 1)]
    packed = [jnp.sum(pick[k] * (rank + chip_first), axis=1, keepdims=True) for k in (0, 1)]
    owner = [jnp.floor(id_col[k] * (1.0 / local)) for k in (0, 1)]
    wide = iota((tokens, 128), 1)
    table = jnp.zeros((tokens, 128), F32)
    for n, col in enumerate((g[0] / total, g[1] / total, *owner, *slot, *packed, *late, scale[0], scale[1])):
        table = jnp.where(wide == n, col, table)
    tok[...] = table

    e_row, n_col = iota((experts, 128), 0), iota((experts, 128), 1)
    e_of = jnp.where(n_col < local, me * local + n_col, flip(me, 1) * local + n_col - local)
    used = n_col < 2 * local
    held = plain(count.astype(BF16), mark(used & (e_row == e_of)))
    start = plain(count.astype(BF16), mark(used & (e_row // (2 * local) == me // 2) & (e_row < e_of)))
    base = plain(stride.astype(BF16), mark(used & (e_row // local == e_of // local) & (e_row < e_of)))
    base_size = plain(stride.astype(BF16), mark(used & (e_row == e_of)))
    lane_of = iota((owners, goal.shape[1]), 1)
    where_to = jnp.full((owners, goal.shape[1]), -1.0, F32)
    for n in range(2 * local):
        at = (lane_of - (n // local) * (goal.shape[1] // 2)).astype(F32) - base[0:1, n:n + 1]
        where_to = jnp.where((at >= 0.0) & (at < held[:, n:n + 1]), at + start[:, n:n + 1], where_to)
    goal[...] = where_to

    first, second = (jnp.concatenate([ids_all[q, k:k + 1] for q in range(owners)], axis=0) for k in (0, 1))
    marks = jnp.concatenate([((first == me * local + j) | (second == me * local + j)).astype(F32) for j in range(local)], axis=0)
    earlier = plain(marks.astype(BF16), (ta < tb).astype(F32).astype(BF16))
    pos[...] = jnp.where(marks > 0.5, earlier, -1.0)
    plan[...] = jnp.where(n_col[0:8] == BRANCH_LANE, branch, base_size).astype(I32)

    def pick_rows(q):
        at = iota((slots, tokens), 0).astype(F32)
        match = jnp.concatenate([(at == pos[j * owners + q:j * owners + q + 1, :]).astype(F32) for j in range(local)], axis=0).astype(BF16)

        def columns(cols):
            block = hid[:, cols] if q == 0 else land[q, :, cols]
            part = jnp.dot(match, block, preferred_element_type=F32).astype(BF16)
            for j in range(local):
                to = near.at[j, q] if q < 2 else far.at[j, q - 2]
                to[:, cols] = part[j * slots:(j + 1) * slots]

        if q < 6:
            @pl.loop(0, width // 512)
            def _(n):
                columns(pl.ds(pl.multiple_of(n * 512, 512), 512))
        else:
            for c in range(0, width, 512):
                columns(pl.ds(c, 512))

    def own_steps(first, last):
        @pl.loop(first, last)
        def _(t):
            e, f, n = local - 1 - t // NF, t % NF, t % RING
            for c in weights(t):
                c.wait()
            x = near[e, :, :, :].reshape(2 * slots, width)
            ffn_part(x, w1p, w3p, w2p, n, mid, yacc, f == 0, 2 * slots)

            @pl.when(f == NF - 1)
            def _():
                for q in (0, 1):
                    y_own[e - LATE, q, :, :] = yacc[q * slots:(q + 1) * slots, :].astype(BF16)

            @pl.when(t + RING < steps)
            def _():
                for c in weights(t + RING):
                    c.start()

    sent = [*to_x.values(), *to_y.values(), to_mate]

    def pass_on(q, c, n, to):
        copy = remote(q, c, n, to)
        copy.start()
        sent.append(copy)
        return copy

    pick_rows(0)
    to_mate.wait_recv()
    pick_rows(1)
    across, mates = {}, {2: [], 4: [], 6: []}
    for n, (cx, cy) in enumerate(zip(x_order, y_order)):
        if n < 2:
            own_steps(n * steps // 2, (n + 1) * steps // 2)
        to_x[cx].wait_recv()
        if cx in (0, 1):
            across[cx] = pass_on(2, cx, 8 + cx, 4)
        mates[2].append(pass_on(2, cx, 12 + cx, 1))
        to_y[cy].wait_recv()
        if cy in (2, 3):
            across[cy] = pass_on(4, cy, 8 + cy, 2)
        mates[4].append(pass_on(4, cy, 16 + cy, 1))
    for q in (2, 4):
        pick_rows(q)
    for q in (2, 4):
        for m in mates[q]:
            m.wait_recv()
        pick_rows(q + 1)
    for c in (0, 2, 1, 3):
        across[c].wait_recv()
        mates[6].append(pass_on(6, c, 20 + c, 1))
    pick_rows(6)
    for m in mates[6]:
        m.wait_recv()
    pick_rows(7)
    for m in sent:
        m.wait_send()
    for c in id_copies:
        c.wait_send()


def gather_call(hidden, ids_t, wr_t, scale, w1, w3, w2, owners, caps):
    tokens, width = hidden.shape
    experts = wr_t.shape[0]
    local, _, ffn = w1.shape
    slots = caps[-1][0] // local
    ft = ffn // NF
    vmem = pl.BlockSpec(memory_space=pltpu.VMEM)
    hbm = pl.BlockSpec(memory_space=pl.ANY)
    return pl.pallas_call(
        functools.partial(gather_kernel, caps),
        name='gather_tokens',
        out_shape=(
            pltpu.VMEM((local, 2, slots, width), BF16),
            pltpu.VMEM((local, owners - 2, slots, width), BF16),
            pltpu.VMEM((local - LATE, 2, slots, width), BF16),
            jax.ShapeDtypeStruct((tokens, 128), F32),
            jax.ShapeDtypeStruct((owners, 2 * local * slots), F32),
            jax.ShapeDtypeStruct((8, 128), I32),
            jax.ShapeDtypeStruct((1,), I32),
            pltpu.VMEM((RING, width, ft), BF16),
            pltpu.VMEM((RING, width, ft), BF16),
            pltpu.VMEM((RING, ft, width), BF16),
        ),
        in_specs=[hbm, *[pl.BlockSpec(memory_space=pltpu.HBM)] * 3, hbm, hbm, hbm],
        out_specs=(*[vmem] * 6, pl.BlockSpec(memory_space=pltpu.SMEM), *[vmem] * 3),
        scratch_shapes=[
            pltpu.VMEM((tokens, width), BF16),
            pltpu.VMEM((2, tokens), I32),
            pltpu.VMEM((experts, width), F32),
            pltpu.SMEM((2,), F32),
            pltpu.VMEM((local * owners, tokens), F32),
            pltpu.VMEM((2 * slots, ft), BF16),
            pltpu.VMEM((2 * slots, width), F32),
            pltpu.VMEM((owners, tokens, width), BF16),
            pltpu.VMEM((owners, 2, tokens), I32),
            pltpu.SemaphoreType.DMA((25,)),
            pltpu.SemaphoreType.DMA((25,)),
            pltpu.SemaphoreType.DMA((owners,)),
            pltpu.SemaphoreType.DMA((owners,)),
            pltpu.SemaphoreType.DMA((RING, 3)),
            pltpu.SemaphoreType.DMA((4,)),
        ],
        compiler_params=pltpu.CompilerParams(collective_id=0, has_side_effects=True, vmem_limit_bytes=13 * 1024 * 1024),
    )(hidden, *(pltpu.with_memory_space_constraint(x, pltpu.HBM) for x in (ids_t, wr_t, scale)), w1, w3, w2)


def expert_kernel(caps, info, rows, y_own, _w1b, _w3b, _w2b, w1, w3, w2, ret, w1b, w3b, w2b, mid, yacc, plan, wsem):
    local, distant, slots, width = rows.shape
    owners = distant + 2
    steps = local * NF
    done = (local - LATE) * NF

    size = [info[0, j] for j in range(local)]
    branch = info[0, BRANCH_LANE]
    for j in range(local):
        rank = jnp.int32(j - LATE if j >= LATE else local - LATE)
        offset = jnp.int32(0)
        for i in range(local):
            if i < LATE and j < LATE and i != j:
                ahead = (size[i] >= size[j]) if i < j else (size[i] > size[j])
                rank = rank + ahead.astype(I32)
            if i < j:
                offset = offset + size[i]
        plan[0, rank] = jnp.int32(j)
        plan[1, rank] = size[j]
        plan[2, rank] = offset
    used = size[0]
    for j in range(1, local):
        used = used + size[j]

    def part_of(t):
        turn = jnp.where(t < NF, 0, 2 * NF - RING)
        return (t % NF + turn) % NF

    def weights(t):
        return weight_copies(w1, w3, w2, w1b, w3b, w2b, wsem, plan[0, t // NF], part_of(t), (t + done - NF) % RING)

    limit = jnp.int32(caps[0][0])
    for n in range(1, len(caps)):
        limit = jnp.where(branch >= n, caps[n][0], limit)

    @pl.loop(used // 16, limit // 16)
    def _(n):
        blank = pl.ds(pl.multiple_of(n * 16, 16), 16)
        for q in range(owners):
            ret[q, blank, :] = jnp.zeros((16, width), BF16)

    @pl.loop(0, steps)
    def _(t):
        r, f, n = t // NF, t % NF, (t + done - NF) % RING
        e = plan[0, r]

        @pl.when(t >= RING)
        def _():
            for c in weights(t):
                c.wait()

        for size in (16, 32, slots):
            m = size * distant

            @pl.when(plan[1, r] == size)
            def _():
                x = rows[e, :, 0:size, :].reshape(m, width)
                ffn_part(x, w1b, w3b, w2b, n, mid, yacc, f == 0, m)

                @pl.when(f == NF - 1)
                def _():
                    first = pl.multiple_of(plan[2, r], 16)
                    for q in (0, 1):
                        mine = y_own[jnp.maximum(e - LATE, 0), q, 0:size, :]
                        ret[q, pl.ds(first, size), :] = jnp.where(e >= LATE, mine, jnp.zeros_like(mine))
                    for q in range(2, owners):
                        ret[q, pl.ds(first, size), :] = yacc[(q - 2) * size:(q - 1) * size, :].astype(BF16)

        @pl.when(t + RING < steps)
        def _():
            for c in weights(t + RING):
                c.start()


def expert_call(sizes, rows, y_own, w1p, w3p, w2p, w1, w3, w2, caps):
    local, distant, slots, width = rows.shape
    owners = distant + 2
    ft = w1p.shape[2]
    hbm = pl.BlockSpec(memory_space=pl.ANY)
    vmem = pl.BlockSpec(memory_space=pltpu.VMEM)
    flops = 3 * 2 * local * slots * owners * width * ft * NF // 2
    return pl.pallas_call(
        functools.partial(expert_kernel, caps),
        name='experts',
        out_shape=(
            pltpu.VMEM((owners, caps[-1][0], width), BF16),
            pltpu.VMEM(w1p.shape, BF16),
            pltpu.VMEM(w3p.shape, BF16),
            pltpu.VMEM(w2p.shape, BF16),
        ),
        in_specs=[vmem] * 6 + [hbm] * 3,
        out_specs=(vmem, vmem, vmem, vmem),
        input_output_aliases={3: 1, 4: 2, 5: 3},
        scratch_shapes=[
            pltpu.VMEM((distant * slots, ft), BF16),
            pltpu.VMEM((distant * slots, width), F32),
            pltpu.SMEM((3, local), I32),
            pltpu.SemaphoreType.DMA((RING, 3)),
        ],
        compiler_params=pltpu.CompilerParams(vmem_limit_bytes=12 * 1024 * 1024),
        cost_estimate=pl.CostEstimate(flops=flops, bytes_accessed=3 * 2 * local * width * ft * NF, transcendentals=0),
    )(sizes, rows, y_own, w1p, w3p, w2p, w1, w3, w2)[0]


REMOTE = (2, 4, 6)


def return_kernel(cap, chip_cap, ret, near, tok, goal, hid, w1, w3, w2, out, half, pack, got, acc, late, late_half, mid, yacc, w1b, w3b, w2b, send, recv, half_send, half_recv, wsem):
    me = lax.axis_index('ep')
    slots = near.shape[2]
    steps = LATE * NF

    def weights(t):
        return weight_copies(w1, w3, w2, w1b, w3b, w2b, wsem, t // NF, t % NF, t % LATE_RING)

    tokens, width = hid.shape
    lanes = goal.shape[1] // 2
    barrier = pltpu.get_barrier_semaphore()
    for q in (1, *REMOTE):
        pl.semaphore_signal(barrier, inc=1, device_id=dev(flip(me, q)), device_id_type=MESH)
    pl.semaphore_wait(barrier, 1 + len(REMOTE))
    halves, copies = {}, {}
    for q in (*REMOTE, 0):
        halves[q] = pltpu.make_async_remote_copy(src_ref=ret.at[q + 1, pl.ds(0, cap)], dst_ref=half.at[q // 2], send_sem=half_send.at[q // 2], recv_sem=half_recv.at[q // 2], device_id=dev(flip(me, 1)), device_id_type=MESH)
        halves[q].start()

    row = iota((chip_cap, cap), 0).astype(F32)
    for q in REMOTE:
        mine = (row == goal[q:q + 1, 0:cap]).astype(F32).astype(BF16)
        for c in range(0, width, 512):
            pack[q // 2 - 1, :, c:c + 512] = jnp.dot(mine, ret[q, 0:cap, c:c + 512], preferred_element_type=F32).astype(BF16)
    for q in REMOTE:
        theirs = (row == goal[q:q + 1, lanes:lanes + cap]).astype(F32).astype(BF16)
        halves[q].wait_recv()
        for c in range(0, width, 512):
            part = jnp.dot(theirs, half[q // 2, :, c:c + 512], preferred_element_type=F32)
            part = part + pack[q // 2 - 1, :, c:c + 512].astype(F32)
            pack[q // 2 - 1, :, c:c + 512] = part.astype(BF16)
        copies[q] = pltpu.make_async_remote_copy(src_ref=pack.at[q // 2 - 1], dst_ref=got.at[q // 2 - 1], send_sem=send.at[q // 2 - 1], recv_sem=recv.at[q // 2 - 1], device_id=dev(flip(me, q)), device_id_type=MESH)
        copies[q].start()

    for t in range(LATE_RING):
        for c in weights(t):
            c.start()
    table = tok[...]

    def chosen(column, peer, at, count):
        lane = iota((tokens, count), 1).astype(F32)
        return jnp.concatenate([((column[k] == peer) & (table[:, at + k:at + k + 1] == lane)).astype(F32) for k in (0, 1)], axis=0).astype(BF16)

    owner = [table[:, 2 + k:3 + k] for k in (0, 1)]
    chip = [jnp.floor(o * 0.5) for o in owner]

    gate = [table[:, k:k + 1] for k in (0, 1)]
    scale = [table[:, 10 + k:11 + k] for k in (0, 1)]

    def add(pick, block, fresh=False, last=False):
        @pl.loop(0, width // 512)
        def _(n):
            cols = pl.ds(pl.multiple_of(n * 512, 512), 512)
            part = jnp.dot(pick, block(cols), preferred_element_type=F32)
            mixed = gate[0] * part[0:tokens] + gate[1] * part[tokens:2 * tokens]
            if not fresh:
                mixed = acc[:, cols] + mixed
            if last:
                out[:, cols] = (scale[0] * hid[:, cols].astype(F32) + scale[1] * mixed).astype(BF16)
            else:
                acc[:, cols] = mixed

    add(chosen(owner, me.astype(F32), 4, cap), lambda c: ret[0, 0:cap, c], fresh=True)
    pick = chosen(owner, flip(me, 1).astype(F32), 4, cap)
    halves[0].wait_recv()
    add(pick, lambda c: half[0, :, c])

    @pl.loop(0, steps)
    def _(t):
        e, f, n = t // NF, t % NF, t % LATE_RING
        for c in weights(t):
            c.wait()
        ffn_part(near[e, :, :, :].reshape(2 * slots, width), w1b, w3b, w2b, n, mid, yacc, f == 0, 2 * slots)

        @pl.when(f == NF - 1)
        def _():
            for q in (0, 1):
                late[q, pl.ds(pl.multiple_of(e * slots, slots), slots), :] = yacc[q * slots:(q + 1) * slots, :].astype(BF16)

        @pl.when(t + LATE_RING < steps)
        def _():
            for c in weights(t + LATE_RING):
                c.start()

    swap = pltpu.make_async_remote_copy(src_ref=late.at[1], dst_ref=late_half, send_sem=half_send.at[4], recv_sem=half_recv.at[4], device_id=dev(flip(me, 1)), device_id_type=MESH)
    swap.start()
    add(chosen(owner, me.astype(F32), 8, LATE * slots), lambda c: late[0, :, c])
    pick = chosen(owner, flip(me, 1).astype(F32), 8, LATE * slots)
    swap.wait_recv()
    add(pick, lambda c: late_half[:, c])
    for q in REMOTE:
        pick = chosen(chip, (flip(me, q) // 2).astype(F32), 6, chip_cap)
        copies[q].wait_recv()
        add(pick, lambda c: got[q // 2 - 1, :, c], last=q == REMOTE[-1])

    for copy in (*halves.values(), *copies.values(), swap):
        copy.wait_send()


def return_call(n, caps, ret, near, tok, goal, hidden, w1, w3, w2):
    owners, _, width = ret.shape
    slots, ft = near.shape[2], w1.shape[2] // NF
    tokens = hidden.shape[0]
    cap, chip_cap = caps
    vmem = pl.BlockSpec(memory_space=pltpu.VMEM)
    return pl.pallas_call(
        functools.partial(return_kernel, cap, chip_cap),
        name=f'return_{cap}_{chip_cap}',
        out_shape=jax.ShapeDtypeStruct((tokens, width), BF16),
        in_specs=[vmem] * 5 + [pl.BlockSpec(memory_space=pl.ANY)] * 3,
        out_specs=vmem,
        scratch_shapes=[
            pltpu.VMEM((owners // 2, cap, width), BF16),
            pltpu.VMEM((len(REMOTE), chip_cap, width), BF16),
            pltpu.VMEM((len(REMOTE), chip_cap, width), BF16),
            pltpu.VMEM((tokens, width), F32),
            pltpu.VMEM((2, LATE * slots, width), BF16),
            pltpu.VMEM((LATE * slots, width), BF16),
            pltpu.VMEM((2 * slots, ft), BF16),
            pltpu.VMEM((2 * slots, width), F32),
            pltpu.VMEM((LATE_RING, width, ft), BF16),
            pltpu.VMEM((LATE_RING, width, ft), BF16),
            pltpu.VMEM((LATE_RING, ft, width), BF16),
            pltpu.SemaphoreType.DMA((len(REMOTE),)),
            pltpu.SemaphoreType.DMA((len(REMOTE),)),
            pltpu.SemaphoreType.DMA((owners // 2 + 1,)),
            pltpu.SemaphoreType.DMA((owners // 2 + 1,)),
            pltpu.SemaphoreType.DMA((LATE_RING, 3)),
        ],
        compiler_params=pltpu.CompilerParams(collective_id=1 + n, has_side_effects=True, vmem_limit_bytes=34 * 1024 * 1024),
    )(ret, near, tok, goal, hidden, w1, w3, w2)


def capacities(local, slots):
    full = [slots * n + 16 * (local - n) for n in range(1, local + 1)]
    chip = [2 * slots + 8 + (slots - 8) * n for n in range(local - 1)]
    return (*zip(full, chip), (local * slots, 2 * local * slots))


def solution(mesh):
    owners = mesh.shape['ep']

    def local_step(hidden, router_w, expert_ids, w_gate, w_up, w_down, post_scale):
        tokens = hidden.shape[0]
        local = w_gate.shape[0]
        slots = tokens // max(1, local * owners // 8)
        caps = capacities(local, slots)
        near, far, y_own, tok, goal, plan, which, w1p, w3p, w2p = gather_call(hidden, expert_ids.T, router_w.T, post_scale, w_gate, w_up, w_down, owners, caps)
        ret = expert_call(plan, far, y_own, w1p, w3p, w2p, w_gate, w_up, w_down, caps)
        branches = [functools.partial(return_call, n, cap) for n, cap in enumerate(caps)]
        return lax.switch(which[0], branches, ret, near, tok, goal, hidden, w_gate, w_up, w_down)

    tok_spec = P(('dp', 'ep'))
    return jax.shard_map(local_step, mesh=mesh, in_specs=(tok_spec, P(), tok_spec, P('ep'), P('ep'), P('ep'), P()), out_specs=tok_spec, check_vma=False)
```
